256 devices in a mesh: sx: 8 (over x, core), sy: 32 (over z, y).
Axes of the slice: x: 4, y: 4, z: 8, core: 2. Of those that a mesh axis runs over, the one named last changes fastest.
Arguments:
- right_side: float32 [8, 8, 8, 65536], P(None, None, None, ('sx', 'sy')), may hold values from -8 to 8
- stretch: float32 [3, 65536], P(None, ('sx', 'sy')), may hold values from 0.3 to 3
- mass_term: float32 [65536], P(('sx', 'sy')), may hold values from 0.5 to 2
- slot_position: int32 [65536], P(('sx', 'sy')), may hold values from 0 to 255, as said below
- coarse_group: int32 [65536], P(('sx', 'sy')), may hold values from 0 to 4095, as said below
Outputs:
- smoothed: float32 [8, 8, 8, 65536], P(None, None, None, ('sx', 'sy'))
- fine_residual: float32 [8, 8, 8, 65536], P(None, None, None, ('sx', 'sy'))
- coarse_rhs: float32 [8, 4096], P(None, ('sx', 'sy'))
The draws below stay inside these ranges and needn't reach their ends.
Inputs may be any that keep to these rules, and one draw needn't show every extreme that they name: `slot_position`: each device's block of 256 entries is a permutation of 0 to 255. `coarse_group`: group k is owned by the device of block index k // 16 (block index i * 32 + j); an element of device (i, j) belongs to a group owned by some device (i, j') of the same first index.
All inputs are finite; a program needn't handle non-finite values.
Results may differ from the reference program's by a relative error of at most 0.00013.
Values sent between devices are 32-bit elements; how exact they have to be, the bound alone decides.
No kernel may reach another device: no remote copies, remote signals or barrier semaphores. Data moves between devices by JAX's collectives and lax.ppermute only.
A program may use at most 128 MiB of HBM per device.

```python
import math
import jax
import jax.numpy as jnp
from jax import lax

NODES = 8
SWEEPS = 2
EX = 1
EY = 2
EZ = 128
GRP_DEV = 16
E_DEV = 256
ELEMENTS = 65536
GROUPS = 4096
N_SX = 8
N_SY = 32
DEVICES = 256


def draw_slot_position(key, part):
    base = jax.random.fold_in(key, 11)
    keys = jax.vmap(lambda number: jax.random.fold_in(base, number))(jnp.arange(DEVICES))
    orders = jax.vmap(lambda single: jax.random.permutation(single, EX * EY * EZ))(keys)
    return orders.reshape(-1).astype(jnp.int32)


def draw_coarse_group(key, part):
    element = jnp.arange(ELEMENTS, dtype=jnp.int32)
    device = element // E_DEV
    local = element % E_DEV
    row_index = device // N_SY
    col_index = device % N_SY
    offset = jax.random.randint(jax.random.fold_in(key, 21), (ELEMENTS,), 0, N_SY)
    offset = jnp.where(local == 0, N_SY // 2, offset)
    offset = jnp.where(local == 1, 1, offset)
    owner_col = (col_index + offset) % N_SY
    member = jax.random.randint(jax.random.fold_in(key, 22), (ELEMENTS,), 0, GRP_DEV)
    return ((row_index * N_SY + owner_col) * GRP_DEV + member).astype(jnp.int32)


def levels(rng, shape, split, low, largest):
    def one(dim, blocks):
        steps = jax.random.uniform(jax.random.fold_in(jax.random.fold_in(rng, 6), dim), (blocks,), jnp.float32, low / len(split), largest / len(split))
        return jnp.repeat(jnp.exp(steps), shape[dim] // blocks).reshape((-1,) + (1,) * (len(shape) - dim - 1))

    level = one(*split[0])
    for cut in split[1:]:
        level = level * one(*cut)
    return level


def noise(stream_key, extent, deviation, limit, split=(), kind=jnp.bfloat16):
    drawn = jax.random.normal(stream_key, extent, jnp.float32) * deviation
    if len(split) > 0:
        drawn = levels(stream_key, extent, split, -0.22, 0.18) * drawn
    return jnp.clip(drawn, min=-limit, max=limit).astype(kind)


def setup_inputs(seed: int = 0) -> dict:
    key_of = jax.random.split(jax.random.key(seed), 6)
    right_side = noise(key_of[0], (NODES, NODES, NODES, ELEMENTS), 1.0, 8.0, ((3, 256),), jnp.float32)
    stretch = jnp.clip(jnp.exp(math.log(3.0) - 2.3025851 * jax.random.uniform(key_of[1], (3, ELEMENTS), jnp.float32) ** levels(key_of[1], (3, ELEMENTS), ((1, 256),), -0.2, 0.2)), 0.3, 3.0)
    mass_term = jnp.clip(jnp.exp(math.log(2.0) - 1.3862944 * jax.random.uniform(key_of[2], (ELEMENTS,), jnp.float32) ** levels(key_of[2], (ELEMENTS,), ((0, 256),), -0.2, 0.2)), 0.5, 2.0)
    slot_position = draw_slot_position(jax.random.fold_in(key_of[5], 71), 0)
    coarse_group = draw_coarse_group(jax.random.fold_in(key_of[5], 71), 0)
    return {"right_side": right_side, "stretch": stretch, "mass_term": mass_term, "slot_position": slot_position, "coarse_group": coarse_group}


relax_factor = 0.35

def leading(values, axis, amount):
    return lax.slice_in_dim(values, 0, amount, axis=axis)

def trailing(values, axis, amount):
    size = values.shape[axis]
    return lax.slice_in_dim(values, size - amount, size, axis=axis)

def extend_axis(values, node_axis, elem_axis):
    top_layer = trailing(values, node_axis, 1)
    bottom = leading(values, node_axis, 1)
    elements = values.shape[elem_axis]
    empty = jnp.zeros_like(trailing(top_layer, elem_axis, 1))
    below_layer = jnp.concatenate([empty, leading(top_layer, elem_axis, elements - 1)], axis=elem_axis)
    above_layer = jnp.concatenate([trailing(bottom, elem_axis, elements - 1), empty], axis=elem_axis)
    return jnp.concatenate([below_layer, values, above_layer], axis=node_axis)

def narrow(extended, node_axis, elem_axis):
    size = extended.shape[node_axis]
    interior = lax.slice_in_dim(extended, 1, size - 1, axis=node_axis)
    lower_rim = leading(extended, node_axis, 1)
    upper_rim = trailing(extended, node_axis, 1)
    elements = extended.shape[elem_axis]
    empty = jnp.zeros_like(trailing(lower_rim, elem_axis, 1))
    add_top = jnp.concatenate([trailing(lower_rim, elem_axis, elements - 1), empty], axis=elem_axis)
    add_bottom = jnp.concatenate([empty, leading(upper_rim, elem_axis, elements - 1)], axis=elem_axis)
    inner_size = interior.shape[node_axis]
    first_layer = leading(interior, node_axis, 1) + add_bottom
    last_layer = trailing(interior, node_axis, 1) + add_top
    middle = lax.slice_in_dim(interior, 1, inner_size - 1, axis=node_axis)
    return jnp.concatenate([first_layer, middle, last_layer], axis=node_axis)

def tables(points):
    order = points + 2
    column = jnp.arange(order).astype(jnp.float32) + 1.0
    sines = jnp.sqrt(2.0 / (order + 1.0)) * jnp.sin(jnp.pi * column[:, None] * column[None, :] / (order + 1.0))
    eigen_values = 2.0 - 2.0 * jnp.cos(jnp.pi * column / (order + 1.0))
    return (sines, eigen_values)

def local_solve(extended, coeffs, mass_grid):
    sines, eigen_values = tables(extended.shape[0] - 2)
    highest = lax.Precision.HIGHEST
    spectral = jnp.einsum('ip,pqrabc->iqrabc', sines, extended, precision=highest)
    spectral = jnp.einsum('jq,iqrabc->ijrabc', sines, spectral, precision=highest)
    spectral = jnp.einsum('kr,ijrabc->ijkabc', sines, spectral, precision=highest)
    lam_i = eigen_values[:, None, None, None, None, None]
    lam_j = eigen_values[None, :, None, None, None, None]
    lam_k = eigen_values[None, None, :, None, None, None]
    denominator = coeffs[0][None, None, None] * lam_i + coeffs[1][None, None, None] * lam_j + coeffs[2][None, None, None] * lam_k + mass_grid[None, None, None]
    spectral = spectral / denominator
    spectral = jnp.einsum('ip,pqrabc->iqrabc', sines, spectral, precision=highest)
    spectral = jnp.einsum('jq,iqrabc->ijrabc', sines, spectral, precision=highest)
    return jnp.einsum('kr,ijrabc->ijkabc', sines, spectral, precision=highest)

def operate(extended, coeffs, mass_grid):
    centre = extended[1:-1, 1:-1, 1:-1]
    lap_x = 2.0 * centre - extended[2:, 1:-1, 1:-1] - extended[:-2, 1:-1, 1:-1]
    lap_y = 2.0 * centre - extended[1:-1, 2:, 1:-1] - extended[1:-1, :-2, 1:-1]
    lap_z = 2.0 * centre - extended[1:-1, 1:-1, 2:] - extended[1:-1, 1:-1, :-2]
    return coeffs[0] * lap_x + coeffs[1] * lap_y + coeffs[2] * lap_z + mass_grid * centre

def extend_all(values):
    return extend_axis(extend_axis(extend_axis(values, 0, 3), 1, 4), 2, 5)

def fold_all(extended):
    return narrow(narrow(narrow(extended, 2, 5), 1, 4), 0, 3)

def reference(right_side, stretch, mass_term, slot_position, coarse_group):
    grid_x = EX * N_SX
    grid_y = EY * N_SY
    element = jnp.arange(ELEMENTS, dtype=jnp.int32)
    device = element // E_DEV
    row_index = device // N_SY
    col_index = device % N_SY
    along_x = slot_position // (EY * EZ)
    along_y = slot_position // EZ % EY
    along_z = slot_position % EZ
    flat_index = (((row_index * EX + along_x) * grid_y + col_index * EY + along_y) * EZ + along_z).astype(jnp.int32)
    grid_shape = (NODES, NODES, NODES, grid_x, grid_y, EZ)
    source = jnp.zeros((NODES, NODES, NODES, ELEMENTS), jnp.float32).at[:, :, :, flat_index].set(right_side).reshape(grid_shape)
    coeffs = jnp.zeros((3, ELEMENTS), jnp.float32).at[:, flat_index].set(stretch).reshape(3, grid_x, grid_y, EZ)
    mass_grid = jnp.zeros((ELEMENTS,), jnp.float32).at[flat_index].set(mass_term).reshape(grid_x, grid_y, EZ)
    solution = jnp.zeros_like(source)
    residual = source
    for sweep in range(SWEEPS):
        correction = fold_all(local_solve(extend_all(residual), coeffs, mass_grid))
        solution = solution + relax_factor * correction
        residual = source - operate(extend_all(solution), coeffs, mass_grid)
    flat_shape = (NODES, NODES, NODES, ELEMENTS)
    smoothed = jnp.take(solution.reshape(flat_shape), flat_index, axis=3)
    fine_residual = jnp.take(residual.reshape(flat_shape), flat_index, axis=3)
    position = jnp.arange(NODES).astype(jnp.float32) / (NODES - 1.0)
    linear_weights = jnp.stack([1.0 - position, position])
    highest = lax.Precision.HIGHEST
    moments = jnp.einsum('xp,yq,zr,pqre->xyze', linear_weights, linear_weights, linear_weights, fine_residual, precision=highest).reshape(8, ELEMENTS)
    coarse_rhs = jax.ops.segment_sum(moments.T, coarse_group, num_segments=GROUPS).T
    return (smoothed, fine_residual, coarse_rhs)
```

```python
import jax
import jax.numpy as jnp
import numpy as np
from jax import lax
from jax.experimental import pallas as pl
from jax.experimental.pallas import tpu as pltpu
from jax.sharding import PartitionSpec as P

NODES = 8
GRP_DEV = 16
LANES = 128
RELAX = 0.35
F32 = jnp.float32
BF16 = jnp.bfloat16


def split_np(a):
    a = np.asarray(a, np.float32)
    hi = np.asarray(jnp.asarray(a).astype(BF16).astype(F32))
    return hi, a - hi


def constants():
    n = NODES + 2
    col = np.arange(n, dtype=np.float64) + 1.0
    s = np.sqrt(2.0 / (n + 1.0)) * np.sin(np.pi * col[:, None] * col[None, :] / (n + 1.0))
    lam = 2.0 - 2.0 * np.cos(np.pi * col / (n + 1.0))
    fwd = np.zeros((104, 112))
    for q in range(n):
        for r in range(n):
            c = q * 8 + r - 1
            if r == 0:
                c = 80 + q
            if r == n - 1:
                c = 96 + q
            fwd[:100, c] = np.outer(s[:, q], s[:, r]).reshape(-1)
    fh, fl = split_np(fwd)
    a1 = np.concatenate([np.concatenate([fh, fh], 1), np.concatenate([fl, fl], 1)], 0)
    bh, bl = split_np(RELAX * fwd.T)
    a2 = np.concatenate([np.concatenate([bh, bh], 1), np.concatenate([bl, bl], 1)], 0)
    lam_j = np.ones((104, LANES), np.float32)
    lam_k = np.ones((104, LANES), np.float32)
    lam_j[:100] = np.repeat(lam, n)[:, None]
    lam_k[:100] = np.tile(lam, n)[:, None]
    t = np.arange(NODES) / (NODES - 1.0)
    w = np.stack([1.0 - t, t])
    wm = np.einsum("ax,by,cz->abcxyz", w, w, w).reshape(8, 512)
    wh, wl = split_np(wm)
    wm = np.concatenate([wh, wl], 0)
    return s, lam, a1, a2, lam_j, lam_k, wm


SINES, LAM, A_FWD, A_BWD, LAM_J, LAM_K, W_MOM = constants()


def split(x):
    hi = x.astype(BF16)
    return hi, (x - hi.astype(F32)).astype(BF16)


def dot(a, b):
    return lax.dot_general(a, b, (((1,), (0,)), ((), ())), preferred_element_type=F32)


def dot_t(a, b):
    return lax.dot_general(a, b, (((1,), (1,)), ((), ())), preferred_element_type=F32)


def flags():
    i = lax.axis_index("sx")
    j = lax.axis_index("sy")
    nx = lax.axis_size("sx")
    ny = lax.axis_size("sy")
    one = lambda c: jnp.where(c, 1.0, 0.0).astype(F32)
    return one(i > 0), one(i < nx - 1), one(j > 0), one(j < ny - 1)


def lane_up(x):
    lane = lax.broadcasted_iota(jnp.int32, x.shape, x.ndim - 1)
    return jnp.where(lane == LANES - 1, 0.0, pltpu.roll(x, LANES - 1, x.ndim - 1))


def lane_down(x):
    lane = lax.broadcasted_iota(jnp.int32, x.shape, x.ndim - 1)
    return jnp.where(lane == 0, 0.0, pltpu.roll(x, 1, x.ndim - 1))


def onehot(slot_row):
    p = lax.broadcasted_iota(jnp.int32, (256, 256), 0)
    return jnp.where(p == slot_row, 1.0, 0.0).astype(BF16)


def place_kernel(rhs_ref, stretch_ref, mass_ref, slot_ref, src_ref, coef_ref, lo_ref, hi_ref):
    oh = onehot(slot_ref[...])
    c = jnp.concatenate([stretch_ref[...], mass_ref[...], jnp.zeros((4, 256), F32)], 0)
    c1, rest = split(c)
    r1 = c - c1.astype(F32)
    c2 = r1.astype(BF16)
    c3 = (r1 - c2.astype(F32)).astype(BF16)
    cg = dot_t(c1, oh) + dot_t(c2, oh) + dot_t(c3, oh)
    coef = jnp.concatenate([cg[0:4, :LANES], cg[0:4, LANES:]], 0)
    coef_ref[...] = coef
    lo_ref[16] = coef
    hi_ref[16] = coef
    for x in range(8):
        a = rhs_ref[x * 64 : (x + 1) * 64, :]
        a1 = a.astype(BF16)
        e = a - a1.astype(F32)
        a2 = e.astype(BF16)
        a3 = (e - a2.astype(F32)).astype(BF16)
        g = dot_t(jnp.concatenate([a1, a2, a3], 0), oh)
        g = g[0:64] + g[64:128] + g[128:192]
        for b in range(2):
            block = g[:, b * LANES : (b + 1) * LANES].reshape(8, 8, LANES)
            src_ref[x, b * 8 : b * 8 + 8] = block
            if x == 0:
                lo_ref[b * 8 : b * 8 + 8] = block
            if x == 7:
                hi_ref[b * 8 : b * 8 + 8] = block


def block_solves(rext, coef_ref, a1_ref, a2_ref, lj_ref, lk_ref, spec, wout):
    for p in range(10):
        base = p * 192
        ends = []
        for z, shift in ((7, lane_down), (0, lane_up)):
            rows = [shift(rext[pl.ds(base + 64 * t + z, 8, stride=8), :]) for t in range(3)]
            ends.append(rows)
        halves = []
        for b in range(2):
            halves.append(
                jnp.concatenate(
                    [rext[base + 64 * b : base + 64 * b + 80, :]]
                    + ends[0][b : b + 2]
                    + ends[1][b : b + 2],
                    0,
                )
            )
        hi, lo = split(jnp.concatenate(halves, 1))
        r = dot(a1_ref[...], jnp.concatenate([hi, lo], 0))
        spec[p] = r[:104] + r[104:]

    even = [i for i in range(0, 10, 2)]
    odd = [i for i in range(1, 10, 2)]
    for b in range(2):
        lanes = slice(b * LANES, (b + 1) * LANES)
        cx, cy, cz, m = [
            jnp.broadcast_to(coef_ref[b * 4 + k : b * 4 + k + 1, :], (8, LANES)) for k in range(4)
        ]

        def chunk(t, carry):
            row = pl.ds(pl.multiple_of(t * 8, 8), 8)
            v = [spec[p, row, lanes] for p in range(10)]
            d0 = cy * lj_ref[row, :] + cz * lk_ref[row, :] + m
            s = [v[p] + v[9 - p] for p in range(5)]
            d = [v[p] - v[9 - p] for p in range(5)]
            z = [None] * 10
            for i in range(10):
                h = s if i % 2 == 0 else d
                acc = h[0] * float(SINES[i, 0])
                for p in range(1, 5):
                    acc = acc + h[p] * float(SINES[i, p])
                z[i] = acc / (d0 + cx * float(LAM[i]))
            for p in range(5):
                e = z[0] * float(SINES[0, p])
                o = z[1] * float(SINES[1, p])
                for i in even[1:]:
                    e = e + z[i] * float(SINES[i, p])
                for i in odd[1:]:
                    o = o + z[i] * float(SINES[i, p])
                spec[p, row, lanes] = e + o
                spec[9 - p, row, lanes] = e - o
            return carry

        lax.fori_loop(0, 13, chunk, 0)

    for p in range(10):
        base = p * 192
        hi, lo = split(spec[p])
        r = dot(a2_ref[...], jnp.concatenate([hi, lo], 0))
        r = r[:112] + r[112:]
        r0 = r[:, :LANES]
        r1 = r[:, LANES:]
        wout[base : base + 64, :] = r0[0:64]
        wout[base + 64 : base + 80, :] = r0[64:80] + r1[0:16]
        wout[base + 80 : base + 144, :] = r1[16:80]
        wout[base + 144 : base + 192, :] = jnp.zeros((48, LANES), F32)
        for off, z, shift in ((80, 7, lane_up), (96, 0, lane_down)):
            rows = [
                r0[off : off + 8],
                r0[off + 8 : off + 16] + r1[off : off + 8],
                r1[off + 8 : off + 16],
            ]
            for t in range(3):
                at = pl.ds(base + 64 * t + z, 8, stride=8)
                wout[at, :] = wout[at, :] + shift(rows[t])


def put(ref, p, y, value):
    n = value.shape[0]
    at = (p * 24 + y) * 8
    ref[at : at + n * 8, :] = value.reshape(n * 8, LANES)


def get(ref, p, y, n):
    at = (p * 24 + y) * 8
    return ref[at : at + n * 8, :].reshape(n, 8, LANES)


def first_kernel(
    src_ref, coef_ref, xl_ref, xr_ref, yd_ref, yu_ref, a1_ref, a2_ref, lj_ref, lk_ref,
    rext_ref, w_ref, to_left_ref, to_right_ref, to_down_ref, to_up_ref, spec, wout,
):
    left, right, down, up = flags()
    zero = jnp.zeros((6, 8, LANES), F32)
    for p in range(10):
        side = {0: left, 9: right}.get(p)
        if p == 0:
            line = xl_ref[0:16] * left
        elif p == 9:
            line = xr_ref[0:16] * right
        else:
            line = src_ref[p - 1]
        fd = down if side is None else down * side
        fu = up if side is None else up * side
        put(rext_ref, p, 0, yd_ref[p : p + 1] * fd)
        put(rext_ref, p, 1, line)
        put(rext_ref, p, 17, yu_ref[p : p + 1] * fu)
        put(rext_ref, p, 18, zero)
    block_solves(rext_ref, coef_ref, a1_ref, a2_ref, lj_ref, lk_ref, spec, wout)
    empty = jnp.zeros((3, 8, LANES), F32)
    to_up_ref[0] = empty
    to_up_ref[11] = empty
    to_down_ref[0] = empty
    to_down_ref[11] = empty
    for p in range(10):
        line = get(wout, p, 0, 18)
        w_ref[p] = line
        if p < 3:
            to_left_ref[p] = line
        if p > 6:
            to_right_ref[p - 7] = line
        side = {0: left, 9: right}.get(p)
        if side is not None:
            line = line * side
        to_down_ref[p + 1] = line[0:3]
        to_up_ref[p + 1] = line[15:18]


def edge_kernel(own_dn_ref, own_up_ref, l_dn_ref, l_up_ref, r_dn_ref, r_up_ref, dn_ref, up_ref):
    left, right, _, _ = flags()
    for own, l, r, out in (
        (own_dn_ref, l_dn_ref, r_dn_ref, dn_ref),
        (own_up_ref, l_up_ref, r_up_ref, up_ref),
    ):
        n = l.shape[0]
        m = own.shape[0]
        out[0:n] = own[0:n] + l[...] * left
        out[n : m - n] = own[n : m - n]
        out[m - n :] = own[m - n :] + r[...] * right


def neighbours_z(u):
    z = lax.broadcasted_iota(jnp.int32, u.shape, 1)
    s = pltpu.roll(u, 7, 1)
    above = jnp.where(z == 7, lane_up(s), s)
    s = pltpu.roll(u, 1, 1)
    below = jnp.where(z == 0, lane_down(s), s)
    return above, below


def second_kernel(
    rext_ref, coef_ref, xl_ref, xr_ref, yd_ref, yu_ref, w_ref, l_ref, r_ref, d_ref, u_ref,
    a1_ref, a2_ref, lj_ref, lk_ref,
    c_ref, to_left_ref, to_right_ref, to_down_ref, to_up_ref, h, cb, r1, spec, wout,
):
    left, right, down, up = flags()
    for x in range(12):
        if x == 0:
            g = l_ref[0] * left
        elif x == 1:
            g = (l_ref[1] + w_ref[0]) * left
        elif x == 2:
            g = l_ref[2] * left + w_ref[1]
        elif x == 9:
            g = w_ref[8] + r_ref[0] * right
        elif x == 10:
            g = (w_ref[9] + r_ref[1]) * right
        elif x == 11:
            g = r_ref[2] * right
        else:
            g = w_ref[x - 1]
        d = d_ref[x] * down
        u = u_ref[x] * up
        h[x, 0] = d[0]
        h[x, 1] = g[0] * down + d[1]
        h[x, 2] = g[1] + d[2]
        h[x, 3:17] = g[2:16]
        h[x, 17] = g[16] + u[0]
        h[x, 18] = g[17] * up + u[1]
        h[x, 19] = u[2]
    for a, own in ((0, xl_ref), (1, None), (2, xr_ref)):
        for b in range(4):
            for k in range(4):
                if b == 0:
                    row = yd_ref[10 + a, 4 + k : 5 + k, :]
                elif b == 3:
                    row = yu_ref[10 + a, k : k + 1, :]
                else:
                    at = (b - 1) * 4 + k
                    row = coef_ref[at : at + 1, :] if own is None else own[16, at : at + 1, :]
                cb[a, b, k] = jnp.broadcast_to(row, (8, LANES))
    zero = jnp.zeros((6, 8, LANES), F32)
    for p in range(10):
        a = 0 if p == 0 else 2 if p == 9 else 1
        for y, n, b in ((0, 1, 0), (1, 4, 1), (5, 4, 1), (9, 4, 2), (13, 4, 2), (17, 1, 3)):
            v = h[p + 1, y + 1 : y + 1 + n]
            above, below = neighbours_z(v)
            two = v + v
            res = get(rext_ref, p, y, n) - (
                cb[a, b, 0] * (two - h[p + 2, y + 1 : y + 1 + n] - h[p, y + 1 : y + 1 + n])
                + cb[a, b, 1] * (two - h[p + 1, y + 2 : y + 2 + n] - h[p + 1, y : y + n])
                + cb[a, b, 2] * (two - above - below)
                + cb[a, b, 3] * v
            )
            if p == 0:
                res = res * left
            if p == 9:
                res = res * right
            if y == 0:
                res = res * down
            if y == 17:
                res = res * up
            put(r1, p, y, res)
        put(r1, p, 18, zero)
    block_solves(r1, coef_ref, a1_ref, a2_ref, lj_ref, lk_ref, spec, wout)
    for p in range(10):
        line = get(wout, p, 0, 18)
        c_ref[p] = h[p + 1, 1:19] + line
        if p < 2:
            to_left_ref[p] = line
        if p > 7:
            to_right_ref[p - 8] = line
        side = {0: left, 9: right}.get(p)
        if side is not None:
            line = line * side
        to_down_ref[p] = line[0:2]
        to_up_ref[p] = line[16:18]


def last_kernel(
    src_ref, coef_ref, c_ref, l_ref, r_ref, d_ref, u_ref, slot_ref, group_ref, wm_ref,
    smooth_ref, res_ref, part_ref, h, mu, mr,
):
    left, right, down, up = flags()
    for p in range(10):
        g = c_ref[p]
        if p == 0:
            g = (g + l_ref[0]) * left
        elif p == 1:
            g = g + l_ref[1] * left
        elif p == 8:
            g = g + r_ref[0] * right
        elif p == 9:
            g = (g + r_ref[1]) * right
        d = d_ref[p] * down
        u = u_ref[p] * up
        h[p, 0] = g[0] * down + d[0]
        h[p, 1] = g[1] + d[1]
        h[p, 2:16] = g[2:16]
        h[p, 16] = g[16] + u[0]
        h[p, 17] = g[17] * up + u[1]
    for b in range(2):
        lanes = slice(b * LANES, (b + 1) * LANES)
        cf = [
            jnp.broadcast_to(coef_ref[b * 4 + k : b * 4 + k + 1, :], (8, LANES)) for k in range(4)
        ]
        for x in range(8):
            p = x + 1
            for y in (0, 4):
                yy = b * 8 + y + 1
                v = h[p, yy : yy + 4]
                above, below = neighbours_z(v)
                two = v + v
                res = src_ref[x, yy - 1 : yy + 3] - (
                    cf[0] * (two - h[p + 1, yy : yy + 4] - h[p - 1, yy : yy + 4])
                    + cf[1] * (two - h[p, yy + 1 : yy + 5] - h[p, yy - 1 : yy + 3])
                    + cf[2] * (two - above - below)
                    + cf[3] * v
                )
                at = (x * 8 + y) * 8
                mu[at : at + 32, lanes] = v.reshape(32, LANES)
                mr[at : at + 32, lanes] = res.reshape(32, LANES)
    oh = onehot(slot_ref[...])
    mom = jnp.zeros((16, 256), F32)
    for x in range(8):
        at = slice(x * 64, x * 64 + 64)
        uh, ul = split(mu[at, :])
        rh, rl = split(mr[at, :])
        o = dot(jnp.concatenate([uh, ul, rh, rl], 0), oh)
        smooth_ref[at, :] = o[0:64] + o[64:128]
        res_ref[at, :] = o[128:192] + o[192:256]
    for x in range(4):
        at = slice(x * 128, x * 128 + 128)
        rh, rl = split(mr[at, :])
        mom = mom + dot(wm_ref[:, at], rh) + dot(wm_ref[:, at], rl)
    mh, ml = split(mom[0:8] + mom[8:16])
    mom = dot(mh, oh) + dot(ml, oh)
    ny = part_ref.shape[0]
    col = group_ref[...] - lax.axis_index("sx") * (ny * GRP_DEV)
    owner = lax.shift_right_logical(col, 4)
    member = jnp.bitwise_and(col, 15)
    sel = lax.broadcasted_iota(jnp.int32, (ny, 256), 0)
    pick = jnp.where(sel == owner, 1.0, 0.0).astype(BF16)
    m16 = lax.broadcasted_iota(jnp.int32, (16, 256), 0) == member
    spread = jnp.concatenate(
        [jnp.where(m16, jnp.broadcast_to(mom[v : v + 1], (16, 256)), 0.0) for v in range(8)], 0
    )
    sh, sl = split(spread)
    part_ref[...] = dot_t(pick, sh) + dot_t(pick, sl)


def sd(*shape):
    return jax.ShapeDtypeStruct(shape, F32)


def ring(value, axis, by):
    n = lax.axis_size(axis)
    return lax.ppermute(value, axis, [(i, (i + by) % n) for i in range(n)])


def call(kernel, outs, scratch=(), **kw):
    return pl.pallas_call(
        kernel,
        out_shape=outs,
        scratch_shapes=[pltpu.VMEM(s, F32) for s in scratch],
        **kw,
    )


def edges(own_dn, own_up, from_left, from_right, first, last, layers):
    rows = own_dn.shape[0]
    n = last - first
    full = pl.BlockSpec((rows, layers, 8, LANES), lambda i: (0, 0, 0, 0))
    top = 18 // layers - 1
    lo = pl.BlockSpec((n, layers, 8, LANES), lambda i: (0, 0, 0, 0))
    hi = pl.BlockSpec((n, layers, 8, LANES), lambda i: (0, top, 0, 0))
    return pl.pallas_call(
        edge_kernel,
        grid=(1,),
        in_specs=[full, full, lo, hi, lo, hi],
        out_specs=[full, full],
        out_shape=[sd(rows, layers, 8, LANES)] * 2,
    )(own_dn, own_up, from_left, from_left, from_right, from_right)


def on_device(right_side, stretch, mass_term, slot_position, coarse_group):
    a1 = jnp.asarray(A_FWD, BF16)
    a2 = jnp.asarray(A_BWD, BF16)
    lj = jnp.asarray(LAM_J, F32)
    lk = jnp.asarray(LAM_K, F32)
    wm = jnp.asarray(W_MOM, BF16)
    slot = slot_position.reshape(1, 256)
    src, coef, lo, hi = call(
        place_kernel, [sd(8, 16, 8, LANES), sd(8, LANES), sd(17, 8, LANES), sd(17, 8, LANES)]
    )(right_side.reshape(512, 256), stretch, mass_term.reshape(1, 256), slot)
    xl = ring(hi, "sx", 1)
    xr = ring(lo, "sx", -1)
    c3 = coef[None]
    to_up = jnp.concatenate([xl[15:16], src[:, 15], xr[15:16], xl[16:17], c3, xr[16:17]], 0)
    to_dn = jnp.concatenate([xl[0:1], src[:, 0], xr[0:1], xl[16:17], c3, xr[16:17]], 0)
    yd = ring(to_up, "sy", 1)
    yu = ring(to_dn, "sy", -1)

    slab = sd(3, 18, 8, LANES)
    side = sd(12, 3, 8, LANES)
    rext, w, to_l, to_r, to_d, to_u = call(
        first_kernel,
        [sd(1920, LANES), sd(10, 18, 8, LANES), slab, slab, side, side],
        [(10, 104, 256), (1920, LANES)],
    )(src, coef, xl, xr, yd, yu, a1, a2, lj, lk)
    fl = ring(to_r, "sx", 1)
    fr = ring(to_l, "sx", -1)
    to_d, to_u = edges(to_d, to_u, fl, fr, 0, 3, 3)
    fd = ring(to_u, "sy", 1)
    fu = ring(to_d, "sy", -1)

    slab = sd(2, 18, 8, LANES)
    side = sd(10, 2, 8, LANES)
    c, to_l, to_r, to_d, to_u = call(
        second_kernel,
        [sd(10, 18, 8, LANES), slab, slab, side, side],
        [(12, 20, 8, LANES), (3, 4, 4, 8, LANES), (1920, LANES), (10, 104, 256), (1920, LANES)],
    )(rext, coef, xl, xr, yd, yu, w, fl, fr, fd, fu, a1, a2, lj, lk)
    fl = ring(to_r, "sx", 1)
    fr = ring(to_l, "sx", -1)
    to_d, to_u = edges(to_d, to_u, fl, fr, 0, 2, 2)
    fd = ring(to_u, "sy", 1)
    fu = ring(to_d, "sy", -1)

    ny = lax.axis_size("sy")
    smooth, res, part = call(
        last_kernel,
        [sd(512, 256), sd(512, 256), sd(ny, LANES)],
        [(10, 18, 8, LANES), (512, 256), (512, 256)],
    )(src, coef, c, fl, fr, fd, fu, slot, coarse_group.reshape(1, 256), wm)
    arrived = lax.all_to_all(part, "sy", split_axis=0, concat_axis=0, tiled=True)
    coarse = arrived.sum(axis=0).reshape(8, GRP_DEV)
    return smooth.reshape(8, 8, 8, 256), res.reshape(8, 8, 8, 256), coarse


def solution(mesh):
    split_all = P(None, None, None, ("sx", "sy"))
    flat = P(("sx", "sy"))
    return jax.shard_map(
        on_device,
        mesh=mesh,
        in_specs=(split_all, P(None, ("sx", "sy")), flat, flat, flat),
        out_specs=(split_all, split_all, P(None, ("sx", "sy"))),
        check_vma=False,
    )
```

```python
import jax
import jax.numpy as jnp
import numpy as np
from jax import lax
from jax.experimental import pallas as pl
from jax.experimental.pallas import tpu as pltpu
from jax.sharding import PartitionSpec as P

NODES = 8
GRP_DEV = 16
LANES = 128
RELAX = 0.35
F32 = jnp.float32
BF16 = jnp.bfloat16


def split_np(a):
    a = np.asarray(a, np.float32)
    hi = np.asarray(jnp.asarray(a).astype(BF16).astype(F32))
    return hi, a - hi


def constants():
    n = NODES + 2
    col = np.arange(n, dtype=np.float64) + 1.0
    s = np.sqrt(2.0 / (n + 1.0)) * np.sin(np.pi * col[:, None] * col[None, :] / (n + 1.0))
    lam = 2.0 - 2.0 * np.cos(np.pi * col / (n + 1.0))
    fwd = np.zeros((104, 112))
    for q in range(n):
        for r in range(n):
            c = q * 8 + r - 1
            if r == 0:
                c = 80 + q
            if r == n - 1:
                c = 96 + q
            fwd[:100, c] = np.outer(s[:, q], s[:, r]).reshape(-1)
    fh, fl = split_np(fwd)
    a1 = np.concatenate([np.concatenate([fh, fh], 1), np.concatenate([fl, fl], 1)], 0)
    bh, bl = split_np(RELAX * fwd.T)
    a2 = np.concatenate([np.concatenate([bh, bh], 1), np.concatenate([bl, bl], 1)], 0)
    lam_j = np.ones((104, LANES), np.float32)
    lam_k = np.ones((104, LANES), np.float32)
    lam_j[:100] = np.repeat(lam, n)[:, None]
    lam_k[:100] = np.tile(lam, n)[:, None]
    t = np.arange(NODES) / (NODES - 1.0)
    w = np.stack([1.0 - t, t])
    wm = np.einsum("ax,by,cz->abcxyz", w, w, w).reshape(8, 512)
    wh, wl = split_np(wm)
    wm = np.concatenate([wh, wl], 0)
    return s, lam, a1, a2, lam_j, lam_k, wm


SINES, LAM, A_FWD, A_BWD, LAM_J, LAM_K, W_MOM = constants()


def split(x):
    hi = x.astype(BF16)
    return hi, (x - hi.astype(F32)).astype(BF16)


def dot(a, b):
    return lax.dot_general(a, b, (((1,), (0,)), ((), ())), preferred_element_type=F32)


def dot_t(a, b):
    return lax.dot_general(a, b, (((1,), (1,)), ((), ())), preferred_element_type=F32)


def flags():
    i = lax.axis_index("sx")
    j = lax.axis_index("sy")
    nx = lax.axis_size("sx")
    ny = lax.axis_size("sy")
    one = lambda c: jnp.where(c, 1.0, 0.0).astype(F32)
    return one(i > 0), one(i < nx - 1), one(j > 0), one(j < ny - 1)


def lane_up(x):
    lane = lax.broadcasted_iota(jnp.int32, x.shape, x.ndim - 1)
    return jnp.where(lane == LANES - 1, 0.0, pltpu.roll(x, LANES - 1, x.ndim - 1))


def lane_down(x):
    lane = lax.broadcasted_iota(jnp.int32, x.shape, x.ndim - 1)
    return jnp.where(lane == 0, 0.0, pltpu.roll(x, 1, x.ndim - 1))


def onehot(slot_row):
    p = lax.broadcasted_iota(jnp.int32, (256, 256), 0)
    return jnp.where(p == slot_row, 1.0, 0.0).astype(BF16)


def place_kernel(rhs_ref, stretch_ref, mass_ref, slot_ref, src_ref, coef_ref, lo_ref, hi_ref):
    oh = onehot(slot_ref[...])
    c = jnp.concatenate([stretch_ref[...], mass_ref[...], jnp.zeros((4, 256), F32)], 0)
    c1, rest = split(c)
    r1 = c - c1.astype(F32)
    c2 = r1.astype(BF16)
    c3 = (r1 - c2.astype(F32)).astype(BF16)
    cg = dot_t(c1, oh) + dot_t(c2, oh) + dot_t(c3, oh)
    coef = jnp.concatenate([cg[0:4, :LANES], cg[0:4, LANES:]], 0)
    coef_ref[...] = coef
    lo_ref[16] = coef
    hi_ref[16] = coef
    for x in range(8):
        a = rhs_ref[x * 64 : (x + 1) * 64, :]
        a1 = a.astype(BF16)
        e = a - a1.astype(F32)
        a2 = e.astype(BF16)
        a3 = (e - a2.astype(F32)).astype(BF16)
        g = dot_t(jnp.concatenate([a1, a2, a3], 0), oh)
        g = g[0:64] + g[64:128] + g[128:192]
        for b in range(2):
            block = g[:, b * LANES : (b + 1) * LANES].reshape(8, 8, LANES)
            src_ref[x, b * 8 : b * 8 + 8] = block
            if x == 0:
                lo_ref[b * 8 : b * 8 + 8] = block
            if x == 7:
                hi_ref[b * 8 : b * 8 + 8] = block


def block_solves(rext, coef_ref, a1_ref, a2_ref, lj_ref, lk_ref, spec, wout):
    for p in range(10):
        base = p * 192
        ends = []
        for z, shift in ((7, lane_down), (0, lane_up)):
            rows = [shift(rext[pl.ds(base + 64 * t + z, 8, stride=8), :]) for t in range(3)]
            ends.append(rows)
        halves = []
        for b in range(2):
            halves.append(
                jnp.concatenate(
                    [rext[base + 64 * b : base + 64 * b + 80, :]]
                    + ends[0][b : b + 2]
                    + ends[1][b : b + 2],
                    0,
                )
            )
        hi, lo = split(jnp.concatenate(halves, 1))
        r = dot(a1_ref[...], jnp.concatenate([hi, lo], 0))
        spec[p] = r[:104] + r[104:]

    even = [i for i in range(0, 10, 2)]
    odd = [i for i in range(1, 10, 2)]
    for b in range(2):
        lanes = slice(b * LANES, (b + 1) * LANES)
        cx, cy, cz, m = [
            jnp.broadcast_to(coef_ref[b * 4 + k : b * 4 + k + 1, :], (8, LANES)) for k in range(4)
        ]

        def chunk(t, carry):
            row = pl.ds(pl.multiple_of(t * 8, 8), 8)
            v = [spec[p, row, lanes] for p in range(10)]
            d0 = cy * lj_ref[row, :] + cz * lk_ref[row, :] + m
            s = [v[p] + v[9 - p] for p in range(5)]
            d = [v[p] - v[9 - p] for p in range(5)]
            z = [None] * 10
            for i in range(10):
                h = s if i % 2 == 0 else d
                acc = h[0] * float(SINES[i, 0])
                for p in range(1, 5):
                    acc = acc + h[p] * float(SINES[i, p])
                z[i] = acc / (d0 + cx * float(LAM[i]))
            for p in range(5):
                e = z[0] * float(SINES[0, p])
                o = z[1] * float(SINES[1, p])
                for i in even[1:]:
                    e = e + z[i] * float(SINES[i, p])
                for i in odd[1:]:
                    o = o + z[i] * float(SINES[i, p])
                spec[p, row, lanes] = e + o
                spec[9 - p, row, lanes] = e - o
            return carry

        lax.fori_loop(0, 13, chunk, 0)

    for p in range(10):
        base = p * 192
        hi, lo = split(spec[p])
        r = dot(a2_ref[...], jnp.concatenate([hi, lo], 0))
        r = r[:112] + r[112:]
        r0 = r[:, :LANES]
        r1 = r[:, LANES:]
        wout[base : base + 64, :] = r0[0:64]
        wout[base + 64 : base + 80, :] = r0[64:80] + r1[0:16]
        wout[base + 80 : base + 144, :] = r1[16:80]
        wout[base + 144 : base + 192, :] = jnp.zeros((48, LANES), F32)
        for off, z, shift in ((80, 7, lane_up), (96, 0, lane_down)):
            rows = [
                r0[off : off + 8],
                r0[off + 8 : off + 16] + r1[off : off + 8],
                r1[off + 8 : off + 16],
            ]
            for t in range(3):
                at = pl.ds(base + 64 * t + z, 8, stride=8)
                wout[at, :] = wout[at, :] + shift(rows[t])


def put(ref, p, y, value):
    n = value.shape[0]
    at = (p * 24 + y) * 8
    ref[at : at + n * 8, :] = value.reshape(n * 8, LANES)


def get(ref, p, y, n):
    at = (p * 24 + y) * 8
    return ref[at : at + n * 8, :].reshape(n, 8, LANES)


def first_kernel(
    src_ref, coef_ref, xl_ref, xr_ref, yd_ref, yu_ref, a1_ref, a2_ref, lj_ref, lk_ref,
    rext_ref, w_ref, to_left_ref, to_right_ref, to_down_ref, to_up_ref, spec, wout,
):
    left, right, down, up = flags()
    zero = jnp.zeros((6, 8, LANES), F32)
    for p in range(10):
        side = {0: left, 9: right}.get(p)
        if p == 0:
            line = xl_ref[0:16] * left
        elif p == 9:
            line = xr_ref[0:16] * right
        else:
            line = src_ref[p - 1]
        fd = down if side is None else down * side
        fu = up if side is None else up * side
        put(rext_ref, p, 0, yd_ref[p : p + 1] * fd)
        put(rext_ref, p, 1, line)
        put(rext_ref, p, 17, yu_ref[p : p + 1] * fu)
        put(rext_ref, p, 18, zero)
    block_solves(rext_ref, coef_ref, a1_ref, a2_ref, lj_ref, lk_ref, spec, wout)
    empty = jnp.zeros((3, 8, LANES), F32)
    to_up_ref[0] = empty
    to_up_ref[11] = empty
    to_down_ref[0] = empty
    to_down_ref[11] = empty
    for p in range(10):
        line = get(wout, p, 0, 18)
        w_ref[p] = line
        if p < 3:
            to_left_ref[p] = line
        if p > 6:
            to_right_ref[p - 7] = line
        side = {0: left, 9: right}.get(p)
        if side is not None:
            line = line * side
        to_down_ref[p + 1] = line[0:3]
        to_up_ref[p + 1] = line[15:18]


def edge_kernel(own_dn_ref, own_up_ref, l_ref, r_ref, dn_ref, up_ref):
    left, right, _, _ = flags()
    n = l_ref.shape[0]
    m = own_dn_ref.shape[0]
    for own, y, out in ((own_dn_ref, 0, dn_ref), (own_up_ref, 18 - n, up_ref)):
        out[0:n] = own[0:n] + l_ref[:, y : y + n] * left
        out[n : m - n] = own[n : m - n]
        out[m - n :] = own[m - n :] + r_ref[:, y : y + n] * right


def neighbours_z(u):
    z = lax.broadcasted_iota(jnp.int32, u.shape, 1)
    s = pltpu.roll(u, 7, 1)
    above = jnp.where(z == 7, lane_up(s), s)
    s = pltpu.roll(u, 1, 1)
    below = jnp.where(z == 0, lane_down(s), s)
    return above, below


def second_kernel(
    rext_ref, coef_ref, xl_ref, xr_ref, yd_ref, yu_ref, w_ref, l_ref, r_ref, d_ref, u_ref,
    a1_ref, a2_ref, lj_ref, lk_ref,
    c_ref, to_left_ref, to_right_ref, to_down_ref, to_up_ref, h, cb, r1, spec, wout,
):
    left, right, down, up = flags()
    for x in range(12):
        if x == 0:
            g = l_ref[0] * left
        elif x == 1:
            g = (l_ref[1] + w_ref[0]) * left
        elif x == 2:
            g = l_ref[2] * left + w_ref[1]
        elif x == 9:
            g = w_ref[8] + r_ref[0] * right
        elif x == 10:
            g = (w_ref[9] + r_ref[1]) * right
        elif x == 11:
            g = r_ref[2] * right
        else:
            g = w_ref[x - 1]
        d = d_ref[x] * down
        u = u_ref[x] * up
        h[x, 0] = d[0]
        h[x, 1] = g[0] * down + d[1]
        h[x, 2] = g[1] + d[2]
        h[x, 3:17] = g[2:16]
        h[x, 17] = g[16] + u[0]
        h[x, 18] = g[17] * up + u[1]
        h[x, 19] = u[2]
    for a, own in ((0, xl_ref), (1, None), (2, xr_ref)):
        for b in range(4):
            for k in range(4):
                if b == 0:
                    row = yd_ref[10 + a, 4 + k : 5 + k, :]
                elif b == 3:
                    row = yu_ref[10 + a, k : k + 1, :]
                else:
                    at = (b - 1) * 4 + k
                    row = coef_ref[at : at + 1, :] if own is None else own[16, at : at + 1, :]
                cb[a, b, k] = jnp.broadcast_to(row, (8, LANES))
    zero = jnp.zeros((6, 8, LANES), F32)
    for p in range(10):
        a = 0 if p == 0 else 2 if p == 9 else 1
        for y, n, b in ((0, 1, 0), (1, 4, 1), (5, 4, 1), (9, 4, 2), (13, 4, 2), (17, 1, 3)):
            v = h[p + 1, y + 1 : y + 1 + n]
            above, below = neighbours_z(v)
            two = v + v
            res = get(rext_ref, p, y, n) - (
                cb[a, b, 0] * (two - h[p + 2, y + 1 : y + 1 + n] - h[p, y + 1 : y + 1 + n])
                + cb[a, b, 1] * (two - h[p + 1, y + 2 : y + 2 + n] - h[p + 1, y : y + n])
                + cb[a, b, 2] * (two - above - below)
                + cb[a, b, 3] * v
            )
            if p == 0:
                res = res * left
            if p == 9:
                res = res * right
            if y == 0:
                res = res * down
            if y == 17:
                res = res * up
            put(r1, p, y, res)
        put(r1, p, 18, zero)
    block_solves(r1, coef_ref, a1_ref, a2_ref, lj_ref, lk_ref, spec, wout)
    for p in range(10):
        line = get(wout, p, 0, 18)
        c_ref[p] = h[p + 1, 1:19] + line
        if p < 2:
            to_left_ref[p] = line
        if p > 7:
            to_right_ref[p - 8] = line
        side = {0: left, 9: right}.get(p)
        if side is not None:
            line = line * side
        to_down_ref[p] = line[0:2]
        to_up_ref[p] = line[16:18]


def last_kernel(
    src_ref, coef_ref, c_ref, l_ref, r_ref, d_ref, u_ref, slot_ref, group_ref, wm_ref,
    smooth_ref, res_ref, part_ref, h, mu, mr,
):
    left, right, down, up = flags()
    for p in range(10):
        g = c_ref[p]
        if p == 0:
            g = (g + l_ref[0]) * left
        elif p == 1:
            g = g + l_ref[1] * left
        elif p == 8:
            g = g + r_ref[0] * right
        elif p == 9:
            g = (g + r_ref[1]) * right
        d = d_ref[p] * down
        u = u_ref[p] * up
        h[p, 0] = g[0] * down + d[0]
        h[p, 1] = g[1] + d[1]
        h[p, 2:16] = g[2:16]
        h[p, 16] = g[16] + u[0]
        h[p, 17] = g[17] * up + u[1]
    for b in range(2):
        lanes = slice(b * LANES, (b + 1) * LANES)
        cf = [
            jnp.broadcast_to(coef_ref[b * 4 + k : b * 4 + k + 1, :], (8, LANES)) for k in range(4)
        ]
        for x in range(8):
            p = x + 1
            for y in (0, 4):
                yy = b * 8 + y + 1
                v = h[p, yy : yy + 4]
                above, below = neighbours_z(v)
                two = v + v
                res = src_ref[x, yy - 1 : yy + 3] - (
                    cf[0] * (two - h[p + 1, yy : yy + 4] - h[p - 1, yy : yy + 4])
                    + cf[1] * (two - h[p, yy + 1 : yy + 5] - h[p, yy - 1 : yy + 3])
                    + cf[2] * (two - above - below)
                    + cf[3] * v
                )
                at = (x * 8 + y) * 8
                mu[at : at + 32, lanes] = v.reshape(32, LANES)
                mr[at : at + 32, lanes] = res.reshape(32, LANES)
    oh = onehot(slot_ref[...])
    mom = jnp.zeros((16, 256), F32)
    for x in range(8):
        at = slice(x * 64, x * 64 + 64)
        uh, ul = split(mu[at, :])
        rh, rl = split(mr[at, :])
        o = dot(jnp.concatenate([uh, ul, rh, rl], 0), oh)
        smooth_ref[at, :] = o[0:64] + o[64:128]
        res_ref[at, :] = o[128:192] + o[192:256]
    for x in range(4):
        at = slice(x * 128, x * 128 + 128)
        rh, rl = split(mr[at, :])
        mom = mom + dot(wm_ref[:, at], rh) + dot(wm_ref[:, at], rl)
    mh, ml = split(mom[0:8] + mom[8:16])
    mom = dot(mh, oh) + dot(ml, oh)
    ny = part_ref.shape[0]
    col = group_ref[...] - lax.axis_index("sx") * (ny * GRP_DEV)
    owner = lax.shift_right_logical(col, 4)
    member = jnp.bitwise_and(col, 15)
    sel = lax.broadcasted_iota(jnp.int32, (ny, 256), 0)
    pick = jnp.where(sel == owner, 1.0, 0.0).astype(BF16)
    m16 = lax.broadcasted_iota(jnp.int32, (16, 256), 0) == member
    spread = jnp.concatenate(
        [jnp.where(m16, jnp.broadcast_to(mom[v : v + 1], (16, 256)), 0.0) for v in range(8)], 0
    )
    sh, sl = split(spread)
    part_ref[...] = dot_t(pick, sh) + dot_t(pick, sl)


def sd(*shape):
    return jax.ShapeDtypeStruct(shape, F32)


def vm(*shape):
    return pltpu.VMEM(shape, F32)


def ring(value, axis, by):
    n = lax.axis_size(axis)
    return lax.ppermute(value, axis, [(i, (i + by) % n) for i in range(n)])


def mark(args):
    return [a if isinstance(a, tuple) else (a, False) for a in args]


def call(kernel, outs, scratch=(), **kw):
    vmem = pl.BlockSpec(memory_space=pltpu.VMEM)

    def run(*args):
        args = [a if at_home else pltpu.with_memory_space_constraint(a, pltpu.VMEM) for a, at_home in mark(args)]
        return pl.pallas_call(
            kernel,
            out_shape=outs,
            in_specs=[vmem] * len(args),
            out_specs=[vmem] * len(outs),
            scratch_shapes=[pltpu.VMEM(s, F32) for s in scratch],
            compiler_params=pltpu.CompilerParams(vmem_limit_bytes=16 << 20),
            **kw,
        )(*args)

    return run


def edges(own_dn, own_up, from_left, from_right):
    return call(edge_kernel, [vm(*own_dn.shape)] * 2)(own_dn, own_up, from_left, from_right)


def on_device(right_side, stretch, mass_term, slot_position, coarse_group):
    a1 = jnp.asarray(A_FWD, BF16)
    a2 = jnp.asarray(A_BWD, BF16)
    lj = jnp.asarray(LAM_J, F32)
    lk = jnp.asarray(LAM_K, F32)
    wm = jnp.asarray(W_MOM, BF16)
    slot = slot_position.reshape(1, 256)
    src, coef, lo, hi = call(
        place_kernel, [vm(8, 16, 8, LANES), vm(8, LANES), vm(17, 8, LANES), vm(17, 8, LANES)]
    )((right_side.reshape(512, 256), True), (stretch, True), (mass_term.reshape(1, 256), True), (slot, True))
    xl = ring(hi, "sx", 1)
    xr = ring(lo, "sx", -1)
    c3 = coef[None]
    to_up = jnp.concatenate([xl[15:16], src[:, 15], xr[15:16], xl[16:17], c3, xr[16:17]], 0)
    to_dn = jnp.concatenate([xl[0:1], src[:, 0], xr[0:1], xl[16:17], c3, xr[16:17]], 0)
    yd = ring(to_up, "sy", 1)
    yu = ring(to_dn, "sy", -1)

    slab = vm(3, 18, 8, LANES)
    side = vm(12, 3, 8, LANES)
    rext, w, to_l, to_r, to_d, to_u = call(
        first_kernel,
        [vm(1920, LANES), vm(10, 18, 8, LANES), slab, slab, side, side],
        [(10, 104, 256), (1920, LANES)],
    )(src, coef, xl, xr, yd, yu, a1, a2, lj, lk)
    fl = ring(to_r, "sx", 1)
    fr = ring(to_l, "sx", -1)
    to_d, to_u = edges(to_d, to_u, fl, fr)
    fd = ring(to_u, "sy", 1)
    fu = ring(to_d, "sy", -1)

    slab = vm(2, 18, 8, LANES)
    side = vm(10, 2, 8, LANES)
    c, to_l, to_r, to_d, to_u = call(
        second_kernel,
        [vm(10, 18, 8, LANES), slab, slab, side, side],
        [(12, 20, 8, LANES), (3, 4, 4, 8, LANES), (1920, LANES), (10, 104, 256), (1920, LANES)],
    )(rext, coef, xl, xr, yd, yu, w, fl, fr, fd, fu, a1, a2, lj, lk)
    fl = ring(to_r, "sx", 1)
    fr = ring(to_l, "sx", -1)
    to_d, to_u = edges(to_d, to_u, fl, fr)
    fd = ring(to_u, "sy", 1)
    fu = ring(to_d, "sy", -1)

    ny = lax.axis_size("sy")
    smooth, res, part = call(
        last_kernel,
        [sd(512, 256), sd(512, 256), vm(ny, LANES)],
        [(10, 18, 8, LANES), (512, 256), (512, 256)],
    )(src, coef, c, fl, fr, fd, fu, (slot, True), (coarse_group.reshape(1, 256), True), wm)
    arrived = lax.all_to_all(part, "sy", split_axis=0, concat_axis=0, tiled=True)
    coarse = arrived.sum(axis=0).reshape(8, GRP_DEV)
    return smooth.reshape(8, 8, 8, 256), res.reshape(8, 8, 8, 256), coarse


def solution(mesh):
    split_all = P(None, None, None, ("sx", "sy"))
    flat = P(("sx", "sy"))
    return jax.shard_map(
        on_device,
        mesh=mesh,
        in_specs=(split_all, P(None, ("sx", "sy")), flat, flat, flat),
        out_specs=(split_all, split_all, P(None, ("sx", "sy"))),
        check_vma=False,
    )
```

```python
import jax
import jax.numpy as jnp
import numpy as np
from jax import lax
from jax.experimental import pallas as pl
from jax.experimental.pallas import tpu as pltpu
from jax.sharding import PartitionSpec as P

NODES = 8
GRP_DEV = 16
LANES = 128
RELAX = 0.35
F32 = jnp.float32
BF16 = jnp.bfloat16


def split_np(a):
    a = np.asarray(a, np.float32)
    hi = np.asarray(jnp.asarray(a).astype(BF16).astype(F32))
    return hi, a - hi


def constants():
    n = NODES + 2
    col = np.arange(n, dtype=np.float64) + 1.0
    s = np.sqrt(2.0 / (n + 1.0)) * np.sin(np.pi * col[:, None] * col[None, :] / (n + 1.0))
    lam = 2.0 - 2.0 * np.cos(np.pi * col / (n + 1.0))
    fwd = np.zeros((104, 112))
    for q in range(n):
        for r in range(n):
            c = q * 8 + r - 1
            if r == 0:
                c = 80 + q
            if r == n - 1:
                c = 96 + q
            fwd[:100, c] = np.outer(s[:, q], s[:, r]).reshape(-1)
    fh, fl = split_np(fwd)
    a1 = np.concatenate([np.concatenate([fh, fh], 1), np.concatenate([fl, fl], 1)], 0)
    bh, bl = split_np(RELAX * fwd.T)
    a2 = np.concatenate([np.concatenate([bh, bh], 1), np.concatenate([bl, bl], 1)], 0)
    lam_j = np.ones((104, LANES), np.float32)
    lam_k = np.ones((104, LANES), np.float32)
    lam_j[:100] = np.repeat(lam, n)[:, None]
    lam_k[:100] = np.tile(lam, n)[:, None]
    t = np.arange(NODES) / (NODES - 1.0)
    w = np.stack([1.0 - t, t])
    wm = np.einsum("ax,by,cz->abcxyz", w, w, w).reshape(8, 512)
    wh, wl = split_np(wm)
    wm = np.concatenate([wh, wl], 0)
    return s, lam, a1, a2, lam_j, lam_k, wm


SINES, LAM, A_FWD, A_BWD, LAM_J, LAM_K, W_MOM = constants()


def split(x):
    hi = x.astype(BF16)
    return hi, (x - hi.astype(F32)).astype(BF16)


def dot(a, b):
    return lax.dot_general(a, b, (((1,), (0,)), ((), ())), preferred_element_type=F32)


def dot_t(a, b):
    return lax.dot_general(a, b, (((1,), (1,)), ((), ())), preferred_element_type=F32)


def flags():
    i = lax.axis_index("sx")
    j = lax.axis_index("sy")
    nx = lax.axis_size("sx")
    ny = lax.axis_size("sy")
    one = lambda c: jnp.where(c, 1.0, 0.0).astype(F32)
    return one(i > 0), one(i < nx - 1), one(j > 0), one(j < ny - 1)


def lane_up(x):
    lane = lax.broadcasted_iota(jnp.int32, x.shape, x.ndim - 1)
    return jnp.where(lane == LANES - 1, 0.0, pltpu.roll(x, LANES - 1, x.ndim - 1))


def lane_down(x):
    lane = lax.broadcasted_iota(jnp.int32, x.shape, x.ndim - 1)
    return jnp.where(lane == 0, 0.0, pltpu.roll(x, 1, x.ndim - 1))


def onehot(slot_row):
    p = lax.broadcasted_iota(jnp.int32, (256, 256), 0)
    return jnp.where(p == slot_row, 1.0, 0.0).astype(BF16)


def place_kernel(
    rhs_hbm, stretch_hbm, mass_hbm, slot_hbm, group_hbm,
    src_ref, coef_ref, to_down_ref, to_up_ref, slot_ref, group_ref,
    rhs_ref, stretch_ref, mass_ref, sems,
):
    small = [
        pltpu.make_async_copy(h, v, sems.at[8 + k])
        for k, (h, v) in enumerate(
            (
                (slot_hbm, slot_ref),
                (stretch_hbm, stretch_ref),
                (mass_hbm, mass_ref),
                (group_hbm, group_ref),
            )
        )
    ]
    big = [
        pltpu.make_async_copy(
            rhs_hbm.at[pl.ds(x * 64, 64), :], rhs_ref.at[pl.ds(x * 64, 64), :], sems.at[x]
        )
        for x in range(8)
    ]
    for c in small + big:
        c.start()
    small[0].wait()
    oh = onehot(slot_ref[...])
    small[1].wait()
    small[2].wait()
    c = jnp.concatenate([stretch_ref[...], mass_ref[...], jnp.zeros((4, 256), F32)], 0)
    c1 = c.astype(BF16)
    r1 = c - c1.astype(F32)
    c2 = r1.astype(BF16)
    c3 = (r1 - c2.astype(F32)).astype(BF16)
    cg = dot_t(c1, oh) + dot_t(c2, oh) + dot_t(c3, oh)
    coef = jnp.concatenate([cg[0:4, :LANES], cg[0:4, LANES:]], 0)
    coef_ref[...] = coef
    to_down_ref[8] = coef
    to_up_ref[8] = coef
    for x in range(8):
        big[x].wait()
        a = rhs_ref[x * 64 : (x + 1) * 64, :]
        a1 = a.astype(BF16)
        e = a - a1.astype(F32)
        a2 = e.astype(BF16)
        a3 = (e - a2.astype(F32)).astype(BF16)
        g = dot_t(jnp.concatenate([a1, a2, a3], 0), oh)
        g = g[0:64] + g[64:128] + g[128:192]
        for b in range(2):
            block = g[:, b * LANES : (b + 1) * LANES].reshape(8, 8, LANES)
            src_ref[x, b * 8 : b * 8 + 8] = block
            if b == 0:
                to_down_ref[x] = block[0]
            else:
                to_up_ref[x] = block[7]
    small[3].wait()


def rim_kernel(src_ref, coef_ref, yd_ref, yu_ref, to_left_ref, to_right_ref):
    coef_y = jnp.concatenate([yd_ref[8, 4:8, :], yu_ref[8, 0:4, :]], 0)
    for x, out in ((0, to_left_ref), (7, to_right_ref)):
        out[0] = yd_ref[x]
        out[1:17] = src_ref[x]
        out[17] = yu_ref[x]
        out[18] = coef_ref[...]
        out[19] = coef_y


def block_solves(rext, coef_ref, a1_ref, a2_ref, lj_ref, lk_ref, spec, wout):
    for p in range(10):
        base = p * 192
        ends = []
        for z, shift in ((7, lane_down), (0, lane_up)):
            rows = [shift(rext[pl.ds(base + 64 * t + z, 8, stride=8), :]) for t in range(3)]
            ends.append(rows)
        halves = []
        for b in range(2):
            halves.append(
                jnp.concatenate(
                    [rext[base + 64 * b : base + 64 * b + 80, :]]
                    + ends[0][b : b + 2]
                    + ends[1][b : b + 2],
                    0,
                )
            )
        hi, lo = split(jnp.concatenate(halves, 1))
        r = dot(a1_ref[...], jnp.concatenate([hi, lo], 0))
        spec[p] = r[:104] + r[104:]

    even = [i for i in range(0, 10, 2)]
    odd = [i for i in range(1, 10, 2)]
    for b in range(2):
        lanes = slice(b * LANES, (b + 1) * LANES)
        cx, cy, cz, m = [
            jnp.broadcast_to(coef_ref[b * 4 + k : b * 4 + k + 1, :], (8, LANES)) for k in range(4)
        ]

        def chunk(t, carry):
            row = pl.ds(pl.multiple_of(t * 8, 8), 8)
            v = [spec[p, row, lanes] for p in range(10)]
            d0 = cy * lj_ref[row, :] + cz * lk_ref[row, :] + m
            s = [v[p] + v[9 - p] for p in range(5)]
            d = [v[p] - v[9 - p] for p in range(5)]
            z = [None] * 10
            for i in range(10):
                h = s if i % 2 == 0 else d
                acc = h[0] * float(SINES[i, 0])
                for p in range(1, 5):
                    acc = acc + h[p] * float(SINES[i, p])
                z[i] = acc / (d0 + cx * float(LAM[i]))
            for p in range(5):
                e = z[0] * float(SINES[0, p])
                o = z[1] * float(SINES[1, p])
                for i in even[1:]:
                    e = e + z[i] * float(SINES[i, p])
                for i in odd[1:]:
                    o = o + z[i] * float(SINES[i, p])
                spec[p, row, lanes] = e + o
                spec[9 - p, row, lanes] = e - o
            return carry

        lax.fori_loop(0, 13, chunk, 0)

    for p in range(10):
        base = p * 192
        hi, lo = split(spec[p])
        r = dot(a2_ref[...], jnp.concatenate([hi, lo], 0))
        r = r[:112] + r[112:]
        r0 = r[:, :LANES]
        r1 = r[:, LANES:]
        wout[base : base + 64, :] = r0[0:64]
        wout[base + 64 : base + 80, :] = r0[64:80] + r1[0:16]
        wout[base + 80 : base + 144, :] = r1[16:80]
        wout[base + 144 : base + 192, :] = jnp.zeros((48, LANES), F32)
        for off, z, shift in ((80, 7, lane_up), (96, 0, lane_down)):
            rows = [
                r0[off : off + 8],
                r0[off + 8 : off + 16] + r1[off : off + 8],
                r1[off + 8 : off + 16],
            ]
            for t in range(3):
                at = pl.ds(base + 64 * t + z, 8, stride=8)
                wout[at, :] = wout[at, :] + shift(rows[t])


def put(ref, p, y, value):
    n = value.shape[0]
    at = (p * 24 + y) * 8
    ref[at : at + n * 8, :] = value.reshape(n * 8, LANES)


def get(ref, p, y, n):
    at = (p * 24 + y) * 8
    return ref[at : at + n * 8, :].reshape(n, 8, LANES)


def with_rows(line, n, d, u, down, up):
    rows_d = d * down
    rows_u = u * up
    low = rows_d[n - 2 : n] + jnp.concatenate([line[0:1] * down, line[1:2]], 0)
    high = rows_u[0:2] + jnp.concatenate([line[16:17], line[17:18] * up], 0)
    parts = [low, line[2:16], high]
    if n > 2:
        parts = [rows_d[0 : n - 2]] + parts + [rows_u[2:n]]
    return jnp.concatenate(parts, 0)


def first_kernel(
    src_ref, coef_ref, xl_ref, xr_ref, yd_ref, yu_ref, a1_ref, a2_ref, lj_ref, lk_ref,
    rext_ref, w_ref, to_down_ref, to_up_ref, spec, wout,
):
    left, right, down, up = flags()
    zero = jnp.zeros((6, 8, LANES), F32)
    for p in range(10):
        if p in (0, 9):
            x_ref, side = (xl_ref, left) if p == 0 else (xr_ref, right)
            put(rext_ref, p, 0, x_ref[0:1] * (side * down))
            put(rext_ref, p, 1, x_ref[1:17] * side)
            put(rext_ref, p, 17, x_ref[17:18] * (side * up))
        else:
            put(rext_ref, p, 0, yd_ref[p - 1 : p] * down)
            put(rext_ref, p, 1, src_ref[p - 1])
            put(rext_ref, p, 17, yu_ref[p - 1 : p] * up)
        put(rext_ref, p, 18, zero)
    block_solves(rext_ref, coef_ref, a1_ref, a2_ref, lj_ref, lk_ref, spec, wout)
    for p in range(10):
        line = get(wout, p, 0, 18)
        w_ref[p] = line
        to_down_ref[p] = line[0:3]
        to_up_ref[p] = line[15:18]


def edge_kernel(w_ref, d_ref, u_ref, to_left_ref, to_right_ref):
    _, _, down, up = flags()
    n = d_ref.shape[1]
    for k in range(n):
        for p, out in ((k, to_left_ref), (10 - n + k, to_right_ref)):
            at = p if w_ref.shape[0] == 10 or p < n else p - 10 + 2 * n
            out[k] = with_rows(w_ref[at], n, d_ref[p], u_ref[p], down, up)


def neighbours_z(u):
    z = lax.broadcasted_iota(jnp.int32, u.shape, 1)
    s = pltpu.roll(u, 7, 1)
    above = jnp.where(z == 7, lane_up(s), s)
    s = pltpu.roll(u, 1, 1)
    below = jnp.where(z == 0, lane_down(s), s)
    return above, below


def second_kernel(
    rext_ref, coef_ref, xl_ref, xr_ref, yd_ref, yu_ref, w_ref, l_ref, r_ref, d_ref, u_ref,
    a1_ref, a2_ref, lj_ref, lk_ref,
    c_ref, edge_ref, to_down_ref, to_up_ref, h, cb, r1, spec, wout,
):
    left, right, down, up = flags()
    for x in range(12):
        if x == 0:
            g = l_ref[0] * left
        elif x == 11:
            g = r_ref[2] * right
        else:
            g = with_rows(w_ref[x - 1], 3, d_ref[x - 1], u_ref[x - 1], down, up)
            if x == 1:
                g = (g + l_ref[1]) * left
            elif x == 2:
                g = g + l_ref[2] * left
            elif x == 9:
                g = g + r_ref[0] * right
            elif x == 10:
                g = (g + r_ref[1]) * right
        h[x] = g
    for a, x_ref in ((0, xl_ref), (1, None), (2, xr_ref)):
        for b in range(4):
            for k in range(4):
                if b == 1 or b == 2:
                    at = (b - 1) * 4 + k
                    row = coef_ref[at : at + 1, :] if x_ref is None else x_ref[18, at : at + 1, :]
                elif x_ref is not None:
                    at = k if b == 0 else 4 + k
                    row = x_ref[19, at : at + 1, :]
                elif b == 0:
                    row = yd_ref[8, 4 + k : 5 + k, :]
                else:
                    row = yu_ref[8, k : k + 1, :]
                cb[a, b, k] = jnp.broadcast_to(row, (8, LANES))
    zero = jnp.zeros((6, 8, LANES), F32)
    for p in range(10):
        a = 0 if p == 0 else 2 if p == 9 else 1
        for y, n, b in ((0, 1, 0), (1, 4, 1), (5, 4, 1), (9, 4, 2), (13, 4, 2), (17, 1, 3)):
            v = h[p + 1, y + 1 : y + 1 + n]
            above, below = neighbours_z(v)
            two = v + v
            res = get(rext_ref, p, y, n) - (
                cb[a, b, 0] * (two - h[p + 2, y + 1 : y + 1 + n] - h[p, y + 1 : y + 1 + n])
                + cb[a, b, 1] * (two - h[p + 1, y + 2 : y + 2 + n] - h[p + 1, y : y + n])
                + cb[a, b, 2] * (two - above - below)
                + cb[a, b, 3] * v
            )
            if p == 0:
                res = res * left
            if p == 9:
                res = res * right
            if y == 0:
                res = res * down
            if y == 17:
                res = res * up
            put(r1, p, y, res)
        put(r1, p, 18, zero)
    block_solves(r1, coef_ref, a1_ref, a2_ref, lj_ref, lk_ref, spec, wout)
    for p in range(10):
        line = get(wout, p, 0, 18)
        c_ref[p] = h[p + 1, 1:19] + line
        if p < 2:
            edge_ref[p] = line
        if p > 7:
            edge_ref[p - 6] = line
        to_down_ref[p] = line[0:2]
        to_up_ref[p] = line[16:18]


def last_kernel(
    src_ref, coef_ref, c_ref, l_ref, r_ref, d_ref, u_ref, slot_ref, group_ref, wm_ref,
    smooth_hbm, res_hbm, part_ref, h, mu, mr, smooth_ref, res_ref, sems,
):
    left, right, down, up = flags()
    for p in range(10):
        g = with_rows(c_ref[p], 2, d_ref[p], u_ref[p], down, up)
        if p == 0:
            g = (g + l_ref[0]) * left
        elif p == 1:
            g = g + l_ref[1] * left
        elif p == 8:
            g = g + r_ref[0] * right
        elif p == 9:
            g = (g + r_ref[1]) * right
        h[p] = g
    for b in range(2):
        lanes = slice(b * LANES, (b + 1) * LANES)
        cf = [
            jnp.broadcast_to(coef_ref[b * 4 + k : b * 4 + k + 1, :], (8, LANES)) for k in range(4)
        ]
        for x in range(8):
            p = x + 1
            for y in (0, 4):
                yy = b * 8 + y + 1
                v = h[p, yy : yy + 4]
                above, below = neighbours_z(v)
                two = v + v
                res = src_ref[x, yy - 1 : yy + 3] - (
                    cf[0] * (two - h[p + 1, yy : yy + 4] - h[p - 1, yy : yy + 4])
                    + cf[1] * (two - h[p, yy + 1 : yy + 5] - h[p, yy - 1 : yy + 3])
                    + cf[2] * (two - above - below)
                    + cf[3] * v
                )
                at = (x * 8 + y) * 8
                mu[at : at + 32, lanes] = v.reshape(32, LANES)
                mr[at : at + 32, lanes] = res.reshape(32, LANES)
    oh = onehot(slot_ref[...])
    mom = jnp.zeros((16, 256), F32)
    copies = []
    for x in range(8):
        at = slice(x * 64, x * 64 + 64)
        uh, ul = split(mu[at, :])
        rh, rl = split(mr[at, :])
        o = dot(jnp.concatenate([uh, ul, rh, rl], 0), oh)
        smooth_ref[at, :] = o[0:64] + o[64:128]
        res_ref[at, :] = o[128:192] + o[192:256]
        for k, (v, hbm) in enumerate(((smooth_ref, smooth_hbm), (res_ref, res_hbm))):
            at = pl.ds(x * 64, 64)
            copies.append(pltpu.make_async_copy(v.at[at, :], hbm.at[at, :], sems.at[2 * x + k]))
            copies[-1].start()
    for x in range(4):
        at = slice(x * 128, x * 128 + 128)
        rh, rl = split(mr[at, :])
        mom = mom + dot(wm_ref[:, at], rh) + dot(wm_ref[:, at], rl)
    mh, ml = split(mom[0:8] + mom[8:16])
    mom = dot(mh, oh) + dot(ml, oh)
    ny = part_ref.shape[0]
    col = group_ref[...] - lax.axis_index("sx") * (ny * GRP_DEV)
    owner = lax.shift_right_logical(col, 4)
    member = jnp.bitwise_and(col, 15)
    sel = lax.broadcasted_iota(jnp.int32, (ny, 256), 0)
    pick = jnp.where(sel == owner, 1.0, 0.0).astype(BF16)
    m16 = lax.broadcasted_iota(jnp.int32, (16, 256), 0) == member
    spread = jnp.concatenate(
        [jnp.where(m16, jnp.broadcast_to(mom[v : v + 1], (16, 256)), 0.0) for v in range(8)], 0
    )
    sh, sl = split(spread)
    part_ref[...] = dot_t(pick, sh) + dot_t(pick, sl)
    for c in copies:
        c.wait()


def sd(*shape):
    return jax.ShapeDtypeStruct(shape, F32)


def vm(*shape):
    return pltpu.VMEM(shape, F32)


def ring(value, axis, by):
    n = lax.axis_size(axis)
    return lax.ppermute(value, axis, [(i, (i + by) % n) for i in range(n)])


def call(kernel, outs, args, scratch=(), hbm_in=0, hbm_out=0, sems=0):
    vmem = pl.BlockSpec(memory_space=pltpu.VMEM)
    hbm = pl.BlockSpec(memory_space=pl.ANY)
    args = [
        a if k < hbm_in else pltpu.with_memory_space_constraint(a, pltpu.VMEM)
        for k, a in enumerate(args)
    ]
    scratch = [pltpu.VMEM(s, F32) for s in scratch]
    if sems:
        scratch.append(pltpu.SemaphoreType.DMA((sems,)))
    return pl.pallas_call(
        kernel,
        out_shape=outs,
        in_specs=[hbm if k < hbm_in else vmem for k in range(len(args))],
        out_specs=[hbm if k < hbm_out else vmem for k in range(len(outs))],
        scratch_shapes=scratch,
        compiler_params=pltpu.CompilerParams(vmem_limit_bytes=16 << 20),
    )(*args)


def on_device(right_side, stretch, mass_term, slot_position, coarse_group):
    a1 = jnp.asarray(A_FWD, BF16)
    a2 = jnp.asarray(A_BWD, BF16)
    lj = jnp.asarray(LAM_J, F32)
    lk = jnp.asarray(LAM_K, F32)
    wm = jnp.asarray(W_MOM, BF16)
    row = pltpu.VMEM((1, 256), jnp.int32)
    src, coef, to_d, to_u, slot, group = call(
        place_kernel,
        [vm(8, 16, 8, LANES), vm(8, LANES), vm(9, 8, LANES), vm(9, 8, LANES), row, row],
        (
            right_side.reshape(512, 256),
            stretch,
            mass_term.reshape(1, 256),
            slot_position.reshape(1, 256),
            coarse_group.reshape(1, 256),
        ),
        [(512, 256), (3, 256), (1, 256)],
        hbm_in=5,
        sems=12,
    )
    yd = ring(to_u, "sy", 1)
    yu = ring(to_d, "sy", -1)
    to_l, to_r = call(rim_kernel, [vm(20, 8, LANES)] * 2, (src, coef, yd, yu))
    xl = ring(to_r, "sx", 1)
    xr = ring(to_l, "sx", -1)

    side = vm(10, 3, 8, LANES)
    rext, w, to_d, to_u = call(
        first_kernel,
        [vm(1920, LANES), vm(10, 18, 8, LANES), side, side],
        (src, coef, xl, xr, yd, yu, a1, a2, lj, lk),
        [(10, 104, 256), (1920, LANES)],
    )
    d = ring(to_u, "sy", 1)
    u = ring(to_d, "sy", -1)
    to_l, to_r = call(edge_kernel, [vm(3, 20, 8, LANES)] * 2, (w, d, u))
    l = ring(to_r, "sx", 1)
    r = ring(to_l, "sx", -1)

    side = vm(10, 2, 8, LANES)
    c, w, to_d, to_u = call(
        second_kernel,
        [vm(10, 18, 8, LANES), vm(4, 18, 8, LANES), side, side],
        (rext, coef, xl, xr, yd, yu, w, l, r, d, u, a1, a2, lj, lk),
        [(12, 20, 8, LANES), (3, 4, 4, 8, LANES), (1920, LANES), (10, 104, 256), (1920, LANES)],
    )
    d = ring(to_u, "sy", 1)
    u = ring(to_d, "sy", -1)
    to_l, to_r = call(edge_kernel, [vm(2, 18, 8, LANES)] * 2, (w, d, u))
    l = ring(to_r, "sx", 1)
    r = ring(to_l, "sx", -1)

    ny = lax.axis_size("sy")
    smooth, res, part = call(
        last_kernel,
        [sd(512, 256), sd(512, 256), vm(ny, LANES)],
        (src, coef, c, l, r, d, u, slot, group, wm),
        [(10, 18, 8, LANES)] + [(512, 256)] * 4,
        hbm_out=2,
        sems=16,
    )
    arrived = lax.all_to_all(part, "sy", split_axis=0, concat_axis=0, tiled=True)
    coarse = arrived.sum(axis=0).reshape(8, GRP_DEV)
    return smooth.reshape(8, 8, 8, 256), res.reshape(8, 8, 8, 256), coarse


def solution(mesh):
    split_all = P(None, None, None, ("sx", "sy"))
    flat = P(("sx", "sy"))
    return jax.shard_map(
        on_device,
        mesh=mesh,
        in_specs=(split_all, P(None, ("sx", "sy")), flat, flat, flat),
        out_specs=(split_all, split_all, P(None, ("sx", "sy"))),
        check_vma=False,
    )
```

```python
import jax
import jax.numpy as jnp
import numpy as np
from jax import lax
from jax.experimental import pallas as pl
from jax.experimental.pallas import tpu as pltpu
from jax.sharding import PartitionSpec as P

NODES = 8
GRP_DEV = 16
LANES = 128
RELAX = 0.35
F32 = jnp.float32
BF16 = jnp.bfloat16


def split_np(a):
    a = np.asarray(a, np.float32)
    hi = np.asarray(jnp.asarray(a).astype(BF16).astype(F32))
    return hi, a - hi


def constants():
    n = NODES + 2
    col = np.arange(n, dtype=np.float64) + 1.0
    s = np.sqrt(2.0 / (n + 1.0)) * np.sin(np.pi * col[:, None] * col[None, :] / (n + 1.0))
    lam = 2.0 - 2.0 * np.cos(np.pi * col / (n + 1.0))
    fwd = np.zeros((104, 112))
    for q in range(n):
        for r in range(n):
            c = q * 8 + r - 1
            if r == 0:
                c = 80 + q
            if r == n - 1:
                c = 96 + q
            fwd[:100, c] = np.outer(s[:, q], s[:, r]).reshape(-1)
    fh, fl = split_np(fwd)
    a1 = np.concatenate([np.concatenate([fh, fh], 1), np.concatenate([fl, fl], 1)], 0)
    bh, bl = split_np(RELAX * fwd.T)
    a2 = np.concatenate([np.concatenate([bh, bh], 1), np.concatenate([bl, bl], 1)], 0)
    lam_j = np.ones((104, LANES), np.float32)
    lam_k = np.ones((104, LANES), np.float32)
    lam_j[:100] = np.repeat(lam, n)[:, None]
    lam_k[:100] = np.tile(lam, n)[:, None]
    t = np.arange(NODES) / (NODES - 1.0)
    w = np.stack([1.0 - t, t])
    wm = np.einsum("ax,by,cz->abcxyz", w, w, w).reshape(8, 512)
    wh, wl = split_np(wm)
    wm = np.concatenate([wh, wl], 0)
    rim = wm.reshape(16, 8, 8, 8)[:, :, [0, 1, 6, 7]].reshape(16, 256)
    return s, lam, a1, a2, lam_j, lam_k, wm, rim


SINES, LAM, A_FWD, A_BWD, LAM_J, LAM_K, W_MOM, W_RIM = constants()


def split(x):
    hi = x.astype(BF16)
    return hi, (x - hi.astype(F32)).astype(BF16)


def dot(a, b):
    return lax.dot_general(a, b, (((1,), (0,)), ((), ())), preferred_element_type=F32)


def dot_t(a, b):
    return lax.dot_general(a, b, (((1,), (1,)), ((), ())), preferred_element_type=F32)


def flags():
    i = lax.axis_index("sx")
    j = lax.axis_index("sy")
    nx = lax.axis_size("sx")
    ny = lax.axis_size("sy")
    one = lambda c: jnp.where(c, 1.0, 0.0).astype(F32)
    return one(i > 0), one(i < nx - 1), one(j > 0), one(j < ny - 1)


def lane_up(x):
    lane = lax.broadcasted_iota(jnp.int32, x.shape, x.ndim - 1)
    return jnp.where(lane == LANES - 1, 0.0, pltpu.roll(x, LANES - 1, x.ndim - 1))


def lane_down(x):
    lane = lax.broadcasted_iota(jnp.int32, x.shape, x.ndim - 1)
    return jnp.where(lane == 0, 0.0, pltpu.roll(x, 1, x.ndim - 1))


def onehot(slot_row):
    p = lax.broadcasted_iota(jnp.int32, (256, 256), 0)
    return jnp.where(p == slot_row, 1.0, 0.0).astype(BF16)


def place_kernel(
    rhs_hbm, stretch_hbm, mass_hbm, slot_hbm, group_hbm,
    src_ref, coef_ref, to_down_ref, to_up_ref, slot_ref,
    rhs_ref, stretch_ref, mass_ref, group_ref, sems,
):
    small = [
        pltpu.make_async_copy(h, v, sems.at[8 + k])
        for k, (h, v) in enumerate(
            (
                (slot_hbm, slot_ref),
                (stretch_hbm, stretch_ref),
                (mass_hbm, mass_ref),
                (group_hbm, group_ref),
            )
        )
    ]
    big = [
        pltpu.make_async_copy(
            rhs_hbm.at[pl.ds(x * 64, 64), :], rhs_ref.at[pl.ds(x * 64, 64), :], sems.at[x]
        )
        for x in range(8)
    ]
    for c in small + big:
        c.start()
    small[0].wait()
    oh = onehot(slot_ref[...])
    for c in small[1:]:
        c.wait()
    c = jnp.concatenate(
        [
            stretch_ref[...],
            mass_ref[...],
            group_ref[...].astype(F32),
            jnp.zeros((3, 256), F32),
        ],
        0,
    )
    c1 = c.astype(BF16)
    r1 = c - c1.astype(F32)
    c2 = r1.astype(BF16)
    c3 = (r1 - c2.astype(F32)).astype(BF16)
    cg = dot_t(c1, oh) + dot_t(c2, oh) + dot_t(c3, oh)
    coef = jnp.concatenate([cg[0:4, :LANES], cg[0:4, LANES:]], 0)
    gr = jnp.concatenate([cg[4:5, :LANES], cg[4:5, LANES:], jnp.zeros((6, LANES), F32)], 0)
    coef_ref[0] = coef
    coef_ref[1] = gr
    for out in (to_down_ref, to_up_ref):
        out[8] = coef
        out[9] = gr
    for x in range(8):
        big[x].wait()
        a = rhs_ref[x * 64 : (x + 1) * 64, :]
        a1 = a.astype(BF16)
        e = a - a1.astype(F32)
        a2 = e.astype(BF16)
        a3 = (e - a2.astype(F32)).astype(BF16)
        g = dot_t(jnp.concatenate([a1, a2, a3], 0), oh)
        g = g[0:64] + g[64:128] + g[128:192]
        for b in range(2):
            block = g[:, b * LANES : (b + 1) * LANES].reshape(8, 8, LANES)
            src_ref[x, b * 8 : b * 8 + 8] = block
            if b == 0:
                to_down_ref[x] = block[0]
            else:
                to_up_ref[x] = block[7]


def rim_kernel(src_ref, coef_ref, yd_ref, yu_ref, to_left_ref, to_right_ref):
    coef_y = jnp.concatenate([yd_ref[8, 4:8, :], yu_ref[8, 0:4, :]], 0)
    for x, out in ((0, to_left_ref), (7, to_right_ref)):
        out[0] = yd_ref[x]
        out[1:17] = src_ref[x]
        out[17] = yu_ref[x]
        out[18] = coef_ref[0]
        out[19] = coef_y


def block_solves(rext, coef_ref, a1_ref, a2_ref, lj_ref, lk_ref, spec, wout):
    for p in range(10):
        base = p * 192
        ends = []
        for z, shift in ((7, lane_down), (0, lane_up)):
            rows = [shift(rext[pl.ds(base + 64 * t + z, 8, stride=8), :]) for t in range(3)]
            ends.append(rows)
        halves = []
        for b in range(2):
            halves.append(
                jnp.concatenate(
                    [rext[base + 64 * b : base + 64 * b + 80, :]]
                    + ends[0][b : b + 2]
                    + ends[1][b : b + 2],
                    0,
                )
            )
        hi, lo = split(jnp.concatenate(halves, 1))
        r = dot(a1_ref[...], jnp.concatenate([hi, lo], 0))
        spec[p] = r[:104] + r[104:]

    even = [i for i in range(0, 10, 2)]
    odd = [i for i in range(1, 10, 2)]
    for b in range(2):
        lanes = slice(b * LANES, (b + 1) * LANES)
        cx, cy, cz, m = [
            jnp.broadcast_to(coef_ref[0, b * 4 + k : b * 4 + k + 1, :], (8, LANES)) for k in range(4)
        ]

        def chunk(t, carry):
            row = pl.ds(pl.multiple_of(t * 8, 8), 8)
            v = [spec[p, row, lanes] for p in range(10)]
            d0 = cy * lj_ref[row, :] + cz * lk_ref[row, :] + m
            s = [v[p] + v[9 - p] for p in range(5)]
            d = [v[p] - v[9 - p] for p in range(5)]
            z = [None] * 10
            for i in range(10):
                h = s if i % 2 == 0 else d
                acc = h[0] * float(SINES[i, 0])
                for p in range(1, 5):
                    acc = acc + h[p] * float(SINES[i, p])
                z[i] = acc / (d0 + cx * float(LAM[i]))
            for p in range(5):
                e = z[0] * float(SINES[0, p])
                o = z[1] * float(SINES[1, p])
                for i in even[1:]:
                    e = e + z[i] * float(SINES[i, p])
                for i in odd[1:]:
                    o = o + z[i] * float(SINES[i, p])
                spec[p, row, lanes] = e + o
                spec[9 - p, row, lanes] = e - o
            return carry

        lax.fori_loop(0, 13, chunk, 0)

    for p in range(10):
        base = p * 192
        hi, lo = split(spec[p])
        r = dot(a2_ref[...], jnp.concatenate([hi, lo], 0))
        r = r[:112] + r[112:]
        r0 = r[:, :LANES]
        r1 = r[:, LANES:]
        wout[base : base + 64, :] = r0[0:64]
        wout[base + 64 : base + 80, :] = r0[64:80] + r1[0:16]
        wout[base + 80 : base + 144, :] = r1[16:80]
        wout[base + 144 : base + 192, :] = jnp.zeros((48, LANES), F32)
        for off, z, shift in ((80, 7, lane_up), (96, 0, lane_down)):
            rows = [
                r0[off : off + 8],
                r0[off + 8 : off + 16] + r1[off : off + 8],
                r1[off + 8 : off + 16],
            ]
            for t in range(3):
                at = pl.ds(base + 64 * t + z, 8, stride=8)
                wout[at, :] = wout[at, :] + shift(rows[t])


def put(ref, p, y, value):
    n = value.shape[0]
    at = (p * 24 + y) * 8
    ref[at : at + n * 8, :] = value.reshape(n * 8, LANES)


def get(ref, p, y, n):
    at = (p * 24 + y) * 8
    return ref[at : at + n * 8, :].reshape(n, 8, LANES)


def with_rows(line, n, d, u, down, up):
    rows_d = d * down
    rows_u = u * up
    low = rows_d[n - 2 : n] + jnp.concatenate([line[0:1] * down, line[1:2]], 0)
    high = rows_u[0:2] + jnp.concatenate([line[16:17], line[17:18] * up], 0)
    parts = [low, line[2:16], high]
    if n > 2:
        parts = [rows_d[0 : n - 2]] + parts + [rows_u[2:n]]
    return jnp.concatenate(parts, 0)


def first_kernel(
    src_ref, coef_ref, xl_ref, xr_ref, yd_ref, yu_ref, a1_ref, a2_ref, lj_ref, lk_ref,
    rext_ref, w_ref, to_down_ref, to_up_ref, spec, wout,
):
    left, right, down, up = flags()
    zero = jnp.zeros((6, 8, LANES), F32)
    for p in range(10):
        if p in (0, 9):
            x_ref, side = (xl_ref, left) if p == 0 else (xr_ref, right)
            put(rext_ref, p, 0, x_ref[0:1] * (side * down))
            put(rext_ref, p, 1, x_ref[1:17] * side)
            put(rext_ref, p, 17, x_ref[17:18] * (side * up))
        else:
            put(rext_ref, p, 0, yd_ref[p - 1 : p] * down)
            put(rext_ref, p, 1, src_ref[p - 1])
            put(rext_ref, p, 17, yu_ref[p - 1 : p] * up)
        put(rext_ref, p, 18, zero)
    block_solves(rext_ref, coef_ref, a1_ref, a2_ref, lj_ref, lk_ref, spec, wout)
    for p in range(10):
        line = get(wout, p, 0, 18)
        w_ref[p] = line
        to_down_ref[p] = line[0:3]
        to_up_ref[p] = line[15:18]


def edge_kernel(w_ref, d_ref, u_ref, to_left_ref, to_right_ref):
    _, _, down, up = flags()
    for k in range(3):
        for p, out in ((k, to_left_ref), (7 + k, to_right_ref)):
            out[k] = with_rows(w_ref[p], 3, d_ref[p], u_ref[p], down, up)


def neighbours_z(u):
    z = lax.broadcasted_iota(jnp.int32, u.shape, 1)
    s = pltpu.roll(u, 7, 1)
    above = jnp.where(z == 7, lane_up(s), s)
    s = pltpu.roll(u, 1, 1)
    below = jnp.where(z == 0, lane_down(s), s)
    return above, below


def second_kernel(
    rext_ref, coef_ref, xl_ref, xr_ref, yd_ref, yu_ref, w_ref, l_ref, r_ref, d_ref, u_ref,
    a1_ref, a2_ref, lj_ref, lk_ref,
    c_ref, to_left_ref, to_right_ref, own_down_ref, own_up_ref, h, cb, r1, spec, wout,
):
    left, right, down, up = flags()
    for x in range(12):
        if x == 0:
            g = l_ref[0] * left
        elif x == 11:
            g = r_ref[2] * right
        else:
            g = with_rows(w_ref[x - 1], 3, d_ref[x - 1], u_ref[x - 1], down, up)
            if x == 1:
                g = (g + l_ref[1]) * left
            elif x == 2:
                g = g + l_ref[2] * left
            elif x == 9:
                g = g + r_ref[0] * right
            elif x == 10:
                g = (g + r_ref[1]) * right
        h[x] = g
    for a, x_ref in ((0, xl_ref), (1, None), (2, xr_ref)):
        for b in range(4):
            for k in range(4):
                if b == 1 or b == 2:
                    at = (b - 1) * 4 + k
                    row = coef_ref[0, at : at + 1, :] if x_ref is None else x_ref[18, at : at + 1, :]
                elif x_ref is not None:
                    at = k if b == 0 else 4 + k
                    row = x_ref[19, at : at + 1, :]
                elif b == 0:
                    row = yd_ref[8, 4 + k : 5 + k, :]
                else:
                    row = yu_ref[8, k : k + 1, :]
                cb[a, b, k] = jnp.broadcast_to(row, (8, LANES))
    zero = jnp.zeros((6, 8, LANES), F32)
    for p in range(10):
        a = 0 if p == 0 else 2 if p == 9 else 1
        for y, n, b in ((0, 1, 0), (1, 4, 1), (5, 4, 1), (9, 4, 2), (13, 4, 2), (17, 1, 3)):
            v = h[p + 1, y + 1 : y + 1 + n]
            above, below = neighbours_z(v)
            two = v + v
            res = get(rext_ref, p, y, n) - (
                cb[a, b, 0] * (two - h[p + 2, y + 1 : y + 1 + n] - h[p, y + 1 : y + 1 + n])
                + cb[a, b, 1] * (two - h[p + 1, y + 2 : y + 2 + n] - h[p + 1, y : y + n])
                + cb[a, b, 2] * (two - above - below)
                + cb[a, b, 3] * v
            )
            if p == 0:
                res = res * left
            if p == 9:
                res = res * right
            if y == 0:
                res = res * down
            if y == 17:
                res = res * up
            put(r1, p, y, res)
        put(r1, p, 18, zero)
    block_solves(r1, coef_ref, a1_ref, a2_ref, lj_ref, lk_ref, spec, wout)
    for p in range(10):
        line = get(wout, p, 0, 18)
        c_ref[p] = h[p + 1, 1:19] + line
        if p < 2:
            to_left_ref[p] = line
        if p > 7:
            to_right_ref[p - 8] = line
        own_down_ref[p] = line[0:2]
        own_up_ref[p] = line[16:18]


def add_x(g, p, l, r, left, right):
    if p == 0:
        return (g + l[0]) * left
    if p == 1:
        return g + l[1] * left
    if p == 8:
        return g + r[0] * right
    if p == 9:
        return (g + r[1]) * right
    return g


def rows_of(tile, at):
    return [jnp.broadcast_to(tile[at + k : at + k + 1, :], (8, LANES)) for k in range(4)]


def stencil(cf, v, x_sum, y_sum):
    above, below = neighbours_z(v)
    two = v + v
    return (
        cf[0] * (two - x_sum) + cf[1] * (two - y_sum) + cf[2] * (two - above - below) + cf[3] * v
    )


def middle_kernel(
    src_ref, coef_ref, yd_ref, yu_ref, c_ref, l_ref, r_ref, own_down_ref, own_up_ref,
    wm_ref, wr_ref,
    mu_ref, mr_ref, to_down_ref, to_up_ref, part_ref, h, rim,
):
    left, right, down, up = flags()
    for p in range(10):
        h[p] = add_x(c_ref[p], p, l_ref, r_ref, left, right)
        e = add_x(own_down_ref[p], p, l_ref[:, 0:2], r_ref[:, 0:2], left, right)
        to_down_ref[p] = jnp.concatenate([e[0:1] * down, e[1:2]], 0)
        e = add_x(own_up_ref[p], p, l_ref[:, 16:18], r_ref[:, 16:18], left, right)
        to_up_ref[p] = jnp.concatenate([e[0:1], e[1:2] * up], 0)
        h[p, 0] = h[p, 0] * down
        h[p, 17] = h[p, 17] * up
    for b in range(2):
        lanes = slice(b * LANES, (b + 1) * LANES)
        cf = rows_of(coef_ref[0], b * 4)
        for x in range(8):
            p = x + 1
            for y in (0, 4):
                yy = b * 8 + y + 1
                v = h[p, yy : yy + 4]
                res = src_ref[x, yy - 1 : yy + 3] - stencil(
                    cf,
                    v,
                    h[p + 1, yy : yy + 4] + h[p - 1, yy : yy + 4],
                    h[p, yy + 1 : yy + 5] + h[p, yy - 1 : yy + 3],
                )
                at = (x * 8 + y) * 8
                mu_ref[at : at + 32, lanes] = v.reshape(32, LANES)
                mr_ref[at : at + 32, lanes] = res.reshape(32, LANES)
    rim[...] = jnp.zeros((256, 256), F32)
    for slab, far, near, tile, b, lanes, y_far, y_near in (
        (to_down_ref, 0, 1, yd_ref, 1, slice(0, LANES), 2, 3),
        (to_up_ref, 1, 0, yu_ref, 0, slice(LANES, 256), 1, 0),
    ):
        cf = rows_of(tile[8], b * 4)
        for x in range(8):
            p = x + 1
            v = slab[p, far : far + 1]
            res = stencil(
                cf,
                v,
                slab[p + 1, far : far + 1] + slab[p - 1, far : far + 1],
                slab[p, near : near + 1],
            )
            at = (x * 4 + y_near) * 8
            rim[at : at + 8, lanes] = -res[0]
            at = (x * 4 + y_far) * 8
            rim[at : at + 8, lanes] = cf[1] * v[0]
    mom = jnp.zeros((16, 256), F32)
    for x in range(4):
        at = slice(x * 128, x * 128 + 128)
        rh, rl = split(mr_ref[at, :])
        mom = mom + dot(wm_ref[:, at], rh) + dot(wm_ref[:, at], rl)
    rh, rl = split(rim[...])
    mom_y = dot(wr_ref[...], rh) + dot(wr_ref[...], rl)
    mom_y = mom_y[0:8] + mom_y[8:16]
    mom = jnp.concatenate(
        [mom[0:8] + mom[8:16], mom_y[:, :LANES] * down, mom_y[:, LANES:] * up], 1
    )
    gr = coef_ref[1]
    group = jnp.concatenate([gr[0:1], gr[1:2], yd_ref[9, 1:2, :], yu_ref[9, 0:1, :]], 1)
    ny = part_ref.shape[0]
    col = (group + 0.5).astype(jnp.int32) - lax.axis_index("sx") * (ny * GRP_DEV)
    owner = lax.shift_right_logical(col, 4)
    member = jnp.bitwise_and(col, 15)
    sel = lax.broadcasted_iota(jnp.int32, (ny, 512), 0)
    pick = jnp.where(sel == owner, 1.0, 0.0).astype(BF16)
    m16 = lax.broadcasted_iota(jnp.int32, (16, 512), 0) == member
    spread = jnp.concatenate(
        [jnp.where(m16, jnp.broadcast_to(mom[v : v + 1], (16, 512)), 0.0) for v in range(8)], 0
    )
    sh, sl = split(spread)
    part_ref[...] = dot_t(pick, sh) + dot_t(pick, sl)


def last_kernel(
    mu_ref, mr_ref, coef_ref, d_ref, u_ref, slot_ref, arrived_ref,
    smooth_hbm, res_hbm, coarse_hbm, smooth_ref, res_ref, coarse_ref, sems,
):
    _, _, down, up = flags()
    total = jnp.sum(arrived_ref[...], axis=0, keepdims=True)
    for v in range(8):
        coarse_ref[v : v + 1, :] = total[:, v * GRP_DEV : (v + 1) * GRP_DEV]
    copies = [pltpu.make_async_copy(coarse_ref, coarse_hbm, sems.at[16])]
    copies[0].start()
    oh = onehot(slot_ref[...])
    sides = (
        (d_ref, down, 0, 1, rows_of(coef_ref[0], 0), 0, 1),
        (u_ref, up, 1, 0, rows_of(coef_ref[0], 4), 7, 6),
    )
    for x in range(8):
        at = slice(x * 64, x * 64 + 64)
        mu = mu_ref[at, :]
        mr = mr_ref[at, :]
        add_u, add_r = [], []
        for slab, on, far, near, cf, y0, y1 in sides:
            p = x + 1
            v = slab[p, near : near + 1] * on
            x_sum = (slab[p + 1, near : near + 1] + slab[p - 1, near : near + 1]) * on
            res = stencil(cf, v, x_sum, slab[p, far : far + 1] * on)
            zero = jnp.zeros((8, LANES), F32)
            ru = [zero] * 8
            rr = [zero] * 8
            ru[y0] = v[0]
            rr[y0] = -res[0]
            rr[y1] = cf[1] * v[0]
            add_u.append(jnp.concatenate(ru, 0))
            add_r.append(jnp.concatenate(rr, 0))
        uh, ul = split(mu + jnp.concatenate(add_u, 1))
        rh, rl = split(mr + jnp.concatenate(add_r, 1))
        o = dot(jnp.concatenate([uh, ul, rh, rl], 0), oh)
        smooth_ref[at, :] = o[0:64] + o[64:128]
        res_ref[at, :] = o[128:192] + o[192:256]
        for k, (v, hbm) in enumerate(((smooth_ref, smooth_hbm), (res_ref, res_hbm))):
            rows = pl.ds(x * 64, 64)
            copies.append(
                pltpu.make_async_copy(v.at[rows, :], hbm.at[rows, :], sems.at[2 * x + k])
            )
            copies[-1].start()
    for c in copies:
        c.wait()


def sd(*shape):
    return jax.ShapeDtypeStruct(shape, F32)


def vm(*shape):
    return pltpu.VMEM(shape, F32)


def ring(value, axis, by):
    n = lax.axis_size(axis)
    return lax.ppermute(value, axis, [(i, (i + by) % n) for i in range(n)])


def call(kernel, outs, args, scratch=(), hbm_in=0, hbm_out=0, sems=0):
    vmem = pl.BlockSpec(memory_space=pltpu.VMEM)
    hbm = pl.BlockSpec(memory_space=pltpu.HBM)
    args = [
        pltpu.with_memory_space_constraint(a, pltpu.HBM if k < hbm_in else pltpu.VMEM)
        for k, a in enumerate(args)
    ]
    scratch = [pltpu.VMEM(s, F32) if isinstance(s, tuple) else s for s in scratch]
    if sems:
        scratch.append(pltpu.SemaphoreType.DMA((sems,)))
    return pl.pallas_call(
        kernel,
        out_shape=outs,
        in_specs=[hbm if k < hbm_in else vmem for k in range(len(args))],
        out_specs=[hbm if k < hbm_out else vmem for k in range(len(outs))],
        scratch_shapes=scratch,
        compiler_params=pltpu.CompilerParams(vmem_limit_bytes=16 << 20),
    )(*args)


def on_device(right_side, stretch, mass_term, slot_position, coarse_group):
    a1 = jnp.asarray(A_FWD, BF16)
    a2 = jnp.asarray(A_BWD, BF16)
    lj = jnp.asarray(LAM_J, F32)
    lk = jnp.asarray(LAM_K, F32)
    wm = jnp.asarray(W_MOM, BF16)
    wr = jnp.asarray(W_RIM, BF16)
    row = pltpu.VMEM((1, 256), jnp.int32)
    src, coef, to_d, to_u, slot = call(
        place_kernel,
        [vm(8, 16, 8, LANES), vm(2, 8, LANES), vm(10, 8, LANES), vm(10, 8, LANES), row],
        (
            right_side.reshape(512, 256),
            stretch,
            mass_term.reshape(1, 256),
            slot_position.reshape(1, 256),
            coarse_group.reshape(1, 256),
        ),
        [(512, 256), (3, 256), (1, 256), row],
        hbm_in=5,
        sems=12,
    )
    yd = ring(to_u, "sy", 1)
    yu = ring(to_d, "sy", -1)
    to_l, to_r = call(rim_kernel, [vm(20, 8, LANES)] * 2, (src, coef, yd, yu))
    xl = ring(to_r, "sx", 1)
    xr = ring(to_l, "sx", -1)

    side = vm(10, 3, 8, LANES)
    rext, w, to_d, to_u = call(
        first_kernel,
        [vm(1920, LANES), vm(10, 18, 8, LANES), side, side],
        (src, coef, xl, xr, yd, yu, a1, a2, lj, lk),
        [(10, 104, 256), (1920, LANES)],
    )
    d = ring(to_u, "sy", 1)
    u = ring(to_d, "sy", -1)
    to_l, to_r = call(edge_kernel, [vm(3, 20, 8, LANES)] * 2, (w, d, u))
    l = ring(to_r, "sx", 1)
    r = ring(to_l, "sx", -1)

    slab = vm(2, 18, 8, LANES)
    side = vm(10, 2, 8, LANES)
    c, to_l, to_r, own_d, own_u = call(
        second_kernel,
        [vm(10, 18, 8, LANES), slab, slab, side, side],
        (rext, coef, xl, xr, yd, yu, w, l, r, d, u, a1, a2, lj, lk),
        [(12, 20, 8, LANES), (3, 4, 4, 8, LANES), (1920, LANES), (10, 104, 256), (1920, LANES)],
    )
    l = ring(to_r, "sx", 1)
    r = ring(to_l, "sx", -1)
    ny = lax.axis_size("sy")
    mu, mr, to_d, to_u, part = call(
        middle_kernel,
        [vm(512, 256), vm(512, 256), side, side, vm(ny, LANES)],
        (src, coef, yd, yu, c, l, r, own_d, own_u, wm, wr),
        [(10, 18, 8, LANES), (256, 256)],
    )
    d = ring(to_u, "sy", 1)
    u = ring(to_d, "sy", -1)
    arrived = lax.all_to_all(part, "sy", split_axis=0, concat_axis=0, tiled=True)
    smooth, res, coarse = call(
        last_kernel,
        [sd(512, 256), sd(512, 256), sd(8, GRP_DEV)],
        (mu, mr, coef, d, u, slot, arrived),
        [(512, 256), (512, 256), (8, GRP_DEV)],
        hbm_out=3,
        sems=17,
    )
    return smooth.reshape(8, 8, 8, 256), res.reshape(8, 8, 8, 256), coarse


def solution(mesh):
    split_all = P(None, None, None, ("sx", "sy"))
    flat = P(("sx", "sy"))
    return jax.shard_map(
        on_device,
        mesh=mesh,
        in_specs=(split_all, P(None, ("sx", "sy")), flat, flat, flat),
        out_specs=(split_all, split_all, P(None, ("sx", "sy"))),
        check_vma=False,
    )
```

```python
import jax
import jax.numpy as jnp
import numpy as np
from jax import lax
from jax.experimental import pallas as pl
from jax.experimental.pallas import tpu as pltpu
from jax.sharding import PartitionSpec as P

NODES = 8
GRP_DEV = 16
LANES = 128
RELAX = 0.35
F32 = jnp.float32
BF16 = jnp.bfloat16


def split_np(a):
    a = np.asarray(a, np.float32)
    hi = np.asarray(jnp.asarray(a).astype(BF16).astype(F32))
    return hi, a - hi


def constants():
    n = NODES + 2
    col = np.arange(n, dtype=np.float64) + 1.0
    s = np.sqrt(2.0 / (n + 1.0)) * np.sin(np.pi * col[:, None] * col[None, :] / (n + 1.0))
    lam = 2.0 - 2.0 * np.cos(np.pi * col / (n + 1.0))
    fwd = np.zeros((104, 112))
    for q in range(n):
        for r in range(n):
            c = q * 8 + r - 1
            if r == 0:
                c = 80 + q
            if r == n - 1:
                c = 96 + q
            fwd[:100, c] = np.outer(s[:, q], s[:, r]).reshape(-1)
    fh, fl = split_np(fwd)
    a1 = np.concatenate([np.concatenate([fh, fh], 1), np.concatenate([fl, fl], 1)], 0)
    bh, bl = split_np(RELAX * fwd.T)
    a2 = np.concatenate([np.concatenate([bh, bh], 1), np.concatenate([bl, bl], 1)], 0)
    lam_j = np.ones((104, LANES), np.float32)
    lam_k = np.ones((104, LANES), np.float32)
    lam_j[:100] = np.repeat(lam, n)[:, None]
    lam_k[:100] = np.tile(lam, n)[:, None]
    t = np.arange(NODES) / (NODES - 1.0)
    w = np.stack([1.0 - t, t])
    wm = np.einsum("ax,by,cz->abcxyz", w, w, w).reshape(8, 512)
    wh, wl = split_np(wm)
    wm = np.concatenate([wh, wl], 0)
    rim = wm.reshape(16, 8, 8, 8)[:, :, [0, 1, 6, 7]].reshape(16, 256)
    return s, lam, a1, a2, lam_j, lam_k, wm, rim


SINES, LAM, A_FWD, A_BWD, LAM_J, LAM_K, W_MOM, W_RIM = constants()


def split(x):
    hi = x.astype(BF16)
    return hi, (x - hi.astype(F32)).astype(BF16)


def dot(a, b):
    return lax.dot_general(a, b, (((1,), (0,)), ((), ())), preferred_element_type=F32)


def dot_t(a, b):
    return lax.dot_general(a, b, (((1,), (1,)), ((), ())), preferred_element_type=F32)


def flags():
    i = lax.axis_index("sx")
    j = lax.axis_index("sy")
    nx = lax.axis_size("sx")
    ny = lax.axis_size("sy")
    one = lambda c: jnp.where(c, 1.0, 0.0).astype(F32)
    return one(i > 0), one(i < nx - 1), one(j > 0), one(j < ny - 1)


def lane_up(x):
    lane = lax.broadcasted_iota(jnp.int32, x.shape, x.ndim - 1)
    return jnp.where(lane == LANES - 1, 0.0, pltpu.roll(x, LANES - 1, x.ndim - 1))


def lane_down(x):
    lane = lax.broadcasted_iota(jnp.int32, x.shape, x.ndim - 1)
    return jnp.where(lane == 0, 0.0, pltpu.roll(x, 1, x.ndim - 1))


def onehot(slot_row):
    p = lax.broadcasted_iota(jnp.int32, (256, 256), 0)
    return jnp.where(p == slot_row, 1.0, 0.0).astype(BF16)


def split3(a):
    a1 = a.astype(BF16)
    e = a - a1.astype(F32)
    a2 = e.astype(BF16)
    return a1, a2, (e - a2.astype(F32)).astype(BF16)


def start_kernel(
    rhs_hbm, stretch_hbm, mass_hbm, slot_hbm, group_hbm,
    coef_ref, to_down_ref, to_up_ref, slot_ref,
    face_ref, stretch_ref, mass_ref, group_ref, sems,
):
    pairs = (
        (slot_hbm, slot_ref),
        (rhs_hbm.at[:, pl.ds(0, 8), :], face_ref.at[0]),
        (rhs_hbm.at[:, pl.ds(56, 8), :], face_ref.at[1]),
        (stretch_hbm, stretch_ref),
        (mass_hbm, mass_ref),
        (group_hbm, group_ref),
    )
    copies = [pltpu.make_async_copy(h, v, sems.at[k]) for k, (h, v) in enumerate(pairs)]
    for c in copies:
        c.start()
    copies[0].wait()
    oh = onehot(slot_ref[...])
    for k, out, b in ((1, to_down_ref, 0), (2, to_up_ref, 1)):
        copies[k].wait()
        g = dot_t(jnp.concatenate(split3(face_ref[k - 1].reshape(64, 256)), 0), oh)
        g = g[0:64] + g[64:128] + g[128:192]
        out[0:8] = g[:, b * LANES : (b + 1) * LANES].reshape(8, 8, LANES)
    for c in copies[3:]:
        c.wait()
    c = jnp.concatenate(
        [
            stretch_ref[...],
            mass_ref[...],
            group_ref[...].astype(F32),
            jnp.zeros((3, 256), F32),
        ],
        0,
    )
    c1, c2, c3 = split3(c)
    cg = dot_t(c1, oh) + dot_t(c2, oh) + dot_t(c3, oh)
    coef = jnp.concatenate([cg[0:4, :LANES], cg[0:4, LANES:]], 0)
    gr = jnp.concatenate([cg[4:5, :LANES], cg[4:5, LANES:], jnp.zeros((6, LANES), F32)], 0)
    coef_ref[0] = coef
    coef_ref[1] = gr
    for out in (to_down_ref, to_up_ref):
        out[8] = coef
        out[9] = gr


def place_kernel(rhs_hbm, slot_ref, src_ref, rhs_ref, sems):
    copies = [
        pltpu.make_async_copy(rhs_hbm.at[x], rhs_ref.at[x], sems.at[x]) for x in range(8)
    ]
    for c in copies:
        c.start()
    oh = onehot(slot_ref[...])
    for x in range(8):
        copies[x].wait()
        g = dot_t(jnp.concatenate(split3(rhs_ref[x]), 0), oh)
        g = g[0:64] + g[64:128] + g[128:192]
        for b in range(2):
            src_ref[x, b * 8 : b * 8 + 8] = g[:, b * LANES : (b + 1) * LANES].reshape(8, 8, LANES)


def rim_kernel(src_ref, coef_ref, yd_ref, yu_ref, to_left_ref, to_right_ref):
    coef_y = jnp.concatenate([yd_ref[8, 4:8, :], yu_ref[8, 0:4, :]], 0)
    for x, out in ((0, to_left_ref), (7, to_right_ref)):
        out[0] = yd_ref[x]
        out[1:17] = src_ref[x]
        out[17] = yu_ref[x]
        out[18] = coef_ref[0]
        out[19] = coef_y


def forward(res, base, a1_ref):
    ends = []
    for z, shift in ((7, lane_down), (0, lane_up)):
        ends.append([shift(res[pl.ds(base + 64 * t + z, 8, stride=8), :]) for t in range(3)])
    halves = [
        jnp.concatenate(
            [res[base + 64 * b : base + 64 * b + 80, :]] + ends[0][b : b + 2] + ends[1][b : b + 2],
            0,
        )
        for b in range(2)
    ]
    hi, lo = split(jnp.concatenate(halves, 1))
    r = dot(a1_ref[...], jnp.concatenate([hi, lo], 0))
    return r[:104] + r[104:]


def finish_solves(layers, coef_ref, a2_ref, lj_ref, lk_ref, spec, wout):
    even = [i for i in range(0, 10, 2)]
    odd = [i for i in range(1, 10, 2)]
    for b in range(2):
        lanes = slice(b * LANES, (b + 1) * LANES)
        cx, cy, cz, m = rows_of(coef_ref[0], b * 4)

        def chunk(t, carry):
            row = pl.ds(pl.multiple_of(t * 8, 8), 8)
            v = [ref[at, row, lanes] for ref, at in layers]
            d0 = cy * lj_ref[row, :] + cz * lk_ref[row, :] + m
            s = [v[p] + v[9 - p] for p in range(5)]
            d = [v[p] - v[9 - p] for p in range(5)]
            z = [None] * 10
            for i in range(10):
                h = s if i % 2 == 0 else d
                acc = h[0] * float(SINES[i, 0])
                for p in range(1, 5):
                    acc = acc + h[p] * float(SINES[i, p])
                z[i] = acc / (d0 + cx * float(LAM[i]))
            for p in range(5):
                e = z[0] * float(SINES[0, p])
                o = z[1] * float(SINES[1, p])
                for i in even[1:]:
                    e = e + z[i] * float(SINES[i, p])
                for i in odd[1:]:
                    o = o + z[i] * float(SINES[i, p])
                spec[p, row, lanes] = e + o
                spec[9 - p, row, lanes] = e - o
            return carry

        lax.fori_loop(0, 13, chunk, 0)

    for p in range(10):
        base = p * 192
        hi, lo = split(spec[p])
        r = dot(a2_ref[...], jnp.concatenate([hi, lo], 0))
        r = r[:112] + r[112:]
        r0 = r[:, :LANES]
        r1 = r[:, LANES:]
        wout[base : base + 64, :] = r0[0:64]
        wout[base + 64 : base + 80, :] = r0[64:80] + r1[0:16]
        wout[base + 80 : base + 144, :] = r1[16:80]
        wout[base + 144 : base + 192, :] = jnp.zeros((48, LANES), F32)
        for off, z, shift in ((80, 7, lane_up), (96, 0, lane_down)):
            rows = [
                r0[off : off + 8],
                r0[off + 8 : off + 16] + r1[off : off + 8],
                r1[off + 8 : off + 16],
            ]
            for t in range(3):
                at = pl.ds(base + 64 * t + z, 8, stride=8)
                wout[at, :] = wout[at, :] + shift(rows[t])


def put(ref, p, y, value):
    n = value.shape[0]
    at = (p * 24 + y) * 8
    ref[at : at + n * 8, :] = value.reshape(n * 8, LANES)


def get(ref, p, y, n):
    at = (p * 24 + y) * 8
    return ref[at : at + n * 8, :].reshape(n, 8, LANES)


def with_rows(line, n, d, u, down, up):
    rows_d = d * down
    rows_u = u * up
    low = rows_d[n - 2 : n] + jnp.concatenate([line[0:1] * down, line[1:2]], 0)
    high = rows_u[0:2] + jnp.concatenate([line[16:17], line[17:18] * up], 0)
    parts = [low, line[2:16], high]
    if n > 2:
        parts = [rows_d[0 : n - 2]] + parts + [rows_u[2:n]]
    return jnp.concatenate(parts, 0)


def put_layer(ref, at, below, line, above):
    put(ref, at, 0, below)
    put(ref, at, 1, line)
    put(ref, at, 17, above)
    put(ref, at, 18, jnp.zeros((6, 8, LANES), F32))


def first_inner_kernel(src_ref, yd_ref, yu_ref, a1_ref, rin_ref, sin_ref):
    _, _, down, up = flags()
    for x in range(8):
        put_layer(rin_ref, x, yd_ref[x : x + 1] * down, src_ref[x], yu_ref[x : x + 1] * up)
        sin_ref[x] = forward(rin_ref, x * 192, a1_ref)


def first_kernel(
    coef_ref, xl_ref, xr_ref, sin_ref, a1_ref, a2_ref, lj_ref, lk_ref,
    rout_ref, w_ref, to_down_ref, to_up_ref, sout, spec, wout,
):
    left, right, down, up = flags()
    for k, (x_ref, side) in enumerate(((xl_ref, left), (xr_ref, right))):
        put_layer(
            rout_ref,
            k,
            x_ref[0:1] * (side * down),
            x_ref[1:17] * side,
            x_ref[17:18] * (side * up),
        )
        sout[k] = forward(rout_ref, k * 192, a1_ref)
    layers = [(sout, 0)] + [(sin_ref, x) for x in range(8)] + [(sout, 1)]
    finish_solves(layers, coef_ref, a2_ref, lj_ref, lk_ref, spec, wout)
    for p in range(10):
        line = get(wout, p, 0, 18)
        w_ref[p] = line
        to_down_ref[p] = line[0:3]
        to_up_ref[p] = line[15:18]


def edge_kernel(w_ref, d_ref, u_ref, to_left_ref, to_right_ref):
    _, _, down, up = flags()
    for k in range(3):
        for p, out in ((k, to_left_ref), (7 + k, to_right_ref)):
            out[k] = with_rows(w_ref[p], 3, d_ref[p], u_ref[p], down, up)


def neighbours_z(u):
    z = lax.broadcasted_iota(jnp.int32, u.shape, 1)
    s = pltpu.roll(u, 7, 1)
    above = jnp.where(z == 7, lane_up(s), s)
    s = pltpu.roll(u, 1, 1)
    below = jnp.where(z == 0, lane_down(s), s)
    return above, below


ROWS = ((0, 1, 0), (1, 4, 1), (5, 4, 1), (9, 4, 2), (13, 4, 2), (17, 1, 3))


def second_residual(get_h, get_r, cb, p, at, res_ref, left, right, down, up):
    for y, n, b in ROWS:
        v = get_h(p + 1, y + 1, n)
        res = get_r(y, n) - stencil(
            cb[b],
            v,
            get_h(p + 2, y + 1, n) + get_h(p, y + 1, n),
            get_h(p + 1, y + 2, n) + get_h(p + 1, y, n),
        )
        if p == 0:
            res = res * left
        if p == 9:
            res = res * right
        if y == 0:
            res = res * down
        if y == 17:
            res = res * up
        put(res_ref, at, y, res)
    put(res_ref, at, 18, jnp.zeros((6, 8, LANES), F32))


def spread_coefs(cb, rows):
    for b, (tile, at) in enumerate(rows):
        for k, v in enumerate(rows_of(tile, at)):
            cb[b, k] = v
    return [[cb.at[b, k] for k in range(4)] for b in range(4)]


class Loaded:
    def __init__(self, refs):
        self.refs = refs

    def __getitem__(self, k):
        return self.refs[k][...]


def second_inner_kernel(
    rin_ref, coef_ref, yd_ref, yu_ref, w_ref, d_ref, u_ref, a1_ref, h_ref, sin_ref, cb, r1,
):
    left, right, down, up = flags()
    for x in range(3, 9):
        h_ref[x - 3] = with_rows(w_ref[x - 1], 3, d_ref[x - 1], u_ref[x - 1], down, up)
    tiles = spread_coefs(
        cb, ((yd_ref[8], 4), (coef_ref[0], 0), (coef_ref[0], 4), (yu_ref[8], 0))
    )
    coefs = [Loaded(t) for t in tiles]
    get_h = lambda x, y, n: h_ref[x - 3, y : y + n]
    for k in range(4):
        p = 3 + k
        get_r = lambda y, n: get(rin_ref, p - 1, y, n)
        second_residual(get_h, get_r, coefs, p, k, r1, left, right, down, up)
        sin_ref[k] = forward(r1, k * 192, a1_ref)


def second_kernel(
    rin_ref, rout_ref, coef_ref, xl_ref, xr_ref, yd_ref, yu_ref, w_ref, l_ref, r_ref, d_ref, u_ref,
    hin_ref, sin_ref, a1_ref, a2_ref, lj_ref, lk_ref,
    c_ref, to_left_ref, to_right_ref, own_down_ref, own_up_ref, h, cb, r1, sout, spec, wout,
):
    left, right, down, up = flags()
    for x in (0, 1, 2, 9, 10, 11):
        if x == 0:
            g = l_ref[0] * left
        elif x == 11:
            g = r_ref[2] * right
        else:
            g = with_rows(w_ref[x - 1], 3, d_ref[x - 1], u_ref[x - 1], down, up)
            if x == 1:
                g = (g + l_ref[1]) * left
            elif x == 2:
                g = g + l_ref[2] * left
            elif x == 9:
                g = g + r_ref[0] * right
            elif x == 10:
                g = (g + r_ref[1]) * right
        h[x if x < 3 else x - 6] = g

    def get_h(x, y, n):
        if 3 <= x <= 8:
            return hin_ref[x - 3, y : y + n]
        return h[x if x < 3 else x - 6, y : y + n]

    coefs = []
    for a, x_ref in ((0, xl_ref), (1, None), (2, xr_ref)):
        if x_ref is None:
            rows = ((yd_ref[8], 4), (coef_ref[0], 0), (coef_ref[0], 4), (yu_ref[8], 0))
        else:
            rows = ((x_ref[19], 0), (x_ref[18], 0), (x_ref[18], 4), (x_ref[19], 4))
        coefs.append([Loaded(t) for t in spread_coefs(cb.at[a], rows)])
    layers = [None] * 3 + [(sin_ref, k) for k in range(4)] + [None] * 3
    for k, p in enumerate((0, 1, 2, 7, 8, 9)):
        if p in (0, 9):
            get_r = lambda y, n: get(rout_ref, 0 if p == 0 else 1, y, n)
        else:
            get_r = lambda y, n: get(rin_ref, p - 1, y, n)
        cb_p = coefs[0 if p == 0 else 2 if p == 9 else 1]
        second_residual(get_h, get_r, cb_p, p, k, r1, left, right, down, up)
        sout[k] = forward(r1, k * 192, a1_ref)
        layers[p] = (sout, k)
    finish_solves(layers, coef_ref, a2_ref, lj_ref, lk_ref, spec, wout)
    for p in range(10):
        line = get(wout, p, 0, 18)
        c_ref[p] = get_h(p + 1, 1, 18) + line
        if p < 2:
            to_left_ref[p] = line
        if p > 7:
            to_right_ref[p - 8] = line
        own_down_ref[p] = line[0:2]
        own_up_ref[p] = line[16:18]


def add_x(g, p, l, r, left, right):
    if p == 0:
        return (g + l[0]) * left
    if p == 1:
        return g + l[1] * left
    if p == 8:
        return g + r[0] * right
    if p == 9:
        return (g + r[1]) * right
    return g


def rows_of(tile, at):
    return [jnp.broadcast_to(tile[at + k : at + k + 1, :], (8, LANES)) for k in range(4)]


def stencil(cf, v, x_sum, y_sum):
    above, below = neighbours_z(v)
    two = v + v
    return (
        cf[0] * (two - x_sum) + cf[1] * (two - y_sum) + cf[2] * (two - above - below) + cf[3] * v
    )


def middle_kernel(
    src_ref, coef_ref, yd_ref, yu_ref, c_ref, l_ref, r_ref, own_down_ref, own_up_ref,
    wm_ref, wr_ref,
    mu_ref, mr_ref, to_down_ref, to_up_ref, part_ref, h, rim,
):
    left, right, down, up = flags()
    for p in range(10):
        h[p] = add_x(c_ref[p], p, l_ref, r_ref, left, right)
        e = add_x(own_down_ref[p], p, l_ref[:, 0:2], r_ref[:, 0:2], left, right)
        to_down_ref[p] = jnp.concatenate([e[0:1] * down, e[1:2]], 0)
        e = add_x(own_up_ref[p], p, l_ref[:, 16:18], r_ref[:, 16:18], left, right)
        to_up_ref[p] = jnp.concatenate([e[0:1], e[1:2] * up], 0)
        h[p, 0] = h[p, 0] * down
        h[p, 17] = h[p, 17] * up
    for b in range(2):
        lanes = slice(b * LANES, (b + 1) * LANES)
        cf = rows_of(coef_ref[0], b * 4)
        for x in range(8):
            p = x + 1
            for y in (0, 4):
                yy = b * 8 + y + 1
                v = h[p, yy : yy + 4]
                res = src_ref[x, yy - 1 : yy + 3] - stencil(
                    cf,
                    v,
                    h[p + 1, yy : yy + 4] + h[p - 1, yy : yy + 4],
                    h[p, yy + 1 : yy + 5] + h[p, yy - 1 : yy + 3],
                )
                at = (x * 8 + y) * 8
                mu_ref[at : at + 32, lanes] = v.reshape(32, LANES)
                mr_ref[at : at + 32, lanes] = res.reshape(32, LANES)
    rim[...] = jnp.zeros((256, 256), F32)
    for slab, far, near, tile, b, lanes, y_far, y_near in (
        (to_down_ref, 0, 1, yd_ref, 1, slice(0, LANES), 2, 3),
        (to_up_ref, 1, 0, yu_ref, 0, slice(LANES, 256), 1, 0),
    ):
        cf = rows_of(tile[8], b * 4)
        for x in range(8):
            p = x + 1
            v = slab[p, far : far + 1]
            res = stencil(
                cf,
                v,
                slab[p + 1, far : far + 1] + slab[p - 1, far : far + 1],
                slab[p, near : near + 1],
            )
            at = (x * 4 + y_near) * 8
            rim[at : at + 8, lanes] = -res[0]
            at = (x * 4 + y_far) * 8
            rim[at : at + 8, lanes] = cf[1] * v[0]
    mom = jnp.zeros((16, 256), F32)
    for x in range(4):
        at = slice(x * 128, x * 128 + 128)
        rh, rl = split(mr_ref[at, :])
        mom = mom + dot(wm_ref[:, at], rh) + dot(wm_ref[:, at], rl)
    rh, rl = split(rim[...])
    mom_y = dot(wr_ref[...], rh) + dot(wr_ref[...], rl)
    mom_y = mom_y[0:8] + mom_y[8:16]
    mom = jnp.concatenate(
        [mom[0:8] + mom[8:16], mom_y[:, :LANES] * down, mom_y[:, LANES:] * up], 1
    )
    gr = coef_ref[1]
    group = jnp.concatenate([gr[0:1], gr[1:2], yd_ref[9, 1:2, :], yu_ref[9, 0:1, :]], 1)
    ny = part_ref.shape[0]
    col = (group + 0.5).astype(jnp.int32) - lax.axis_index("sx") * (ny * GRP_DEV)
    owner = lax.shift_right_logical(col, 4)
    member = jnp.bitwise_and(col, 15)
    sel = lax.broadcasted_iota(jnp.int32, (ny, 512), 0)
    pick = jnp.where(sel == owner, 1.0, 0.0).astype(BF16)
    m16 = lax.broadcasted_iota(jnp.int32, (16, 512), 0) == member
    spread = jnp.concatenate(
        [jnp.where(m16, jnp.broadcast_to(mom[v : v + 1], (16, 512)), 0.0) for v in range(8)], 0
    )
    sh, sl = split(spread)
    part_ref[...] = dot_t(pick, sh) + dot_t(pick, sl)


def last_kernel(
    mu_ref, mr_ref, coef_ref, d_ref, u_ref, slot_ref, arrived_ref,
    smooth_hbm, res_hbm, coarse_hbm, smooth_ref, res_ref, coarse_ref, sems,
):
    _, _, down, up = flags()
    total = jnp.sum(arrived_ref[...], axis=0, keepdims=True)
    for v in range(8):
        coarse_ref[v : v + 1, :] = total[:, v * GRP_DEV : (v + 1) * GRP_DEV]
    copies = [pltpu.make_async_copy(coarse_ref, coarse_hbm, sems.at[16])]
    copies[0].start()
    oh = onehot(slot_ref[...])
    sides = (
        (d_ref, down, 0, 1, rows_of(coef_ref[0], 0), 0, 1),
        (u_ref, up, 1, 0, rows_of(coef_ref[0], 4), 7, 6),
    )
    for x in range(8):
        at = slice(x * 64, x * 64 + 64)
        mu = mu_ref[at, :]
        mr = mr_ref[at, :]
        add_u, add_r = [], []
        for slab, on, far, near, cf, y0, y1 in sides:
            p = x + 1
            v = slab[p, near : near + 1] * on
            x_sum = (slab[p + 1, near : near + 1] + slab[p - 1, near : near + 1]) * on
            res = stencil(cf, v, x_sum, slab[p, far : far + 1] * on)
            zero = jnp.zeros((8, LANES), F32)
            ru = [zero] * 8
            rr = [zero] * 8
            ru[y0] = v[0]
            rr[y0] = -res[0]
            rr[y1] = cf[1] * v[0]
            add_u.append(jnp.concatenate(ru, 0))
            add_r.append(jnp.concatenate(rr, 0))
        uh, ul = split(mu + jnp.concatenate(add_u, 1))
        rh, rl = split(mr + jnp.concatenate(add_r, 1))
        o = dot(jnp.concatenate([uh, ul, rh, rl], 0), oh)
        smooth_ref[at, :] = o[0:64] + o[64:128]
        res_ref[at, :] = o[128:192] + o[192:256]
        for k, (v, hbm) in enumerate(((smooth_ref, smooth_hbm), (res_ref, res_hbm))):
            rows = pl.ds(x * 64, 64)
            copies.append(
                pltpu.make_async_copy(v.at[rows, :], hbm.at[rows, :], sems.at[2 * x + k])
            )
            copies[-1].start()
    for c in copies:
        c.wait()


def sd(*shape):
    return jax.ShapeDtypeStruct(shape, F32)


def vm(*shape):
    return pltpu.VMEM(shape, F32)


def ring(value, axis, by):
    n = lax.axis_size(axis)
    return lax.ppermute(value, axis, [(i, (i + by) % n) for i in range(n)])


def call(kernel, outs, args, scratch=(), hbm_in=0, hbm_out=0, sems=0):
    vmem = pl.BlockSpec(memory_space=pltpu.VMEM)
    hbm = pl.BlockSpec(memory_space=pltpu.HBM)
    args = [
        pltpu.with_memory_space_constraint(a, pltpu.HBM if k < hbm_in else pltpu.VMEM)
        for k, a in enumerate(args)
    ]
    scratch = [pltpu.VMEM(s, F32) if isinstance(s, tuple) else s for s in scratch]
    if sems:
        scratch.append(pltpu.SemaphoreType.DMA((sems,)))
    return pl.pallas_call(
        kernel,
        out_shape=outs,
        in_specs=[hbm if k < hbm_in else vmem for k in range(len(args))],
        out_specs=[hbm if k < hbm_out else vmem for k in range(len(outs))],
        scratch_shapes=scratch,
        compiler_params=pltpu.CompilerParams(vmem_limit_bytes=16 << 20),
    )(*args)


def on_device(right_side, stretch, mass_term, slot_position, coarse_group):
    a1 = jnp.asarray(A_FWD, BF16)
    a2 = jnp.asarray(A_BWD, BF16)
    lj = jnp.asarray(LAM_J, F32)
    lk = jnp.asarray(LAM_K, F32)
    wm = jnp.asarray(W_MOM, BF16)
    wr = jnp.asarray(W_RIM, BF16)
    row = pltpu.VMEM((1, 256), jnp.int32)
    rhs = right_side.reshape(8, 64, 256)
    coef, to_d, to_u, slot = call(
        start_kernel,
        [vm(2, 8, LANES), vm(10, 8, LANES), vm(10, 8, LANES), row],
        (
            rhs,
            stretch,
            mass_term.reshape(1, 256),
            slot_position.reshape(1, 256),
            coarse_group.reshape(1, 256),
        ),
        [(2, 8, 8, 256), (3, 256), (1, 256), row],
        hbm_in=5,
        sems=6,
    )
    yd = ring(to_u, "sy", 1)
    yu = ring(to_d, "sy", -1)
    src = call(
        place_kernel, [vm(8, 16, 8, LANES)], (rhs, slot), [(8, 64, 256)], hbm_in=1, sems=8
    )[0]
    to_l, to_r = call(rim_kernel, [vm(20, 8, LANES)] * 2, (src, coef, yd, yu))
    xl = ring(to_r, "sx", 1)
    xr = ring(to_l, "sx", -1)
    rin, sin = call(
        first_inner_kernel, [vm(8 * 192, LANES), vm(8, 104, 256)], (src, yd, yu, a1)
    )

    side = vm(10, 3, 8, LANES)
    rout, w, to_d, to_u = call(
        first_kernel,
        [vm(2 * 192, LANES), vm(10, 18, 8, LANES), side, side],
        (coef, xl, xr, sin, a1, a2, lj, lk),
        [(2, 104, 256), (10, 104, 256), (1920, LANES)],
    )
    d = ring(to_u, "sy", 1)
    u = ring(to_d, "sy", -1)
    to_l, to_r = call(edge_kernel, [vm(3, 20, 8, LANES)] * 2, (w, d, u))
    l = ring(to_r, "sx", 1)
    r = ring(to_l, "sx", -1)
    hin, sin = call(
        second_inner_kernel,
        [vm(6, 20, 8, LANES), vm(4, 104, 256)],
        (rin, coef, yd, yu, w, d, u, a1),
        [(4, 4, 8, LANES), (4 * 192, LANES)],
    )

    slab = vm(2, 18, 8, LANES)
    side = vm(10, 2, 8, LANES)
    c, to_l, to_r, own_d, own_u = call(
        second_kernel,
        [vm(10, 18, 8, LANES), slab, slab, side, side],
        (rin, rout, coef, xl, xr, yd, yu, w, l, r, d, u, hin, sin, a1, a2, lj, lk),
        [
            (6, 20, 8, LANES),
            (3, 4, 4, 8, LANES),
            (6 * 192, LANES),
            (6, 104, 256),
            (10, 104, 256),
            (1920, LANES),
        ],
    )
    l = ring(to_r, "sx", 1)
    r = ring(to_l, "sx", -1)
    ny = lax.axis_size("sy")
    mu, mr, to_d, to_u, part = call(
        middle_kernel,
        [vm(512, 256), vm(512, 256), side, side, vm(ny, LANES)],
        (src, coef, yd, yu, c, l, r, own_d, own_u, wm, wr),
        [(10, 18, 8, LANES), (256, 256)],
    )
    d = ring(to_u, "sy", 1)
    u = ring(to_d, "sy", -1)
    arrived = lax.all_to_all(part, "sy", split_axis=0, concat_axis=0, tiled=True)
    smooth, res, coarse = call(
        last_kernel,
        [sd(512, 256), sd(512, 256), sd(8, GRP_DEV)],
        (mu, mr, coef, d, u, slot, arrived),
        [(512, 256), (512, 256), (8, GRP_DEV)],
        hbm_out=3,
        sems=17,
    )
    return smooth.reshape(8, 8, 8, 256), res.reshape(8, 8, 8, 256), coarse


def solution(mesh):
    split_all = P(None, None, None, ("sx", "sy"))
    flat = P(("sx", "sy"))
    return jax.shard_map(
        on_device,
        mesh=mesh,
        in_specs=(split_all, P(None, ("sx", "sy")), flat, flat, flat),
        out_specs=(split_all, split_all, P(None, ("sx", "sy"))),
        check_vma=False,
    )
```

```python
import jax
import jax.numpy as jnp
import numpy as np
from jax import lax
from jax.experimental import pallas as pl
from jax.experimental.pallas import tpu as pltpu
from jax.sharding import PartitionSpec as P

NODES = 8
GRP_DEV = 16
LANES = 128
RELAX = 0.35
F32 = jnp.float32
BF16 = jnp.bfloat16


def split_np(a):
    a = np.asarray(a, np.float32)
    hi = np.asarray(jnp.asarray(a).astype(BF16).astype(F32))
    return hi, a - hi


def constants():
    n = NODES + 2
    col = np.arange(n, dtype=np.float64) + 1.0
    s = np.sqrt(2.0 / (n + 1.0)) * np.sin(np.pi * col[:, None] * col[None, :] / (n + 1.0))
    lam = 2.0 - 2.0 * np.cos(np.pi * col / (n + 1.0))
    fwd = np.zeros((104, 112))
    for q in range(n):
        for r in range(n):
            c = q * 8 + r - 1
            if r == 0:
                c = 80 + q
            if r == n - 1:
                c = 96 + q
            fwd[:100, c] = np.outer(s[:, q], s[:, r]).reshape(-1)
    fh, fl = split_np(fwd)
    a1 = np.concatenate([np.concatenate([fh, fh], 1), np.concatenate([fl, fl], 1)], 0)
    bh, bl = split_np(RELAX * fwd.T)
    a2 = np.concatenate([np.concatenate([bh, bh], 1), np.concatenate([bl, bl], 1)], 0)
    lam_j = np.ones((104, LANES), np.float32)
    lam_k = np.ones((104, LANES), np.float32)
    lam_j[:100] = np.repeat(lam, n)[:, None]
    lam_k[:100] = np.tile(lam, n)[:, None]
    t = np.arange(NODES) / (NODES - 1.0)
    w = np.stack([1.0 - t, t])
    wm = np.einsum("ax,by,cz->abcxyz", w, w, w).reshape(8, 512)
    wh, wl = split_np(wm)
    wm = np.concatenate([wh, wl], 0)
    rim = wm.reshape(16, 8, 8, 8)[:, :, [0, 1, 6, 7]].reshape(16, 256)
    return s, lam, a1, a2, lam_j, lam_k, wm, rim


SINES, LAM, A_FWD, A_BWD, LAM_J, LAM_K, W_MOM, W_RIM = constants()


def split(x):
    hi = x.astype(BF16)
    return hi, (x - hi.astype(F32)).astype(BF16)


def dot(a, b):
    return lax.dot_general(a, b, (((1,), (0,)), ((), ())), preferred_element_type=F32)


def dot_t(a, b):
    return lax.dot_general(a, b, (((1,), (1,)), ((), ())), preferred_element_type=F32)


def flags():
    i = lax.axis_index("sx")
    j = lax.axis_index("sy")
    nx = lax.axis_size("sx")
    ny = lax.axis_size("sy")
    one = lambda c: jnp.where(c, 1.0, 0.0).astype(F32)
    return one(i > 0), one(i < nx - 1), one(j > 0), one(j < ny - 1)


def lane_up(x):
    lane = lax.broadcasted_iota(jnp.int32, x.shape, x.ndim - 1)
    return jnp.where(lane == LANES - 1, 0.0, pltpu.roll(x, LANES - 1, x.ndim - 1))


def lane_down(x):
    lane = lax.broadcasted_iota(jnp.int32, x.shape, x.ndim - 1)
    return jnp.where(lane == 0, 0.0, pltpu.roll(x, 1, x.ndim - 1))


def onehot(slot_row):
    p = lax.broadcasted_iota(jnp.int32, (256, 256), 0)
    return jnp.where(p == slot_row, 1.0, 0.0).astype(BF16)


def split3(a):
    a1 = a.astype(BF16)
    e = a - a1.astype(F32)
    a2 = e.astype(BF16)
    return a1, a2, (e - a2.astype(F32)).astype(BF16)


def start_kernel(
    rhs_hbm, stretch_hbm, mass_hbm, slot_hbm, group_hbm,
    coef_ref, to_down_ref, to_up_ref, slot_ref,
    face_ref, stretch_ref, mass_ref, group_ref, sems,
):
    pairs = (
        (slot_hbm, slot_ref),
        (rhs_hbm.at[:, pl.ds(0, 8), :], face_ref.at[0]),
        (rhs_hbm.at[:, pl.ds(56, 8), :], face_ref.at[1]),
        (stretch_hbm, stretch_ref),
        (mass_hbm, mass_ref),
        (group_hbm, group_ref),
    )
    copies = [pltpu.make_async_copy(h, v, sems.at[k]) for k, (h, v) in enumerate(pairs)]
    for c in copies:
        c.start()
    copies[0].wait()
    oh = onehot(slot_ref[...])
    for k, out, b in ((1, to_down_ref, 0), (2, to_up_ref, 1)):
        copies[k].wait()
        g = dot_t(jnp.concatenate(split3(face_ref[k - 1].reshape(64, 256)), 0), oh)
        g = g[0:64] + g[64:128] + g[128:192]
        out[0:8] = g[:, b * LANES : (b + 1) * LANES].reshape(8, 8, LANES)
    for c in copies[3:]:
        c.wait()
    c = jnp.concatenate(
        [
            stretch_ref[...],
            mass_ref[...],
            group_ref[...].astype(F32),
            jnp.zeros((3, 256), F32),
        ],
        0,
    )
    c1, c2, c3 = split3(c)
    cg = dot_t(c1, oh) + dot_t(c2, oh) + dot_t(c3, oh)
    coef = jnp.concatenate([cg[0:4, :LANES], cg[0:4, LANES:]], 0)
    gr = jnp.concatenate([cg[4:5, :LANES], cg[4:5, LANES:], jnp.zeros((6, LANES), F32)], 0)
    coef_ref[0] = coef
    coef_ref[1] = gr
    for out in (to_down_ref, to_up_ref):
        out[8] = coef
        out[9] = gr


def place_kernel(rhs_hbm, slot_ref, src_ref, rhs_ref, sems):
    copies = [
        pltpu.make_async_copy(rhs_hbm.at[x], rhs_ref.at[x], sems.at[x]) for x in range(8)
    ]
    for c in copies:
        c.start()
    oh = onehot(slot_ref[...])
    for x in range(8):
        copies[x].wait()
        g = dot_t(jnp.concatenate(split3(rhs_ref[x]), 0), oh)
        g = g[0:64] + g[64:128] + g[128:192]
        for b in range(2):
            src_ref[x, b * 8 : b * 8 + 8] = g[:, b * LANES : (b + 1) * LANES].reshape(8, 8, LANES)


def rim_kernel(src_ref, coef_ref, yd_ref, yu_ref, to_left_ref, to_right_ref):
    coef_y = jnp.concatenate([yd_ref[8, 4:8, :], yu_ref[8, 0:4, :]], 0)
    for x, out in ((0, to_left_ref), (7, to_right_ref)):
        out[0] = yd_ref[x]
        out[1:17] = src_ref[x]
        out[17] = yu_ref[x]
        out[18] = coef_ref[0]
        out[19] = coef_y


def forward(res, base, a1_ref):
    ends = []
    for z, shift in ((7, lane_down), (0, lane_up)):
        ends.append([shift(res[pl.ds(base + 64 * t + z, 8, stride=8), :]) for t in range(3)])
    halves = [
        jnp.concatenate(
            [res[base + 64 * b : base + 64 * b + 80, :]] + ends[0][b : b + 2] + ends[1][b : b + 2],
            0,
        )
        for b in range(2)
    ]
    hi, lo = split(jnp.concatenate(halves, 1))
    r = dot(a1_ref[...], jnp.concatenate([hi, lo], 0))
    return r[:104] + r[104:]


def finish_solves(layers, coef_ref, a2_ref, lj_ref, lk_ref, spec, wout):
    even = [i for i in range(0, 10, 2)]
    odd = [i for i in range(1, 10, 2)]
    for b in range(2):
        lanes = slice(b * LANES, (b + 1) * LANES)
        cx, cy, cz, m = rows_of(coef_ref[0], b * 4)

        def chunk(t, carry):
            row = pl.ds(pl.multiple_of(t * 8, 8), 8)
            v = [ref[at, row, lanes] for ref, at in layers]
            d0 = cy * lj_ref[row, :] + cz * lk_ref[row, :] + m
            s = [v[p] + v[9 - p] for p in range(5)]
            d = [v[p] - v[9 - p] for p in range(5)]
            z = [None] * 10
            for i in range(10):
                h = s if i % 2 == 0 else d
                acc = h[0] * float(SINES[i, 0])
                for p in range(1, 5):
                    acc = acc + h[p] * float(SINES[i, p])
                z[i] = acc / (d0 + cx * float(LAM[i]))
            for p in range(5):
                e = z[0] * float(SINES[0, p])
                o = z[1] * float(SINES[1, p])
                for i in even[1:]:
                    e = e + z[i] * float(SINES[i, p])
                for i in odd[1:]:
                    o = o + z[i] * float(SINES[i, p])
                spec[p, row, lanes] = e + o
                spec[9 - p, row, lanes] = e - o
            return carry

        lax.fori_loop(0, 13, chunk, 0)

    for p in range(10):
        base = p * 192
        hi, lo = split(spec[p])
        r = dot(a2_ref[...], jnp.concatenate([hi, lo], 0))
        r = r[:112] + r[112:]
        r0 = r[:, :LANES]
        r1 = r[:, LANES:]
        wout[base : base + 64, :] = r0[0:64]
        wout[base + 64 : base + 80, :] = r0[64:80] + r1[0:16]
        wout[base + 80 : base + 144, :] = r1[16:80]
        wout[base + 144 : base + 192, :] = jnp.zeros((48, LANES), F32)
        for off, z, shift in ((80, 7, lane_up), (96, 0, lane_down)):
            rows = [
                r0[off : off + 8],
                r0[off + 8 : off + 16] + r1[off : off + 8],
                r1[off + 8 : off + 16],
            ]
            for t in range(3):
                at = pl.ds(base + 64 * t + z, 8, stride=8)
                wout[at, :] = wout[at, :] + shift(rows[t])


def put(ref, p, y, value):
    n = value.shape[0]
    at = (p * 24 + y) * 8
    ref[at : at + n * 8, :] = value.reshape(n * 8, LANES)


def get(ref, p, y, n):
    at = (p * 24 + y) * 8
    return ref[at : at + n * 8, :].reshape(n, 8, LANES)


def with_rows(line, n, d, u, down, up):
    rows_d = d * down
    rows_u = u * up
    low = rows_d[n - 2 : n] + jnp.concatenate([line[0:1] * down, line[1:2]], 0)
    high = rows_u[0:2] + jnp.concatenate([line[16:17], line[17:18] * up], 0)
    parts = [low, line[2:16], high]
    if n > 2:
        parts = [rows_d[0 : n - 2]] + parts + [rows_u[2:n]]
    return jnp.concatenate(parts, 0)


def put_layer(ref, at, below, line, above):
    put(ref, at, 0, below)
    put(ref, at, 1, line)
    put(ref, at, 17, above)
    put(ref, at, 18, jnp.zeros((6, 8, LANES), F32))


def first_inner_kernel(src_ref, yd_ref, yu_ref, a1_ref, rin_ref, sin_ref):
    _, _, down, up = flags()
    for x in range(8):
        put_layer(rin_ref, x, yd_ref[x : x + 1] * down, src_ref[x], yu_ref[x : x + 1] * up)
        sin_ref[x] = forward(rin_ref, x * 192, a1_ref)


def first_kernel(
    coef_ref, xl_ref, xr_ref, sin_ref, a1_ref, a2_ref, lj_ref, lk_ref,
    rout_ref, w_ref, to_down_ref, to_up_ref, sout, spec, wout,
):
    left, right, down, up = flags()
    for k, (x_ref, side) in enumerate(((xl_ref, left), (xr_ref, right))):
        put_layer(
            rout_ref,
            k,
            x_ref[0:1] * (side * down),
            x_ref[1:17] * side,
            x_ref[17:18] * (side * up),
        )
        sout[k] = forward(rout_ref, k * 192, a1_ref)
    layers = [(sout, 0)] + [(sin_ref, x) for x in range(8)] + [(sout, 1)]
    finish_solves(layers, coef_ref, a2_ref, lj_ref, lk_ref, spec, wout)
    for p in range(10):
        line = get(wout, p, 0, 18)
        w_ref[p] = line
        to_down_ref[p] = line[0:3]
        to_up_ref[p] = line[15:18]


def edge_kernel(w_ref, d_ref, u_ref, to_left_ref, to_right_ref):
    _, _, down, up = flags()
    for k in range(3):
        for p, out in ((k, to_left_ref), (7 + k, to_right_ref)):
            out[k] = with_rows(w_ref[p], 3, d_ref[p], u_ref[p], down, up)


def neighbours_z(u):
    z = lax.broadcasted_iota(jnp.int32, u.shape, 1)
    s = pltpu.roll(u, 7, 1)
    above = jnp.where(z == 7, lane_up(s), s)
    s = pltpu.roll(u, 1, 1)
    below = jnp.where(z == 0, lane_down(s), s)
    return above, below


ROWS = ((0, 1, 0), (1, 4, 1), (5, 4, 1), (9, 4, 2), (13, 4, 2), (17, 1, 3))


def second_residual(get_h, get_r, cb, p, at, res_ref, left, right, down, up):
    for y, n, b in ROWS:
        v = get_h(p + 1, y + 1, n)
        res = get_r(y, n) - stencil(
            cb[b],
            v,
            get_h(p + 2, y + 1, n) + get_h(p, y + 1, n),
            get_h(p + 1, y + 2, n) + get_h(p + 1, y, n),
        )
        if p == 0:
            res = res * left
        if p == 9:
            res = res * right
        if y == 0:
            res = res * down
        if y == 17:
            res = res * up
        put(res_ref, at, y, res)
    put(res_ref, at, 18, jnp.zeros((6, 8, LANES), F32))


def spread_coefs(cb, rows):
    for b, (tile, at) in enumerate(rows):
        for k, v in enumerate(rows_of(tile, at)):
            cb[b, k] = v
    return [[cb.at[b, k] for k in range(4)] for b in range(4)]


class Loaded:
    def __init__(self, refs):
        self.refs = refs

    def __getitem__(self, k):
        return self.refs[k][...]


def second_inner_kernel(
    rin_ref, coef_ref, yd_ref, yu_ref, w_ref, d_ref, u_ref, a1_ref, h_ref, sin_ref, cb, r1,
):
    left, right, down, up = flags()
    for x in range(3, 9):
        h_ref[x - 3] = with_rows(w_ref[x - 1], 3, d_ref[x - 1], u_ref[x - 1], down, up)
    tiles = spread_coefs(
        cb, ((yd_ref[8], 4), (coef_ref[0], 0), (coef_ref[0], 4), (yu_ref[8], 0))
    )
    coefs = [Loaded(t) for t in tiles]
    get_h = lambda x, y, n: h_ref[x - 3, y : y + n]
    for k in range(4):
        p = 3 + k
        get_r = lambda y, n: get(rin_ref, p - 1, y, n)
        second_residual(get_h, get_r, coefs, p, k, r1, left, right, down, up)
        sin_ref[k] = forward(r1, k * 192, a1_ref)


def second_kernel(
    rin_ref, rout_ref, coef_ref, xl_ref, xr_ref, yd_ref, yu_ref, w_ref, l_ref, r_ref, d_ref, u_ref,
    hin_ref, sin_ref, a1_ref, a2_ref, lj_ref, lk_ref,
    c_ref, to_left_ref, to_right_ref, own_down_ref, own_up_ref, h, cb, r1, sout, spec, wout,
):
    left, right, down, up = flags()
    for x in (0, 1, 2, 9, 10, 11):
        if x == 0:
            g = l_ref[0] * left
        elif x == 11:
            g = r_ref[2] * right
        else:
            g = with_rows(w_ref[x - 1], 3, d_ref[x - 1], u_ref[x - 1], down, up)
            if x == 1:
                g = (g + l_ref[1]) * left
            elif x == 2:
                g = g + l_ref[2] * left
            elif x == 9:
                g = g + r_ref[0] * right
            elif x == 10:
                g = (g + r_ref[1]) * right
        h[x if x < 3 else x - 6] = g

    def get_h(x, y, n):
        if 3 <= x <= 8:
            return hin_ref[x - 3, y : y + n]
        return h[x if x < 3 else x - 6, y : y + n]

    coefs = []
    for a, x_ref in ((0, xl_ref), (1, None), (2, xr_ref)):
        if x_ref is None:
            rows = ((yd_ref[8], 4), (coef_ref[0], 0), (coef_ref[0], 4), (yu_ref[8], 0))
        else:
            rows = ((x_ref[19], 0), (x_ref[18], 0), (x_ref[18], 4), (x_ref[19], 4))
        coefs.append([Loaded(t) for t in spread_coefs(cb.at[a], rows)])
    layers = [None] * 3 + [(sin_ref, k) for k in range(4)] + [None] * 3
    for k, p in enumerate((0, 1, 2, 7, 8, 9)):
        if p in (0, 9):
            get_r = lambda y, n: get(rout_ref, 0 if p == 0 else 1, y, n)
        else:
            get_r = lambda y, n: get(rin_ref, p - 1, y, n)
        cb_p = coefs[0 if p == 0 else 2 if p == 9 else 1]
        second_residual(get_h, get_r, cb_p, p, k, r1, left, right, down, up)
        sout[k] = forward(r1, k * 192, a1_ref)
        layers[p] = (sout, k)
    finish_solves(layers, coef_ref, a2_ref, lj_ref, lk_ref, spec, wout)
    for p in range(10):
        line = get(wout, p, 0, 18)
        c_ref[p] = get_h(p + 1, 1, 18) + line
        if p < 2:
            to_left_ref[p] = line
        if p > 7:
            to_right_ref[p - 8] = line
        own_down_ref[p] = line[0:2]
        own_up_ref[p] = line[16:18]


def add_x(g, p, l, r, left, right):
    if p == 0:
        return (g + l[0]) * left
    if p == 1:
        return g + l[1] * left
    if p == 8:
        return g + r[0] * right
    if p == 9:
        return (g + r[1]) * right
    return g


def rows_of(tile, at):
    return [jnp.broadcast_to(tile[at + k : at + k + 1, :], (8, LANES)) for k in range(4)]


def stencil(cf, v, x_sum, y_sum):
    above, below = neighbours_z(v)
    two = v + v
    return (
        cf[0] * (two - x_sum) + cf[1] * (two - y_sum) + cf[2] * (two - above - below) + cf[3] * v
    )


def column_residual(get_h, src_ref, cf, x, b, mr_ref, at):
    lanes = slice(b * LANES, (b + 1) * LANES)
    for y in (0, 4):
        yy = b * 8 + y + 1
        p = x + 1
        v = get_h(p, yy, 4)
        res = src_ref[x, yy - 1 : yy + 3] - stencil(
            cf,
            v,
            get_h(p + 1, yy, 4) + get_h(p - 1, yy, 4),
            get_h(p, yy + 1, 4) + get_h(p, yy - 1, 4),
        )
        mr_ref[at, y * 8 : y * 8 + 32, lanes] = res.reshape(32, LANES)


def moments(wm_ref, x, rows):
    rh, rl = split(rows)
    w = wm_ref[:, x * 64 : x * 64 + rows.shape[0]]
    return dot(w, rh) + dot(w, rl)


def to_slots(uv, oh):
    hi, lo = split(uv)
    n = uv.shape[0]
    o = dot(jnp.concatenate([hi, lo], 0), oh)
    return o[:n] + o[n:]


def middle_inner_kernel(
    src_ref, coef_ref, yd_ref, yu_ref, c_ref, slot_ref, wm_ref,
    smooth_hbm, res_hbm, mr_ref, mom_ref, pick_ref, member_ref, h, smooth_ref, res_ref, sems,
):
    _, _, down, up = flags()
    oh = onehot(slot_ref[...])
    copies = []
    for x in range(1, 7):
        both = [c_ref[x + 1, 8 * b + 2 : 8 * b + 8].reshape(48, LANES) for b in range(2)]
        smooth_ref[x - 1] = to_slots(jnp.concatenate(both, 1), oh)
    copies.append(
        pltpu.make_async_copy(smooth_ref, smooth_hbm.at[pl.ds(1, 6), pl.ds(8, 48), :], sems.at[0])
    )
    copies[0].start()
    for k in range(6):
        h[k] = c_ref[k + 2]
        h[k, 0] = c_ref[k + 2, 0] * down
        h[k, 17] = c_ref[k + 2, 17] * up
    get_h = lambda p, y, n: h[p - 2, y : y + n]
    coefs = [rows_of(coef_ref[0], 0), rows_of(coef_ref[0], 4)]
    for k in range(4):
        for b in range(2):
            column_residual(get_h, src_ref, coefs[b], 2 + k, b, mr_ref, k)
        res_ref[k] = to_slots(mr_ref[k, 16:48, :], oh)
    copies.append(
        pltpu.make_async_copy(res_ref, res_hbm.at[pl.ds(2, 4), pl.ds(16, 32), :], sems.at[1])
    )
    copies[1].start()
    mom = jnp.zeros((16, 256), F32)
    for k in (0, 2):
        mom = mom + moments(wm_ref, 2 + k, mr_ref[k : k + 2].reshape(128, 256))
    mom_ref[...] = mom
    gr = coef_ref[1]
    group = jnp.concatenate([gr[0:1], gr[1:2], yd_ref[9, 1:2, :], yu_ref[9, 0:1, :]], 1)
    ny = pick_ref.shape[0]
    col = (group + 0.5).astype(jnp.int32) - lax.axis_index("sx") * (ny * GRP_DEV)
    owner = lax.shift_right_logical(col, 4)
    member = jnp.bitwise_and(col, 15)
    sel = lax.broadcasted_iota(jnp.int32, (ny, 512), 0)
    pick_ref[...] = jnp.where(sel == owner, 1.0, 0.0)
    sel = lax.broadcasted_iota(jnp.int32, (16, 512), 0)
    member_ref[...] = jnp.where(sel == member, 1.0, 0.0)
    for c in copies:
        c.wait()


def middle_kernel(
    src_ref, coef_ref, yd_ref, yu_ref, c_ref, l_ref, r_ref, own_down_ref, own_up_ref,
    mom_ref, pick_ref, member_ref, wm_ref, wr_ref,
    u_ref, mr_ref, to_down_ref, to_up_ref, part_ref, h, rim,
):
    left, right, down, up = flags()
    for p in range(10):
        e = add_x(own_down_ref[p], p, l_ref[:, 0:2], r_ref[:, 0:2], left, right)
        to_down_ref[p] = jnp.concatenate([e[0:1] * down, e[1:2]], 0)
        e = add_x(own_up_ref[p], p, l_ref[:, 16:18], r_ref[:, 16:18], left, right)
        to_up_ref[p] = jnp.concatenate([e[0:1], e[1:2] * up], 0)
        if 3 < p < 6:
            continue
        g = add_x(c_ref[p], p, l_ref, r_ref, left, right)
        h[p] = g
        h[p, 0] = g[0] * down
        h[p, 17] = g[17] * up
    u_ref[0] = h[1, 1:17]
    u_ref[1] = h[8, 1:17]
    get_h = lambda p, y, n: h[p, y : y + n]
    coefs = [rows_of(coef_ref[0], 0), rows_of(coef_ref[0], 4)]
    for k, x in enumerate((0, 1, 6, 7)):
        for b in range(2):
            column_residual(get_h, src_ref, coefs[b], x, b, mr_ref, k)
    rim[...] = jnp.zeros((256, 256), F32)
    for slab, far, near, tile, b, lanes, y_far, y_near in (
        (to_down_ref, 0, 1, yd_ref, 1, slice(0, LANES), 2, 3),
        (to_up_ref, 1, 0, yu_ref, 0, slice(LANES, 256), 1, 0),
    ):
        cf = rows_of(tile[8], b * 4)
        for x in range(8):
            p = x + 1
            v = slab[p, far : far + 1]
            res = stencil(
                cf,
                v,
                slab[p + 1, far : far + 1] + slab[p - 1, far : far + 1],
                slab[p, near : near + 1],
            )
            at = (x * 4 + y_near) * 8
            rim[at : at + 8, lanes] = -res[0]
            at = (x * 4 + y_far) * 8
            rim[at : at + 8, lanes] = cf[1] * v[0]
    mom = mom_ref[...]
    mom = mom + moments(wm_ref, 0, mr_ref[0:2].reshape(128, 256))
    mom = mom + moments(wm_ref, 6, mr_ref[2:4].reshape(128, 256))
    rh, rl = split(rim[...])
    mom_y = dot(wr_ref[...], rh) + dot(wr_ref[...], rl)
    mom_y = mom_y[0:8] + mom_y[8:16]
    mom = jnp.concatenate(
        [mom[0:8] + mom[8:16], mom_y[:, :LANES] * down, mom_y[:, LANES:] * up], 1
    )
    member = member_ref[...]
    spread = jnp.concatenate([member * mom[v : v + 1] for v in range(8)], 0)
    sh, sl = split(spread)
    pick = pick_ref[...].astype(BF16)
    part_ref[...] = dot_t(pick, sh) + dot_t(pick, sl)


def last_kernel(
    smooth_in, res_in, c_ref, uout_ref, rin_ref, rout_ref, coef_ref, d_ref, u_ref, slot_ref,
    arrived_ref,
    smooth_hbm, res_hbm, coarse_hbm, smooth_ref, res_ref, coarse_ref, sems,
):
    _, _, down, up = flags()
    total = jnp.sum(arrived_ref[...], axis=0, keepdims=True)
    for v in range(8):
        coarse_ref[v : v + 1, :] = total[:, v * GRP_DEV : (v + 1) * GRP_DEV]
    copies = [pltpu.make_async_copy(coarse_ref, coarse_hbm, sems.at[8])]
    copies[0].start()

    def send(ref, hbm, x, nx, row, rows):
        at = (pl.ds(x, nx), pl.ds(row, rows), slice(None))
        k = len(copies) - 1
        copies.append(pltpu.make_async_copy(ref.at[at], hbm.at[at], sems.at[k]))
        copies[-1].start()

    oh = onehot(slot_ref[...])
    sides = (
        (d_ref, down, 0, 1, rows_of(coef_ref[0], 0)),
        (u_ref, up, 1, 0, rows_of(coef_ref[0], 4)),
    )

    def added(x):
        out = []
        for slab, on, far, near, cf in sides:
            p = x + 1
            v = slab[p, near : near + 1] * on
            x_sum = (slab[p + 1, near : near + 1] + slab[p - 1, near : near + 1]) * on
            res = stencil(cf, v, x_sum, slab[p, far : far + 1] * on)
            out.append((v[0], -res[0], cf[1] * v[0]))
        return out

    zero = jnp.zeros((8, LANES), F32)
    pairs = [added(x) for x in range(8)]
    for k, x in enumerate((0, 1, 6, 7)):
        (_, d0, d1), (_, e0, e1) = pairs[x]
        add = jnp.concatenate(
            [
                jnp.concatenate([d0, d1] + [zero] * 6, 0),
                jnp.concatenate([zero] * 6 + [e1, e0], 0),
            ],
            1,
        )
        res_ref[x] = to_slots(rout_ref[k] + add, oh)
        if k == 1:
            send(res_ref, res_hbm, 0, 2, 0, 64)
    send(res_ref, res_hbm, 6, 2, 0, 64)
    low, high = [], []
    for k in range(4):
        (_, d0, d1), (_, e0, e1) = pairs[2 + k]
        z2 = jnp.zeros((16, LANES), F32)
        low.append(
            rin_ref[k, 0:16, :] + jnp.concatenate([jnp.concatenate([d0, d1], 0), z2], 1)
        )
        high.append(
            rin_ref[k, 48:64, :] + jnp.concatenate([z2, jnp.concatenate([e1, e0], 0)], 1)
        )
    res_ref[2:6, 0:16, :] = to_slots(jnp.concatenate(low, 0), oh).reshape(4, 16, 256)
    send(res_ref, res_hbm, 2, 4, 0, 16)
    res_ref[2:6, 48:64, :] = to_slots(jnp.concatenate(high, 0), oh).reshape(4, 16, 256)
    send(res_ref, res_hbm, 2, 4, 48, 16)
    for k, x in enumerate((0, 7)):
        (d0, _, _), (e0, _, _) = pairs[x]
        both = [uout_ref[k, 0:8].reshape(64, LANES), uout_ref[k, 8:16].reshape(64, LANES)]
        both[0] = both[0] + jnp.concatenate([d0] + [zero] * 7, 0)
        both[1] = both[1] + jnp.concatenate([zero] * 7 + [e0], 0)
        smooth_ref[x] = to_slots(jnp.concatenate(both, 1), oh)
        send(smooth_ref, smooth_hbm, x, 1, 0, 64)
    low, high = [], []
    for x in range(1, 7):
        (d0, _, _), (e0, _, _) = pairs[x]
        c = [c_ref[x + 1, y] for y in (1, 9, 8, 16)]
        low.append(jnp.concatenate([c[0] + d0, c[1]], 1))
        high.append(jnp.concatenate([c[2], c[3] + e0], 1))
    smooth_ref[1:7, 0:8, :] = to_slots(jnp.concatenate(low, 0), oh).reshape(6, 8, 256)
    send(smooth_ref, smooth_hbm, 1, 6, 0, 8)
    smooth_ref[1:7, 56:64, :] = to_slots(jnp.concatenate(high, 0), oh).reshape(6, 8, 256)
    send(smooth_ref, smooth_hbm, 1, 6, 56, 8)
    for c in copies:
        c.wait()


def sd(*shape):
    return jax.ShapeDtypeStruct(shape, F32)


def vm(*shape):
    return pltpu.VMEM(shape, F32)


def ring(value, axis, by):
    n = lax.axis_size(axis)
    return lax.ppermute(value, axis, [(i, (i + by) % n) for i in range(n)])


def call(kernel, outs, args, scratch=(), hbm_in=0, hbm_out=0, sems=0, alias=0):
    vmem = pl.BlockSpec(memory_space=pltpu.VMEM)
    hbm = pl.BlockSpec(memory_space=pltpu.HBM)
    args = [
        pltpu.with_memory_space_constraint(a, pltpu.HBM if k < hbm_in else pltpu.VMEM)
        for k, a in enumerate(args)
    ]
    scratch = [pltpu.VMEM(s, F32) if isinstance(s, tuple) else s for s in scratch]
    if sems:
        scratch.append(pltpu.SemaphoreType.DMA((sems,)))
    return pl.pallas_call(
        kernel,
        out_shape=outs,
        in_specs=[hbm if k < hbm_in else vmem for k in range(len(args))],
        out_specs=[hbm if k < hbm_out else vmem for k in range(len(outs))],
        scratch_shapes=scratch,
        input_output_aliases={k: k for k in range(alias)},
        compiler_params=pltpu.CompilerParams(vmem_limit_bytes=16 << 20),
    )(*args)


def on_device(right_side, stretch, mass_term, slot_position, coarse_group):
    a1 = jnp.asarray(A_FWD, BF16)
    a2 = jnp.asarray(A_BWD, BF16)
    lj = jnp.asarray(LAM_J, F32)
    lk = jnp.asarray(LAM_K, F32)
    wm = jnp.asarray(W_MOM, BF16)
    wr = jnp.asarray(W_RIM, BF16)
    row = pltpu.VMEM((1, 256), jnp.int32)
    rhs = right_side.reshape(8, 64, 256)
    coef, to_d, to_u, slot = call(
        start_kernel,
        [vm(2, 8, LANES), vm(10, 8, LANES), vm(10, 8, LANES), row],
        (
            rhs,
            stretch,
            mass_term.reshape(1, 256),
            slot_position.reshape(1, 256),
            coarse_group.reshape(1, 256),
        ),
        [(2, 8, 8, 256), (3, 256), (1, 256), row],
        hbm_in=5,
        sems=6,
    )
    yd = ring(to_u, "sy", 1)
    yu = ring(to_d, "sy", -1)
    src = call(
        place_kernel, [vm(8, 16, 8, LANES)], (rhs, slot), [(8, 64, 256)], hbm_in=1, sems=8
    )[0]
    to_l, to_r = call(rim_kernel, [vm(20, 8, LANES)] * 2, (src, coef, yd, yu))
    xl = ring(to_r, "sx", 1)
    xr = ring(to_l, "sx", -1)
    rin, sin = call(
        first_inner_kernel, [vm(8 * 192, LANES), vm(8, 104, 256)], (src, yd, yu, a1)
    )

    side = vm(10, 3, 8, LANES)
    rout, w, to_d, to_u = call(
        first_kernel,
        [vm(2 * 192, LANES), vm(10, 18, 8, LANES), side, side],
        (coef, xl, xr, sin, a1, a2, lj, lk),
        [(2, 104, 256), (10, 104, 256), (1920, LANES)],
    )
    d = ring(to_u, "sy", 1)
    u = ring(to_d, "sy", -1)
    to_l, to_r = call(edge_kernel, [vm(3, 20, 8, LANES)] * 2, (w, d, u))
    l = ring(to_r, "sx", 1)
    r = ring(to_l, "sx", -1)
    hin, sin = call(
        second_inner_kernel,
        [vm(6, 20, 8, LANES), vm(4, 104, 256)],
        (rin, coef, yd, yu, w, d, u, a1),
        [(4, 4, 8, LANES), (4 * 192, LANES)],
    )

    slab = vm(2, 18, 8, LANES)
    side = vm(10, 2, 8, LANES)
    c, to_l, to_r, own_d, own_u = call(
        second_kernel,
        [vm(10, 18, 8, LANES), slab, slab, side, side],
        (rin, rout, coef, xl, xr, yd, yu, w, l, r, d, u, hin, sin, a1, a2, lj, lk),
        [
            (6, 20, 8, LANES),
            (3, 4, 4, 8, LANES),
            (6 * 192, LANES),
            (6, 104, 256),
            (10, 104, 256),
            (1920, LANES),
        ],
    )
    l = ring(to_r, "sx", 1)
    r = ring(to_l, "sx", -1)
    ny = lax.axis_size("sy")
    smooth, res, rin, mom, pick, member = call(
        middle_inner_kernel,
        [sd(8, 64, 256), sd(8, 64, 256), vm(4, 64, 256), vm(16, 256), vm(ny, 512), vm(16, 512)],
        (src, coef, yd, yu, c, slot, wm),
        [(6, 18, 8, LANES), (6, 48, 256), (4, 32, 256)],
        hbm_out=2,
        sems=2,
    )
    uout, rout, to_d, to_u, part = call(
        middle_kernel,
        [vm(2, 16, 8, LANES), vm(4, 64, 256), side, side, vm(ny, LANES)],
        (src, coef, yd, yu, c, l, r, own_d, own_u, mom, pick, member, wm, wr),
        [(10, 18, 8, LANES), (256, 256)],
    )
    d = ring(to_u, "sy", 1)
    u = ring(to_d, "sy", -1)
    arrived = lax.all_to_all(part, "sy", split_axis=0, concat_axis=0, tiled=True)
    smooth, res, coarse = call(
        last_kernel,
        [sd(8, 64, 256), sd(8, 64, 256), sd(8, GRP_DEV)],
        (smooth, res, c, uout, rin, rout, coef, d, u, slot, arrived),
        [(8, 64, 256), (8, 64, 256), (8, GRP_DEV)],
        hbm_in=2,
        hbm_out=3,
        sems=9,
        alias=2,
    )
    return smooth.reshape(8, 8, 8, 256), res.reshape(8, 8, 8, 256), coarse


def solution(mesh):
    split_all = P(None, None, None, ("sx", "sy"))
    flat = P(("sx", "sy"))
    return jax.shard_map(
        on_device,
        mesh=mesh,
        in_specs=(split_all, P(None, ("sx", "sy")), flat, flat, flat),
        out_specs=(split_all, split_all, P(None, ("sx", "sy"))),
        check_vma=False,
    )
```

```python
import jax
import jax.numpy as jnp
import numpy as np
from jax import lax
from jax.experimental import pallas as pl
from jax.experimental.pallas import tpu as pltpu
from jax.sharding import PartitionSpec as P

NODES = 8
GRP_DEV = 16
LANES = 128
RELAX = 0.35
F32 = jnp.float32
BF16 = jnp.bfloat16


def split_np(a):
    a = np.asarray(a, np.float32)
    hi = np.asarray(jnp.asarray(a).astype(BF16).astype(F32))
    return hi, a - hi


def constants():
    n = NODES + 2
    col = np.arange(n, dtype=np.float64) + 1.0
    s = np.sqrt(2.0 / (n + 1.0)) * np.sin(np.pi * col[:, None] * col[None, :] / (n + 1.0))
    lam = 2.0 - 2.0 * np.cos(np.pi * col / (n + 1.0))
    fwd = np.zeros((104, 112))
    for q in range(n):
        for r in range(n):
            c = q * 8 + r - 1
            if r == 0:
                c = 80 + q
            if r == n - 1:
                c = 96 + q
            fwd[:100, c] = np.outer(s[:, q], s[:, r]).reshape(-1)
    fh, fl = split_np(fwd)
    a1 = np.concatenate([np.concatenate([fh, fh], 1), np.concatenate([fl, fl], 1)], 0)
    bh, bl = split_np(RELAX * fwd.T)
    a2 = np.concatenate([np.concatenate([bh, bh], 1), np.concatenate([bl, bl], 1)], 0)
    lam_j = np.ones((104, LANES), np.float32)
    lam_k = np.ones((104, LANES), np.float32)
    lam_j[:100] = np.repeat(lam, n)[:, None]
    lam_k[:100] = np.tile(lam, n)[:, None]
    t = np.arange(NODES) / (NODES - 1.0)
    w = np.stack([1.0 - t, t])
    wm = np.einsum("ax,by,cz->abcxyz", w, w, w).reshape(8, 512)
    wh, wl = split_np(wm)
    wm = np.concatenate([wh, wl], 0)
    rim = wm.reshape(16, 8, 8, 8)[:, :, [0, 1, 6, 7]].reshape(16, 256)
    return s, lam, a1, a2, lam_j, lam_k, wm, rim


SINES, LAM, A_FWD, A_BWD, LAM_J, LAM_K, W_MOM, W_RIM = constants()


def split(x):
    hi = x.astype(BF16)
    return hi, (x - hi.astype(F32)).astype(BF16)


def dot(a, b):
    return lax.dot_general(a, b, (((1,), (0,)), ((), ())), preferred_element_type=F32)


def dot_t(a, b):
    return lax.dot_general(a, b, (((1,), (1,)), ((), ())), preferred_element_type=F32)


def flags():
    i = lax.axis_index("sx")
    j = lax.axis_index("sy")
    nx = lax.axis_size("sx")
    ny = lax.axis_size("sy")
    one = lambda c: jnp.where(c, 1.0, 0.0).astype(F32)
    return one(i > 0), one(i < nx - 1), one(j > 0), one(j < ny - 1)


def lane_up(x):
    lane = lax.broadcasted_iota(jnp.int32, x.shape, x.ndim - 1)
    return jnp.where(lane == LANES - 1, 0.0, pltpu.roll(x, LANES - 1, x.ndim - 1))


def lane_down(x):
    lane = lax.broadcasted_iota(jnp.int32, x.shape, x.ndim - 1)
    return jnp.where(lane == 0, 0.0, pltpu.roll(x, 1, x.ndim - 1))


def onehot(slot_row):
    p = lax.broadcasted_iota(jnp.int32, (256, 256), 0)
    return jnp.where(p == slot_row, 1.0, 0.0).astype(BF16)


def split3(a):
    a1 = a.astype(BF16)
    e = a - a1.astype(F32)
    a2 = e.astype(BF16)
    return a1, a2, (e - a2.astype(F32)).astype(BF16)


def start_kernel(
    rhs_hbm, stretch_hbm, mass_hbm, slot_hbm, group_hbm,
    coef_ref, to_down_ref, to_up_ref, slot_ref,
    face_ref, stretch_ref, mass_ref, group_ref, sems,
):
    pairs = (
        (slot_hbm, slot_ref),
        (rhs_hbm.at[:, pl.ds(0, 8), :], face_ref.at[0]),
        (rhs_hbm.at[:, pl.ds(56, 8), :], face_ref.at[1]),
        (stretch_hbm, stretch_ref),
        (mass_hbm, mass_ref),
        (group_hbm, group_ref),
    )
    copies = [pltpu.make_async_copy(h, v, sems.at[k]) for k, (h, v) in enumerate(pairs)]
    for c in copies:
        c.start()
    copies[0].wait()
    oh = onehot(slot_ref[...])
    for k, out, b in ((1, to_down_ref, 0), (2, to_up_ref, 1)):
        copies[k].wait()
        g = dot_t(jnp.concatenate(split3(face_ref[k - 1].reshape(64, 256)), 0), oh)
        g = g[0:64] + g[64:128] + g[128:192]
        out[0:8] = g[:, b * LANES : (b + 1) * LANES].reshape(8, 8, LANES)
    for c in copies[3:]:
        c.wait()
    c = jnp.concatenate(
        [
            stretch_ref[...],
            mass_ref[...],
            group_ref[...].astype(F32),
            jnp.zeros((3, 256), F32),
        ],
        0,
    )
    c1, c2, c3 = split3(c)
    cg = dot_t(c1, oh) + dot_t(c2, oh) + dot_t(c3, oh)
    coef = jnp.concatenate([cg[0:4, :LANES], cg[0:4, LANES:]], 0)
    gr = jnp.concatenate([cg[4:5, :LANES], cg[4:5, LANES:], jnp.zeros((6, LANES), F32)], 0)
    coef_ref[0] = coef
    coef_ref[1] = gr
    for out in (to_down_ref, to_up_ref):
        out[8] = coef
        out[9] = gr


def place_kernel(
    rhs_hbm, lam_hbm, slot_ref, coef_ref, src_ref, dinv_ref, rhs_ref, lam_ref, sems
):
    copies = [
        pltpu.make_async_copy(rhs_hbm.at[x], rhs_ref.at[x], sems.at[x]) for x in range(8)
    ]
    lam = pltpu.make_async_copy(lam_hbm, lam_ref, sems.at[8])
    lam.start()
    for c in copies:
        c.start()
    oh = onehot(slot_ref[...])
    lam.wait()
    for b in range(2):
        lanes = slice(b * LANES, (b + 1) * LANES)
        cx, cy, cz, m = rows_of(coef_ref[0], b * 4)
        cxl = [cx * float(v) for v in LAM]
        for t in range(13):
            row = slice(t * 8, t * 8 + 8)
            d0 = cy * lam_ref[0, row, :] + cz * lam_ref[1, row, :] + m
            for i in range(10):
                dinv_ref[i, row, lanes] = 1.0 / (d0 + cxl[i])
    for x in range(8):
        copies[x].wait()
        g = dot_t(jnp.concatenate(split3(rhs_ref[x]), 0), oh)
        g = g[0:64] + g[64:128] + g[128:192]
        for b in range(2):
            src_ref[x, b * 8 : b * 8 + 8] = g[:, b * LANES : (b + 1) * LANES].reshape(8, 8, LANES)


def rim_kernel(src_ref, coef_ref, yd_ref, yu_ref, to_left_ref, to_right_ref):
    coef_y = jnp.concatenate([yd_ref[8, 4:8, :], yu_ref[8, 0:4, :]], 0)
    for x, out in ((0, to_left_ref), (7, to_right_ref)):
        out[0] = yd_ref[x]
        out[1:17] = src_ref[x]
        out[17] = yu_ref[x]
        out[18] = coef_ref[0]
        out[19] = coef_y


def forward(res, base, a1_ref):
    ends = []
    for z, shift in ((7, lane_down), (0, lane_up)):
        ends.append([shift(res[pl.ds(base + 64 * t + z, 8, stride=8), :]) for t in range(3)])
    halves = [
        jnp.concatenate(
            [res[base + 64 * b : base + 64 * b + 80, :]] + ends[0][b : b + 2] + ends[1][b : b + 2],
            0,
        )
        for b in range(2)
    ]
    hi, lo = split(jnp.concatenate(halves, 1))
    r = dot(a1_ref[...], jnp.concatenate([hi, lo], 0))
    return r[:104] + r[104:]


def along_x(layers, partial, row, lanes):
    acc = [None if partial is None else partial[i, row, lanes] for i in range(10)]
    for p, (low, high) in layers.items():
        v = low[0][low[1], row, lanes]
        w = high[0][high[1], row, lanes]
        h = (v + w, v - w)
        for i in range(10):
            term = h[i % 2] * float(SINES[i, p])
            acc[i] = term if acc[i] is None else acc[i] + term
    return acc


def partial_x(layers, out_ref):
    for b in range(2):
        lanes = slice(b * LANES, (b + 1) * LANES)

        def chunk(t, carry):
            row = pl.ds(pl.multiple_of(t * 8, 8), 8)
            for i, v in enumerate(along_x(layers, None, row, lanes)):
                out_ref[i, row, lanes] = v
            return carry

        lax.fori_loop(0, 13, chunk, 0)


def finish_solves(layers, partial, dinv_ref, a2_ref, spec, wout):
    for b in range(2):
        lanes = slice(b * LANES, (b + 1) * LANES)

        def chunk(t, carry):
            row = pl.ds(pl.multiple_of(t * 8, 8), 8)
            z = along_x(layers, partial, row, lanes)
            z = [z[i] * dinv_ref[i, row, lanes] for i in range(10)]
            for p in range(5):
                e = z[0] * float(SINES[0, p])
                o = z[1] * float(SINES[1, p])
                for i in range(2, 10, 2):
                    e = e + z[i] * float(SINES[i, p])
                    o = o + z[i + 1] * float(SINES[i + 1, p])
                spec[p, row, lanes] = e + o
                spec[9 - p, row, lanes] = e - o
            return carry

        lax.fori_loop(0, 13, chunk, 0)

    for p in range(10):
        base = p * 192
        hi, lo = split(spec[p])
        r = dot(a2_ref[...], jnp.concatenate([hi, lo], 0))
        r = r[:112] + r[112:]
        r0 = r[:, :LANES]
        r1 = r[:, LANES:]
        wout[base : base + 64, :] = r0[0:64]
        wout[base + 64 : base + 80, :] = r0[64:80] + r1[0:16]
        wout[base + 80 : base + 144, :] = r1[16:80]
        wout[base + 144 : base + 192, :] = jnp.zeros((48, LANES), F32)
        for off, z, shift in ((80, 7, lane_up), (96, 0, lane_down)):
            rows = [
                r0[off : off + 8],
                r0[off + 8 : off + 16] + r1[off : off + 8],
                r1[off + 8 : off + 16],
            ]
            for t in range(3):
                at = pl.ds(base + 64 * t + z, 8, stride=8)
                wout[at, :] = wout[at, :] + shift(rows[t])


def put(ref, p, y, value):
    n = value.shape[0]
    at = (p * 24 + y) * 8
    ref[at : at + n * 8, :] = value.reshape(n * 8, LANES)


def get(ref, p, y, n):
    at = (p * 24 + y) * 8
    return ref[at : at + n * 8, :].reshape(n, 8, LANES)


def with_rows(line, n, d, u, down, up):
    rows_d = d * down
    rows_u = u * up
    low = rows_d[n - 2 : n] + jnp.concatenate([line[0:1] * down, line[1:2]], 0)
    high = rows_u[0:2] + jnp.concatenate([line[16:17], line[17:18] * up], 0)
    parts = [low, line[2:16], high]
    if n > 2:
        parts = [rows_d[0 : n - 2]] + parts + [rows_u[2:n]]
    return jnp.concatenate(parts, 0)


def put_layer(ref, at, below, line, above):
    put(ref, at, 0, below)
    put(ref, at, 1, line)
    put(ref, at, 17, above)
    put(ref, at, 18, jnp.zeros((6, 8, LANES), F32))


def first_inner_kernel(src_ref, yd_ref, yu_ref, a1_ref, rin_ref, sin_ref, sout):
    _, _, down, up = flags()
    for x in range(8):
        put_layer(rin_ref, x, yd_ref[x : x + 1] * down, src_ref[x], yu_ref[x : x + 1] * up)
        sout[x] = forward(rin_ref, x * 192, a1_ref)
    partial_x({p: ((sout, p - 1), (sout, 8 - p)) for p in range(1, 5)}, sin_ref)


def first_kernel(
    xl_ref, xr_ref, sin_ref, dinv_ref, a1_ref, a2_ref,
    rout_ref, w_ref, to_down_ref, to_up_ref, sout, spec, wout,
):
    left, right, down, up = flags()
    for k, (x_ref, side) in enumerate(((xl_ref, left), (xr_ref, right))):
        put_layer(
            rout_ref,
            k,
            x_ref[0:1] * (side * down),
            x_ref[1:17] * side,
            x_ref[17:18] * (side * up),
        )
        sout[k] = forward(rout_ref, k * 192, a1_ref)
    finish_solves({0: ((sout, 0), (sout, 1))}, sin_ref, dinv_ref, a2_ref, spec, wout)
    for p in range(10):
        line = get(wout, p, 0, 18)
        w_ref[p] = line
        to_down_ref[p] = line[0:3]
        to_up_ref[p] = line[15:18]


def edge_kernel(w_ref, d_ref, u_ref, to_left_ref, to_right_ref):
    _, _, down, up = flags()
    for k in range(3):
        for p, out in ((k, to_left_ref), (7 + k, to_right_ref)):
            out[k] = with_rows(w_ref[p], 3, d_ref[p], u_ref[p], down, up)


def neighbours_z(u):
    z = lax.broadcasted_iota(jnp.int32, u.shape, 1)
    s = pltpu.roll(u, 7, 1)
    above = jnp.where(z == 7, lane_up(s), s)
    s = pltpu.roll(u, 1, 1)
    below = jnp.where(z == 0, lane_down(s), s)
    return above, below


ROWS = ((0, 1, 0), (1, 4, 1), (5, 4, 1), (9, 4, 2), (13, 4, 2), (17, 1, 3))


def second_residual(get_h, get_r, cb, p, at, res_ref, left, right, down, up):
    for y, n, b in ROWS:
        v = get_h(p + 1, y + 1, n)
        res = get_r(y, n) - stencil(
            cb[b],
            v,
            get_h(p + 2, y + 1, n) + get_h(p, y + 1, n),
            get_h(p + 1, y + 2, n) + get_h(p + 1, y, n),
        )
        if p == 0:
            res = res * left
        if p == 9:
            res = res * right
        if y == 0:
            res = res * down
        if y == 17:
            res = res * up
        put(res_ref, at, y, res)
    put(res_ref, at, 18, jnp.zeros((6, 8, LANES), F32))


def spread_coefs(cb, rows):
    for b, (tile, at) in enumerate(rows):
        for k, v in enumerate(rows_of(tile, at)):
            cb[b, k] = v
    return [[cb.at[b, k] for k in range(4)] for b in range(4)]


class Loaded:
    def __init__(self, refs):
        self.refs = refs

    def __getitem__(self, k):
        return self.refs[k][...]


def second_inner_kernel(
    rin_ref, coef_ref, yd_ref, yu_ref, w_ref, d_ref, u_ref, a1_ref, h_ref, sin_ref, cb, r1, sout,
):
    left, right, down, up = flags()
    for x in range(3, 9):
        h_ref[x - 3] = with_rows(w_ref[x - 1], 3, d_ref[x - 1], u_ref[x - 1], down, up)
    tiles = spread_coefs(
        cb, ((yd_ref[8], 4), (coef_ref[0], 0), (coef_ref[0], 4), (yu_ref[8], 0))
    )
    coefs = [Loaded(t) for t in tiles]
    get_h = lambda x, y, n: h_ref[x - 3, y : y + n]
    for k in range(4):
        p = 3 + k
        get_r = lambda y, n: get(rin_ref, p - 1, y, n)
        second_residual(get_h, get_r, coefs, p, k, r1, left, right, down, up)
        sout[k] = forward(r1, k * 192, a1_ref)
    partial_x({p: ((sout, p - 3), (sout, 6 - p)) for p in (3, 4)}, sin_ref)


def second_kernel(
    rin_ref, rout_ref, coef_ref, xl_ref, xr_ref, yd_ref, yu_ref, w_ref, l_ref, r_ref, d_ref, u_ref,
    hin_ref, sin_ref, dinv_ref, a1_ref, a2_ref,
    c_ref, to_left_ref, to_right_ref, own_down_ref, own_up_ref, h, cb, r1, sout, spec, wout,
):
    left, right, down, up = flags()
    for x in (0, 1, 2, 9, 10, 11):
        if x == 0:
            g = l_ref[0] * left
        elif x == 11:
            g = r_ref[2] * right
        else:
            g = with_rows(w_ref[x - 1], 3, d_ref[x - 1], u_ref[x - 1], down, up)
            if x == 1:
                g = (g + l_ref[1]) * left
            elif x == 2:
                g = g + l_ref[2] * left
            elif x == 9:
                g = g + r_ref[0] * right
            elif x == 10:
                g = (g + r_ref[1]) * right
        h[x if x < 3 else x - 6] = g

    def get_h(x, y, n):
        if 3 <= x <= 8:
            return hin_ref[x - 3, y : y + n]
        return h[x if x < 3 else x - 6, y : y + n]

    coefs = []
    for a, x_ref in ((0, xl_ref), (1, None), (2, xr_ref)):
        if x_ref is None:
            rows = ((yd_ref[8], 4), (coef_ref[0], 0), (coef_ref[0], 4), (yu_ref[8], 0))
        else:
            rows = ((x_ref[19], 0), (x_ref[18], 0), (x_ref[18], 4), (x_ref[19], 4))
        coefs.append([Loaded(t) for t in spread_coefs(cb.at[a], rows)])
    for k, p in enumerate((0, 1, 2, 7, 8, 9)):
        if p in (0, 9):
            get_r = lambda y, n: get(rout_ref, 0 if p == 0 else 1, y, n)
        else:
            get_r = lambda y, n: get(rin_ref, p - 1, y, n)
        cb_p = coefs[0 if p == 0 else 2 if p == 9 else 1]
        second_residual(get_h, get_r, cb_p, p, k, r1, left, right, down, up)
        sout[k] = forward(r1, k * 192, a1_ref)
    layers = {p: ((sout, p), (sout, 5 - p)) for p in range(3)}
    finish_solves(layers, sin_ref, dinv_ref, a2_ref, spec, wout)
    for p in range(10):
        line = get(wout, p, 0, 18)
        c_ref[p] = get_h(p + 1, 1, 18) + line
        if p < 2:
            to_left_ref[p] = line
        if p > 7:
            to_right_ref[p - 8] = line
        own_down_ref[p] = line[0:2]
        own_up_ref[p] = line[16:18]


def add_x(g, p, l, r, left, right):
    if p == 0:
        return (g + l[0]) * left
    if p == 1:
        return g + l[1] * left
    if p == 8:
        return g + r[0] * right
    if p == 9:
        return (g + r[1]) * right
    return g


def rows_of(tile, at):
    return [jnp.broadcast_to(tile[at + k : at + k + 1, :], (8, LANES)) for k in range(4)]


def stencil(cf, v, x_sum, y_sum):
    above, below = neighbours_z(v)
    two = v + v
    return (
        cf[0] * (two - x_sum) + cf[1] * (two - y_sum) + cf[2] * (two - above - below) + cf[3] * v
    )


def column_residual(get_h, src_ref, cf, x, b, mr_ref, at):
    lanes = slice(b * LANES, (b + 1) * LANES)
    for y in (0, 4):
        yy = b * 8 + y + 1
        p = x + 1
        v = get_h(p, yy, 4)
        res = src_ref[x, yy - 1 : yy + 3] - stencil(
            cf,
            v,
            get_h(p + 1, yy, 4) + get_h(p - 1, yy, 4),
            get_h(p, yy + 1, 4) + get_h(p, yy - 1, 4),
        )
        mr_ref[at, y * 8 : y * 8 + 32, lanes] = res.reshape(32, LANES)


def moments(wm_ref, x, rows):
    rh, rl = split(rows)
    w = wm_ref[:, x * 64 : x * 64 + rows.shape[0]]
    return dot(w, rh) + dot(w, rl)


def to_slots(uv, oh):
    hi, lo = split(uv)
    n = uv.shape[0]
    o = dot(jnp.concatenate([hi, lo], 0), oh)
    return o[:n] + o[n:]


def middle_inner_kernel(
    src_ref, coef_ref, yd_ref, yu_ref, c_ref, slot_ref, wm_ref,
    smooth_hbm, res_hbm, mr_ref, mom_ref, pick_ref, member_ref, h, smooth_ref, res_ref, sems,
):
    _, _, down, up = flags()
    oh = onehot(slot_ref[...])
    copies = []
    for x in range(1, 7):
        both = [c_ref[x + 1, 8 * b + 2 : 8 * b + 8].reshape(48, LANES) for b in range(2)]
        smooth_ref[x - 1] = to_slots(jnp.concatenate(both, 1), oh)
    copies.append(
        pltpu.make_async_copy(smooth_ref, smooth_hbm.at[pl.ds(1, 6), pl.ds(8, 48), :], sems.at[0])
    )
    copies[0].start()
    for k in range(6):
        h[k] = c_ref[k + 2]
        h[k, 0] = c_ref[k + 2, 0] * down
        h[k, 17] = c_ref[k + 2, 17] * up
    get_h = lambda p, y, n: h[p - 2, y : y + n]
    coefs = [rows_of(coef_ref[0], 0), rows_of(coef_ref[0], 4)]
    for k in range(4):
        for b in range(2):
            column_residual(get_h, src_ref, coefs[b], 2 + k, b, mr_ref, k)
        res_ref[k] = to_slots(mr_ref[k, 16:48, :], oh)
    copies.append(
        pltpu.make_async_copy(res_ref, res_hbm.at[pl.ds(2, 4), pl.ds(16, 32), :], sems.at[1])
    )
    copies[1].start()
    mom = jnp.zeros((16, 256), F32)
    for k in (0, 2):
        mom = mom + moments(wm_ref, 2 + k, mr_ref[k : k + 2].reshape(128, 256))
    mom_ref[...] = mom
    gr = coef_ref[1]
    group = jnp.concatenate([gr[0:1], gr[1:2], yd_ref[9, 1:2, :], yu_ref[9, 0:1, :]], 1)
    ny = pick_ref.shape[0]
    col = (group + 0.5).astype(jnp.int32) - lax.axis_index("sx") * (ny * GRP_DEV)
    owner = lax.shift_right_logical(col, 4)
    member = jnp.bitwise_and(col, 15)
    sel = lax.broadcasted_iota(jnp.int32, (ny, 512), 0)
    pick_ref[...] = jnp.where(sel == owner, 1.0, 0.0)
    sel = lax.broadcasted_iota(jnp.int32, (16, 512), 0)
    member_ref[...] = jnp.where(sel == member, 1.0, 0.0)
    for c in copies:
        c.wait()


def middle_kernel(
    src_ref, coef_ref, yd_ref, yu_ref, c_ref, l_ref, r_ref, own_down_ref, own_up_ref,
    mom_ref, pick_ref, member_ref, wm_ref, wr_ref,
    u_ref, mr_ref, to_down_ref, to_up_ref, part_ref, h, rim, edge,
):
    left, right, down, up = flags()
    for p in range(10):
        e = add_x(own_down_ref[p], p, l_ref[:, 0:2], r_ref[:, 0:2], left, right)
        edge[0, p] = jnp.concatenate([e[0:1] * down, e[1:2]], 0)
        e = add_x(own_up_ref[p], p, l_ref[:, 16:18], r_ref[:, 16:18], left, right)
        edge[1, p] = jnp.concatenate([e[0:1], e[1:2] * up], 0)
        if 3 < p < 6:
            continue
        g = add_x(c_ref[p], p, l_ref, r_ref, left, right)
        h[p] = g
        h[p, 0] = g[0] * down
        h[p, 17] = g[17] * up
    u_ref[0] = h[1, 1:17]
    u_ref[1] = h[8, 1:17]
    get_h = lambda p, y, n: h[p, y : y + n]
    coefs = [rows_of(coef_ref[0], 0), rows_of(coef_ref[0], 4)]
    for k, x in enumerate((0, 1, 6, 7)):
        for b in range(2):
            column_residual(get_h, src_ref, coefs[b], x, b, mr_ref, k)
    rim[...] = jnp.zeros((256, 256), F32)
    for k, out, far, near, tile, b, lanes, y_far, y_near in (
        (0, to_down_ref, 0, 1, yd_ref, 1, slice(0, LANES), 2, 3),
        (1, to_up_ref, 1, 0, yu_ref, 0, slice(LANES, 256), 1, 0),
    ):
        slab = edge.at[k]
        cf = rows_of(tile[8], b * 4)
        for x in range(8):
            p = x + 1
            v = slab[p, far : far + 1]
            res = stencil(
                cf,
                v,
                slab[p + 1, far : far + 1] + slab[p - 1, far : far + 1],
                slab[p, near : near + 1],
            )
            out[0, x] = v[0]
            out[1, x] = -res[0]
            at = (x * 4 + y_near) * 8
            rim[at : at + 8, lanes] = -res[0]
            at = (x * 4 + y_far) * 8
            rim[at : at + 8, lanes] = cf[1] * v[0]
    mom = mom_ref[...]
    mom = mom + moments(wm_ref, 0, mr_ref[0:2].reshape(128, 256))
    mom = mom + moments(wm_ref, 6, mr_ref[2:4].reshape(128, 256))
    rh, rl = split(rim[...])
    mom_y = dot(wr_ref[...], rh) + dot(wr_ref[...], rl)
    mom_y = mom_y[0:8] + mom_y[8:16]
    mom = jnp.concatenate(
        [mom[0:8] + mom[8:16], mom_y[:, :LANES] * down, mom_y[:, LANES:] * up], 1
    )
    member = member_ref[...]
    spread = jnp.concatenate([member * mom[v : v + 1] for v in range(8)], 0)
    sh, sl = split(spread)
    pick = pick_ref[...].astype(BF16)
    part_ref[...] = dot_t(pick, sh) + dot_t(pick, sl)


def last_kernel(
    smooth_in, res_in, c_ref, uout_ref, rin_ref, rout_ref, coef_ref, d_ref, u_ref, slot_ref,
    arrived_ref,
    smooth_hbm, res_hbm, coarse_hbm, smooth_ref, res_ref, coarse_ref, sems,
):
    _, _, down, up = flags()
    total = jnp.sum(arrived_ref[...], axis=0, keepdims=True)
    for v in range(8):
        coarse_ref[v : v + 1, :] = total[:, v * GRP_DEV : (v + 1) * GRP_DEV]
    copies = [pltpu.make_async_copy(coarse_ref, coarse_hbm, sems.at[8])]
    copies[0].start()

    def send(ref, hbm, x, nx, row, rows):
        at = (pl.ds(x, nx), pl.ds(row, rows), slice(None))
        k = len(copies) - 1
        copies.append(pltpu.make_async_copy(ref.at[at], hbm.at[at], sems.at[k]))
        copies[-1].start()

    oh = onehot(slot_ref[...])
    sides = (
        (d_ref, down, jnp.broadcast_to(coef_ref[0, 1:2, :], (8, LANES))),
        (u_ref, up, jnp.broadcast_to(coef_ref[0, 5:6, :], (8, LANES))),
    )

    def added(x):
        out = []
        for slab, on, cy in sides:
            v = slab[0, x] * on
            out.append((v, slab[1, x] * on, cy * v))
        return out

    zero = jnp.zeros((8, LANES), F32)
    pairs = [added(x) for x in range(8)]
    for k, x in enumerate((0, 1, 6, 7)):
        (_, d0, d1), (_, e0, e1) = pairs[x]
        add = jnp.concatenate(
            [
                jnp.concatenate([d0, d1] + [zero] * 6, 0),
                jnp.concatenate([zero] * 6 + [e1, e0], 0),
            ],
            1,
        )
        res_ref[x] = to_slots(rout_ref[k] + add, oh)
        if k == 1:
            send(res_ref, res_hbm, 0, 2, 0, 64)
    send(res_ref, res_hbm, 6, 2, 0, 64)
    low, high = [], []
    for k in range(4):
        (_, d0, d1), (_, e0, e1) = pairs[2 + k]
        z2 = jnp.zeros((16, LANES), F32)
        low.append(
            rin_ref[k, 0:16, :] + jnp.concatenate([jnp.concatenate([d0, d1], 0), z2], 1)
        )
        high.append(
            rin_ref[k, 48:64, :] + jnp.concatenate([z2, jnp.concatenate([e1, e0], 0)], 1)
        )
    res_ref[2:6, 0:16, :] = to_slots(jnp.concatenate(low, 0), oh).reshape(4, 16, 256)
    send(res_ref, res_hbm, 2, 4, 0, 16)
    res_ref[2:6, 48:64, :] = to_slots(jnp.concatenate(high, 0), oh).reshape(4, 16, 256)
    send(res_ref, res_hbm, 2, 4, 48, 16)
    for k, x in enumerate((0, 7)):
        (d0, _, _), (e0, _, _) = pairs[x]
        both = [uout_ref[k, 0:8].reshape(64, LANES), uout_ref[k, 8:16].reshape(64, LANES)]
        both[0] = both[0] + jnp.concatenate([d0] + [zero] * 7, 0)
        both[1] = both[1] + jnp.concatenate([zero] * 7 + [e0], 0)
        smooth_ref[x] = to_slots(jnp.concatenate(both, 1), oh)
        send(smooth_ref, smooth_hbm, x, 1, 0, 64)
    low, high = [], []
    for x in range(1, 7):
        (d0, _, _), (e0, _, _) = pairs[x]
        c = [c_ref[x + 1, y] for y in (1, 9, 8, 16)]
        low.append(jnp.concatenate([c[0] + d0, c[1]], 1))
        high.append(jnp.concatenate([c[2], c[3] + e0], 1))
    smooth_ref[1:7, 0:8, :] = to_slots(jnp.concatenate(low, 0), oh).reshape(6, 8, 256)
    send(smooth_ref, smooth_hbm, 1, 6, 0, 8)
    smooth_ref[1:7, 56:64, :] = to_slots(jnp.concatenate(high, 0), oh).reshape(6, 8, 256)
    send(smooth_ref, smooth_hbm, 1, 6, 56, 8)
    for c in copies:
        c.wait()


def sd(*shape):
    return jax.ShapeDtypeStruct(shape, F32)


def vm(*shape):
    return pltpu.VMEM(shape, F32)


def ring(value, axis, by):
    n = lax.axis_size(axis)
    return lax.ppermute(value, axis, [(i, (i + by) % n) for i in range(n)])


def call(kernel, outs, args, scratch=(), hbm_in=0, hbm_out=0, sems=0, alias=0):
    vmem = pl.BlockSpec(memory_space=pltpu.VMEM)
    hbm = pl.BlockSpec(memory_space=pltpu.HBM)
    args = [
        pltpu.with_memory_space_constraint(a, pltpu.HBM if k < hbm_in else pltpu.VMEM)
        for k, a in enumerate(args)
    ]
    scratch = [pltpu.VMEM(s, F32) if isinstance(s, tuple) else s for s in scratch]
    if sems:
        scratch.append(pltpu.SemaphoreType.DMA((sems,)))
    return pl.pallas_call(
        kernel,
        out_shape=outs,
        in_specs=[hbm if k < hbm_in else vmem for k in range(len(args))],
        out_specs=[hbm if k < hbm_out else vmem for k in range(len(outs))],
        scratch_shapes=scratch,
        input_output_aliases={k: k for k in range(alias)},
        compiler_params=pltpu.CompilerParams(vmem_limit_bytes=16 << 20),
    )(*args)


def on_device(right_side, stretch, mass_term, slot_position, coarse_group):
    a1 = jnp.asarray(A_FWD, BF16)
    a2 = jnp.asarray(A_BWD, BF16)
    lam = jnp.asarray(np.stack([LAM_J, LAM_K]), F32)
    wm = jnp.asarray(W_MOM, BF16)
    wr = jnp.asarray(W_RIM, BF16)
    row = pltpu.VMEM((1, 256), jnp.int32)
    rhs = right_side.reshape(8, 64, 256)
    coef, to_d, to_u, slot = call(
        start_kernel,
        [vm(2, 8, LANES), vm(10, 8, LANES), vm(10, 8, LANES), row],
        (
            rhs,
            stretch,
            mass_term.reshape(1, 256),
            slot_position.reshape(1, 256),
            coarse_group.reshape(1, 256),
        ),
        [(2, 8, 8, 256), (3, 256), (1, 256), row],
        hbm_in=5,
        sems=6,
    )
    yd = ring(to_u, "sy", 1)
    yu = ring(to_d, "sy", -1)
    src, dinv = call(
        place_kernel,
        [vm(8, 16, 8, LANES), vm(10, 104, 256)],
        (rhs, lam, slot, coef),
        [(8, 64, 256), (2, 104, LANES)],
        hbm_in=2,
        sems=9,
    )
    to_l, to_r = call(rim_kernel, [vm(20, 8, LANES)] * 2, (src, coef, yd, yu))
    xl = ring(to_r, "sx", 1)
    xr = ring(to_l, "sx", -1)
    rin, sin = call(
        first_inner_kernel,
        [vm(8 * 192, LANES), vm(10, 104, 256)],
        (src, yd, yu, a1),
        [(8, 104, 256)],
    )

    side = vm(10, 3, 8, LANES)
    rout, w, to_d, to_u = call(
        first_kernel,
        [vm(2 * 192, LANES), vm(10, 18, 8, LANES), side, side],
        (xl, xr, sin, dinv, a1, a2),
        [(2, 104, 256), (10, 104, 256), (1920, LANES)],
    )
    d = ring(to_u, "sy", 1)
    u = ring(to_d, "sy", -1)
    to_l, to_r = call(edge_kernel, [vm(3, 20, 8, LANES)] * 2, (w, d, u))
    l = ring(to_r, "sx", 1)
    r = ring(to_l, "sx", -1)
    hin, sin = call(
        second_inner_kernel,
        [vm(6, 20, 8, LANES), vm(10, 104, 256)],
        (rin, coef, yd, yu, w, d, u, a1),
        [(4, 4, 8, LANES), (4 * 192, LANES), (4, 104, 256)],
    )

    slab = vm(2, 18, 8, LANES)
    side = vm(10, 2, 8, LANES)
    c, to_l, to_r, own_d, own_u = call(
        second_kernel,
        [vm(10, 18, 8, LANES), slab, slab, side, side],
        (rin, rout, coef, xl, xr, yd, yu, w, l, r, d, u, hin, sin, dinv, a1, a2),
        [
            (6, 20, 8, LANES),
            (3, 4, 4, 8, LANES),
            (6 * 192, LANES),
            (6, 104, 256),
            (10, 104, 256),
            (1920, LANES),
        ],
    )
    l = ring(to_r, "sx", 1)
    r = ring(to_l, "sx", -1)
    edge = vm(2, 8, 8, LANES)
    ny = lax.axis_size("sy")
    smooth, res, rin, mom, pick, member = call(
        middle_inner_kernel,
        [sd(8, 64, 256), sd(8, 64, 256), vm(4, 64, 256), vm(16, 256), vm(ny, 512), vm(16, 512)],
        (src, coef, yd, yu, c, slot, wm),
        [(6, 18, 8, LANES), (6, 48, 256), (4, 32, 256)],
        hbm_out=2,
        sems=2,
    )
    uout, rout, to_d, to_u, part = call(
        middle_kernel,
        [vm(2, 16, 8, LANES), vm(4, 64, 256), edge, edge, vm(ny, LANES)],
        (src, coef, yd, yu, c, l, r, own_d, own_u, mom, pick, member, wm, wr),
        [(10, 18, 8, LANES), (256, 256), (2, 10, 2, 8, LANES)],
    )
    d = ring(to_u, "sy", 1)
    u = ring(to_d, "sy", -1)
    arrived = lax.all_to_all(part, "sy", split_axis=0, concat_axis=0, tiled=True)
    smooth, res, coarse = call(
        last_kernel,
        [sd(8, 64, 256), sd(8, 64, 256), sd(8, GRP_DEV)],
        (smooth, res, c, uout, rin, rout, coef, d, u, slot, arrived),
        [(8, 64, 256), (8, 64, 256), (8, GRP_DEV)],
        hbm_in=2,
        hbm_out=3,
        sems=9,
        alias=2,
    )
    return smooth.reshape(8, 8, 8, 256), res.reshape(8, 8, 8, 256), coarse


def solution(mesh):
    split_all = P(None, None, None, ("sx", "sy"))
    flat = P(("sx", "sy"))
    return jax.shard_map(
        on_device,
        mesh=mesh,
        in_specs=(split_all, P(None, ("sx", "sy")), flat, flat, flat),
        out_specs=(split_all, split_all, P(None, ("sx", "sy"))),
        check_vma=False,
    )
```

```python
import jax
import jax.numpy as jnp
import numpy as np
from jax import lax
from jax.experimental import pallas as pl
from jax.experimental.pallas import tpu as pltpu
from jax.sharding import PartitionSpec as P

NODES = 8
GRP_DEV = 16
LANES = 128
RELAX = 0.35
F32 = jnp.float32
BF16 = jnp.bfloat16


def split_np(a):
    a = np.asarray(a, np.float32)
    hi = np.asarray(jnp.asarray(a).astype(BF16).astype(F32))
    return hi, a - hi


def constants():
    n = NODES + 2
    col = np.arange(n, dtype=np.float64) + 1.0
    s = np.sqrt(2.0 / (n + 1.0)) * np.sin(np.pi * col[:, None] * col[None, :] / (n + 1.0))
    lam = 2.0 - 2.0 * np.cos(np.pi * col / (n + 1.0))
    fwd = np.zeros((104, 112))
    for q in range(n):
        for r in range(n):
            c = q * 8 + r - 1
            if r == 0:
                c = 80 + q
            if r == n - 1:
                c = 96 + q
            fwd[:100, c] = np.outer(s[:, q], s[:, r]).reshape(-1)
    fh, fl = split_np(fwd)
    a1 = np.concatenate([np.concatenate([fh, fh], 1), np.concatenate([fl, fl], 1)], 0)
    bh, bl = split_np(RELAX * fwd.T)
    a2 = np.concatenate([np.concatenate([bh, bh], 1), np.concatenate([bl, bl], 1)], 0)
    lam_j = np.ones((104, LANES), np.float32)
    lam_k = np.ones((104, LANES), np.float32)
    lam_j[:100] = np.repeat(lam, n)[:, None]
    lam_k[:100] = np.tile(lam, n)[:, None]
    t = np.arange(NODES) / (NODES - 1.0)
    w = np.stack([1.0 - t, t])
    wm = np.einsum("ax,by,cz->abcxyz", w, w, w).reshape(8, 512)
    wh, wl = split_np(wm)
    wm = np.concatenate([wh, wl], 0)
    rim = wm.reshape(16, 8, 8, 8)[:, :, [0, 1, 6, 7]].reshape(16, 256)
    return s, lam, a1, a2, lam_j, lam_k, wm, rim


SINES, LAM, A_FWD, A_BWD, LAM_J, LAM_K, W_MOM, W_RIM = constants()


def split(x):
    hi = x.astype(BF16)
    return hi, (x - hi.astype(F32)).astype(BF16)


def dot(a, b):
    return lax.dot_general(a, b, (((1,), (0,)), ((), ())), preferred_element_type=F32)


def dot_t(a, b):
    return lax.dot_general(a, b, (((1,), (1,)), ((), ())), preferred_element_type=F32)


def flags():
    i = lax.axis_index("sx")
    j = lax.axis_index("sy")
    nx = lax.axis_size("sx")
    ny = lax.axis_size("sy")
    one = lambda c: jnp.where(c, 1.0, 0.0).astype(F32)
    return one(i > 0), one(i < nx - 1), one(j > 0), one(j < ny - 1)


def lane_up(x):
    lane = lax.broadcasted_iota(jnp.int32, x.shape, x.ndim - 1)
    return jnp.where(lane == LANES - 1, 0.0, pltpu.roll(x, LANES - 1, x.ndim - 1))


def lane_down(x):
    lane = lax.broadcasted_iota(jnp.int32, x.shape, x.ndim - 1)
    return jnp.where(lane == 0, 0.0, pltpu.roll(x, 1, x.ndim - 1))


def onehot(slot_row):
    p = lax.broadcasted_iota(jnp.int32, (256, 256), 0)
    return jnp.where(p == slot_row, 1.0, 0.0).astype(BF16)


def split3(a):
    a1 = a.astype(BF16)
    e = a - a1.astype(F32)
    a2 = e.astype(BF16)
    return a1, a2, (e - a2.astype(F32)).astype(BF16)


def start_kernel(
    rhs_hbm, stretch_hbm, mass_hbm, slot_hbm, group_hbm,
    coef_ref, to_down_ref, to_up_ref, slot_ref,
    face_ref, stretch_ref, mass_ref, group_ref, sems,
):
    pairs = (
        (slot_hbm, slot_ref),
        (rhs_hbm.at[:, pl.ds(0, 8), :], face_ref.at[0]),
        (rhs_hbm.at[:, pl.ds(56, 8), :], face_ref.at[1]),
        (stretch_hbm, stretch_ref),
        (mass_hbm, mass_ref),
        (group_hbm, group_ref),
    )
    copies = [pltpu.make_async_copy(h, v, sems.at[k]) for k, (h, v) in enumerate(pairs)]
    for c in copies:
        c.start()
    copies[0].wait()
    oh = onehot(slot_ref[...])
    for k, out, b in ((1, to_down_ref, 0), (2, to_up_ref, 1)):
        copies[k].wait()
        g = dot_t(jnp.concatenate(split3(face_ref[k - 1].reshape(64, 256)), 0), oh)
        g = g[0:64] + g[64:128] + g[128:192]
        out[0:8] = g[:, b * LANES : (b + 1) * LANES].reshape(8, 8, LANES)
    for c in copies[3:]:
        c.wait()
    c = jnp.concatenate(
        [
            stretch_ref[...],
            mass_ref[...],
            group_ref[...].astype(F32),
            jnp.zeros((3, 256), F32),
        ],
        0,
    )
    c1, c2, c3 = split3(c)
    cg = dot_t(c1, oh) + dot_t(c2, oh) + dot_t(c3, oh)
    coef = jnp.concatenate([cg[0:4, :LANES], cg[0:4, LANES:]], 0)
    gr = jnp.concatenate([cg[4:5, :LANES], cg[4:5, LANES:], jnp.zeros((6, LANES), F32)], 0)
    coef_ref[0] = coef
    coef_ref[1] = gr
    pad = jnp.zeros((3, LANES), F32)
    to_down_ref[8] = jnp.concatenate([coef[0:4], gr[0:1], pad], 0)
    to_up_ref[8] = jnp.concatenate([coef[4:8], gr[1:2], pad], 0)


def place_kernel(
    rhs_hbm, lam_hbm, slot_ref, coef_ref, src_ref, dinv_ref, rhs_ref, lam_ref, sems
):
    copies = [
        pltpu.make_async_copy(rhs_hbm.at[x], rhs_ref.at[x], sems.at[x]) for x in range(8)
    ]
    lam = pltpu.make_async_copy(lam_hbm, lam_ref, sems.at[8])
    lam.start()
    for c in copies:
        c.start()
    oh = onehot(slot_ref[...])
    lam.wait()
    for b in range(2):
        lanes = slice(b * LANES, (b + 1) * LANES)
        cx, cy, cz, m, _ = rows_of(coef_ref[0], b * 4)
        cxl = [cx * float(v) for v in LAM]
        for t in range(13):
            row = slice(t * 8, t * 8 + 8)
            d0 = cy * lam_ref[0, row, :] + cz * lam_ref[1, row, :] + m
            for i in range(10):
                dinv_ref[i, row, lanes] = 1.0 / (d0 + cxl[i])
    for x in range(8):
        copies[x].wait()
        g = dot_t(jnp.concatenate(split3(rhs_ref[x]), 0), oh)
        g = g[0:64] + g[64:128] + g[128:192]
        for b in range(2):
            src_ref[x, b * 8 : b * 8 + 8] = g[:, b * LANES : (b + 1) * LANES].reshape(8, 8, LANES)


def rim_kernel(src_ref, coef_ref, yd_ref, yu_ref, to_left_ref, to_right_ref):
    coef_y = jnp.concatenate([yd_ref[8, 0:4, :], yu_ref[8, 0:4, :]], 0)
    for x, out in ((0, to_left_ref), (7, to_right_ref)):
        out[0] = yd_ref[x]
        out[1:17] = src_ref[x]
        out[17] = yu_ref[x]
        out[18] = coef_ref[0]
        out[19] = coef_y


def forward(res, base, a1_ref):
    ends = []
    for z, shift in ((7, lane_down), (0, lane_up)):
        ends.append([shift(res[pl.ds(base + 64 * t + z, 8, stride=8), :]) for t in range(3)])
    halves = [
        jnp.concatenate(
            [res[base + 64 * b : base + 64 * b + 80, :]] + ends[0][b : b + 2] + ends[1][b : b + 2],
            0,
        )
        for b in range(2)
    ]
    hi, lo = split(jnp.concatenate(halves, 1))
    r = dot(a1_ref[...], jnp.concatenate([hi, lo], 0))
    return r[:104] + r[104:]


def along_x(layers, partial, row, lanes):
    acc = [None if partial is None else partial[i, row, lanes] for i in range(10)]
    for p, (low, high) in layers.items():
        v = low[0][low[1], row, lanes]
        w = high[0][high[1], row, lanes]
        h = (v + w, v - w)
        for i in range(10):
            term = h[i % 2] * float(SINES[i, p])
            acc[i] = term if acc[i] is None else acc[i] + term
    return acc


def partial_x(layers, out_ref):
    for b in range(2):
        lanes = slice(b * LANES, (b + 1) * LANES)

        def chunk(t, carry):
            row = pl.ds(pl.multiple_of(t * 8, 8), 8)
            for i, v in enumerate(along_x(layers, None, row, lanes)):
                out_ref[i, row, lanes] = v
            return carry

        lax.fori_loop(0, 13, chunk, 0)


def finish_solves(layers, partial, dinv_ref, a2_ref, spec, wout):
    for b in range(2):
        lanes = slice(b * LANES, (b + 1) * LANES)

        def chunk(t, carry):
            row = pl.ds(pl.multiple_of(t * 8, 8), 8)
            z = along_x(layers, partial, row, lanes)
            z = [z[i] * dinv_ref[i, row, lanes] for i in range(10)]
            for p in range(5):
                e = z[0] * float(SINES[0, p])
                o = z[1] * float(SINES[1, p])
                for i in range(2, 10, 2):
                    e = e + z[i] * float(SINES[i, p])
                    o = o + z[i + 1] * float(SINES[i + 1, p])
                spec[p, row, lanes] = e + o
                spec[9 - p, row, lanes] = e - o
            return carry

        lax.fori_loop(0, 13, chunk, 0)

    for p in range(10):
        base = p * 192
        hi, lo = split(spec[p])
        r = dot(a2_ref[...], jnp.concatenate([hi, lo], 0))
        r = r[:112] + r[112:]
        r0 = r[:, :LANES]
        r1 = r[:, LANES:]
        wout[base : base + 64, :] = r0[0:64]
        wout[base + 64 : base + 80, :] = r0[64:80] + r1[0:16]
        wout[base + 80 : base + 144, :] = r1[16:80]
        wout[base + 144 : base + 192, :] = jnp.zeros((48, LANES), F32)
        for off, z, shift in ((80, 7, lane_up), (96, 0, lane_down)):
            rows = [
                r0[off : off + 8],
                r0[off + 8 : off + 16] + r1[off : off + 8],
                r1[off + 8 : off + 16],
            ]
            for t in range(3):
                at = pl.ds(base + 64 * t + z, 8, stride=8)
                wout[at, :] = wout[at, :] + shift(rows[t])


def put(ref, p, y, value):
    n = value.shape[0]
    at = (p * 24 + y) * 8
    ref[at : at + n * 8, :] = value.reshape(n * 8, LANES)


def get(ref, p, y, n):
    at = (p * 24 + y) * 8
    return ref[at : at + n * 8, :].reshape(n, 8, LANES)


def with_rows(line, n, d, u, down, up):
    rows_d = d * down
    rows_u = u * up
    low = rows_d[n - 2 : n] + jnp.concatenate([line[0:1] * down, line[1:2]], 0)
    high = rows_u[0:2] + jnp.concatenate([line[16:17], line[17:18] * up], 0)
    parts = [low, line[2:16], high]
    if n > 2:
        parts = [rows_d[0 : n - 2]] + parts + [rows_u[2:n]]
    return jnp.concatenate(parts, 0)


def put_layer(ref, at, below, line, above):
    put(ref, at, 0, below)
    put(ref, at, 1, line)
    put(ref, at, 17, above)
    put(ref, at, 18, jnp.zeros((6, 8, LANES), F32))


def first_inner_kernel(src_ref, yd_ref, yu_ref, a1_ref, rin_ref, sin_ref, sout):
    _, _, down, up = flags()
    for x in range(8):
        put_layer(rin_ref, x, yd_ref[x : x + 1] * down, src_ref[x], yu_ref[x : x + 1] * up)
        sout[x] = forward(rin_ref, x * 192, a1_ref)
    partial_x({p: ((sout, p - 1), (sout, 8 - p)) for p in range(1, 5)}, sin_ref)


def first_kernel(
    xl_ref, xr_ref, sin_ref, dinv_ref, a1_ref, a2_ref,
    rout_ref, wout, to_down_ref, to_up_ref, sout, spec,
):
    left, right, down, up = flags()
    for k, (x_ref, side) in enumerate(((xl_ref, left), (xr_ref, right))):
        put_layer(
            rout_ref,
            k,
            x_ref[0:1] * (side * down),
            x_ref[1:17] * side,
            x_ref[17:18] * (side * up),
        )
        sout[k] = forward(rout_ref, k * 192, a1_ref)
    finish_solves({0: ((sout, 0), (sout, 1))}, sin_ref, dinv_ref, a2_ref, spec, wout)
    for p in range(10):
        to_down_ref[p] = get(wout, p, 0, 3)
        to_up_ref[p] = get(wout, p, 15, 3)


def even_row():
    return lax.rem(lax.axis_index("sy"), 2) == 0


class Picked:
    def __init__(self, first, second):
        self.refs = (first, second)

    def __getitem__(self, at):
        return jnp.where(even_row(), self.refs[0][at], self.refs[1][at])


def edge_kernel(w_ref, d_ref, u_ref, a_ref, b_ref):
    _, _, down, up = flags()
    even = even_row()
    for k in range(3):
        to_l, to_r = [
            with_rows(get(w_ref, p, 0, 18), 3, d_ref[p], u_ref[p], down, up) for p in (k, 7 + k)
        ]
        a_ref[k] = jnp.where(even, to_r, to_l)
        b_ref[k] = jnp.where(even, to_l, to_r)


def neighbours_z(u):
    z = lax.broadcasted_iota(jnp.int32, u.shape, 1)
    s = pltpu.roll(u, 7, 1)
    above = jnp.where(z == 7, lane_up(s), s)
    s = pltpu.roll(u, 1, 1)
    below = jnp.where(z == 0, lane_down(s), s)
    return above, below


ROWS = ((0, 1, 0), (1, 4, 1), (5, 4, 1), (9, 4, 2), (13, 4, 2), (17, 1, 3))


def second_residual(get_h, get_r, cb, p, at, res_ref, left, right, down, up):
    for y, n, b in ROWS:
        v = get_h(p + 1, y + 1, n)
        res = get_r(y, n) - stencil(
            cb[b],
            v,
            get_h(p + 2, y + 1, n) + get_h(p, y + 1, n),
            get_h(p + 1, y + 2, n) + get_h(p + 1, y, n),
        )
        if p == 0:
            res = res * left
        if p == 9:
            res = res * right
        if y == 0:
            res = res * down
        if y == 17:
            res = res * up
        put(res_ref, at, y, res)
    put(res_ref, at, 18, jnp.zeros((6, 8, LANES), F32))


def spread_coefs(cb, rows):
    for b, (tile, at) in enumerate(rows):
        for k, v in enumerate(rows_of(tile, at)):
            cb[b, k] = v
    return [[cb.at[b, k] for k in range(5)] for b in range(4)]


class Loaded:
    def __init__(self, refs):
        self.refs = refs

    def __getitem__(self, k):
        return self.refs[k][...]


def second_inner_kernel(
    rin_ref, coef_ref, yd_ref, yu_ref, w_ref, d_ref, u_ref, a1_ref, h_ref, sin_ref, cb, r1, sout,
):
    left, right, down, up = flags()
    for x in range(3, 9):
        h_ref[x - 3] = with_rows(get(w_ref, x - 1, 0, 18), 3, d_ref[x - 1], u_ref[x - 1], down, up)
    tiles = spread_coefs(
        cb, ((yd_ref[8], 0), (coef_ref[0], 0), (coef_ref[0], 4), (yu_ref[8], 0))
    )
    coefs = [Loaded(t) for t in tiles]
    get_h = lambda x, y, n: h_ref[x - 3, y : y + n]
    for k in range(4):
        p = 3 + k
        get_r = lambda y, n: get(rin_ref, p - 1, y, n)
        second_residual(get_h, get_r, coefs, p, k, r1, left, right, down, up)
        sout[k] = forward(r1, k * 192, a1_ref)
    partial_x({p: ((sout, p - 3), (sout, 6 - p)) for p in (3, 4)}, sin_ref)


def second_kernel(
    rin_ref, rout_ref, coef_ref, xl_ref, xr_ref, yd_ref, yu_ref, w_ref, a_ref, b_ref, d_ref, u_ref,
    hin_ref, sin_ref, dinv_ref, a1_ref, a2_ref,
    c_ref, to_a_ref, to_b_ref, own_down_ref, own_up_ref, h, cb, r1, sout, spec, wout,
):
    left, right, down, up = flags()
    l_ref, r_ref = Picked(a_ref, b_ref), Picked(b_ref, a_ref)
    for x in (0, 1, 2, 9, 10, 11):
        if x == 0:
            g = l_ref[0] * left
        elif x == 11:
            g = r_ref[2] * right
        else:
            g = with_rows(get(w_ref, x - 1, 0, 18), 3, d_ref[x - 1], u_ref[x - 1], down, up)
            if x == 1:
                g = (g + l_ref[1]) * left
            elif x == 2:
                g = g + l_ref[2] * left
            elif x == 9:
                g = g + r_ref[0] * right
            elif x == 10:
                g = (g + r_ref[1]) * right
        h[x if x < 3 else x - 6] = g

    def get_h(x, y, n):
        if 3 <= x <= 8:
            return hin_ref[x - 3, y : y + n]
        return h[x if x < 3 else x - 6, y : y + n]

    coefs = []
    for a, x_ref in ((0, xl_ref), (1, None), (2, xr_ref)):
        if x_ref is None:
            rows = ((yd_ref[8], 0), (coef_ref[0], 0), (coef_ref[0], 4), (yu_ref[8], 0))
        else:
            rows = ((x_ref[19], 0), (x_ref[18], 0), (x_ref[18], 4), (x_ref[19], 4))
        coefs.append([Loaded(t) for t in spread_coefs(cb.at[a], rows)])
    for k, p in enumerate((0, 1, 2, 7, 8, 9)):
        if p in (0, 9):
            get_r = lambda y, n: get(rout_ref, 0 if p == 0 else 1, y, n)
        else:
            get_r = lambda y, n: get(rin_ref, p - 1, y, n)
        cb_p = coefs[0 if p == 0 else 2 if p == 9 else 1]
        second_residual(get_h, get_r, cb_p, p, k, r1, left, right, down, up)
        sout[k] = forward(r1, k * 192, a1_ref)
    layers = {p: ((sout, p), (sout, 5 - p)) for p in range(3)}
    finish_solves(layers, sin_ref, dinv_ref, a2_ref, spec, wout)
    for p in range(10):
        line = get(wout, p, 0, 18)
        c_ref[p] = get_h(p + 1, 1, 18) + line
        own_down_ref[p] = line[0:2]
        own_up_ref[p] = line[16:18]
    even = even_row()
    for k in range(2):
        to_l, to_r = get(wout, k, 0, 18), get(wout, 8 + k, 0, 18)
        to_a_ref[k] = jnp.where(even, to_r, to_l)
        to_b_ref[k] = jnp.where(even, to_l, to_r)


def add_x(g, p, l, r, left, right, y=slice(0, 18)):
    if p == 0:
        return (g + l[0, y]) * left
    if p == 1:
        return g + l[1, y] * left
    if p == 8:
        return g + r[0, y] * right
    if p == 9:
        return (g + r[1, y]) * right
    return g


def rows_of(tile, at):
    c = [jnp.broadcast_to(tile[at + k : at + k + 1, :], (8, LANES)) for k in range(4)]
    return c + [2.0 * (c[0] + c[1] + c[2]) + c[3]]


def stencil(cf, v, x_sum, y_sum):
    above, below = neighbours_z(v)
    return cf[4] * v - cf[0] * x_sum - cf[1] * y_sum - cf[2] * (above + below)


def column_residual(get_h, src_ref, cf, x, b, mr_ref, at):
    lanes = slice(b * LANES, (b + 1) * LANES)
    for y in (0, 4):
        yy = b * 8 + y + 1
        p = x + 1
        v = get_h(p, yy, 4)
        res = src_ref[x, yy - 1 : yy + 3] - stencil(
            cf,
            v,
            get_h(p + 1, yy, 4) + get_h(p - 1, yy, 4),
            get_h(p, yy + 1, 4) + get_h(p, yy - 1, 4),
        )
        mr_ref[at, y * 8 : y * 8 + 32, lanes] = res.reshape(32, LANES)


def moments(wm_ref, x, rows):
    rh, rl = split(rows)
    w = wm_ref[:, x * 64 : x * 64 + rows.shape[0]]
    return dot(w, rh) + dot(w, rl)


def to_slots(uv, oh):
    hi, lo = split(uv)
    n = uv.shape[0]
    o = dot(jnp.concatenate([hi, lo], 0), oh)
    return o[:n] + o[n:]


def middle_inner_kernel(
    src_ref, coef_ref, yd_ref, yu_ref, c_ref, slot_ref, wm_ref,
    smooth_hbm, res_hbm, mr_ref, mom_ref, pick_ref, member_ref, h, smooth_ref, res_ref, sems,
):
    _, _, down, up = flags()
    oh = onehot(slot_ref[...])
    copies = []
    for x in range(1, 7):
        both = [c_ref[x + 1, 8 * b + 2 : 8 * b + 8].reshape(48, LANES) for b in range(2)]
        smooth_ref[x - 1] = to_slots(jnp.concatenate(both, 1), oh)
    copies.append(
        pltpu.make_async_copy(smooth_ref, smooth_hbm.at[pl.ds(1, 6), pl.ds(8, 48), :], sems.at[0])
    )
    copies[0].start()
    for k in range(6):
        h[k] = c_ref[k + 2]
        h[k, 0] = c_ref[k + 2, 0] * down
        h[k, 17] = c_ref[k + 2, 17] * up
    get_h = lambda p, y, n: h[p - 2, y : y + n]
    coefs = [rows_of(coef_ref[0], 0), rows_of(coef_ref[0], 4)]
    for k in range(4):
        for b in range(2):
            column_residual(get_h, src_ref, coefs[b], 2 + k, b, mr_ref, k)
        res_ref[k] = to_slots(mr_ref[k, 16:48, :], oh)
    copies.append(
        pltpu.make_async_copy(res_ref, res_hbm.at[pl.ds(2, 4), pl.ds(16, 32), :], sems.at[1])
    )
    copies[1].start()
    mom = jnp.zeros((16, 256), F32)
    for k in (0, 2):
        mom = mom + moments(wm_ref, 2 + k, mr_ref[k : k + 2].reshape(128, 256))
    mom_ref[...] = mom
    gr = coef_ref[1]
    group = jnp.concatenate([gr[0:1], gr[1:2], yd_ref[8, 4:5, :], yu_ref[8, 4:5, :]], 1)
    ny = pick_ref.shape[0]
    col = (group + 0.5).astype(jnp.int32) - lax.axis_index("sx") * (ny * GRP_DEV)
    owner = lax.shift_right_logical(col, 4)
    member = jnp.bitwise_and(col, 15)
    sel = lax.broadcasted_iota(jnp.int32, (ny, 512), 0)
    pick_ref[...] = jnp.where(sel == owner, 1.0, 0.0)
    sel = lax.broadcasted_iota(jnp.int32, (16, 512), 0)
    member_ref[...] = jnp.where(sel == member, 1.0, 0.0)
    for c in copies:
        c.wait()


def middle_kernel(
    src_ref, coef_ref, yd_ref, yu_ref, c_ref, a_ref, b_ref, own_down_ref, own_up_ref,
    mom_ref, pick_ref, member_ref, wm_ref, wr_ref,
    u_ref, mr_ref, to_down_ref, to_up_ref, part_ref, h, rim, edge,
):
    left, right, down, up = flags()
    l_ref, r_ref = Picked(a_ref, b_ref), Picked(b_ref, a_ref)
    for p in range(10):
        e = add_x(own_down_ref[p], p, l_ref, r_ref, left, right, slice(0, 2))
        edge[0, p] = jnp.concatenate([e[0:1] * down, e[1:2]], 0)
        e = add_x(own_up_ref[p], p, l_ref, r_ref, left, right, slice(16, 18))
        edge[1, p] = jnp.concatenate([e[0:1], e[1:2] * up], 0)
        if 3 < p < 6:
            continue
        g = add_x(c_ref[p], p, l_ref, r_ref, left, right)
        h[p] = g
        h[p, 0] = g[0] * down
        h[p, 17] = g[17] * up
    u_ref[0] = h[1, 1:17]
    u_ref[1] = h[8, 1:17]
    get_h = lambda p, y, n: h[p, y : y + n]
    coefs = [rows_of(coef_ref[0], 0), rows_of(coef_ref[0], 4)]
    for k, x in enumerate((0, 1, 6, 7)):
        for b in range(2):
            column_residual(get_h, src_ref, coefs[b], x, b, mr_ref, k)
    rim[...] = jnp.zeros((256, 256), F32)
    for k, out, far, near, tile, lanes, y_far, y_near in (
        (0, to_down_ref, 0, 1, yd_ref, slice(0, LANES), 2, 3),
        (1, to_up_ref, 1, 0, yu_ref, slice(LANES, 256), 1, 0),
    ):
        slab = edge.at[k]
        cf = rows_of(tile[8], 0)
        for x in range(8):
            p = x + 1
            v = slab[p, far : far + 1]
            res = stencil(
                cf,
                v,
                slab[p + 1, far : far + 1] + slab[p - 1, far : far + 1],
                slab[p, near : near + 1],
            )
            out[0, x] = v[0]
            out[1, x] = -res[0]
            at = (x * 4 + y_near) * 8
            rim[at : at + 8, lanes] = -res[0]
            at = (x * 4 + y_far) * 8
            rim[at : at + 8, lanes] = cf[1] * v[0]
    mom = mom_ref[...]
    mom = mom + moments(wm_ref, 0, mr_ref[0:2].reshape(128, 256))
    mom = mom + moments(wm_ref, 6, mr_ref[2:4].reshape(128, 256))
    rh, rl = split(rim[...])
    mom_y = dot(wr_ref[...], rh) + dot(wr_ref[...], rl)
    mom_y = mom_y[0:8] + mom_y[8:16]
    mom = jnp.concatenate(
        [mom[0:8] + mom[8:16], mom_y[:, :LANES] * down, mom_y[:, LANES:] * up], 1
    )
    member = member_ref[...]
    spread = jnp.concatenate([member * mom[v : v + 1] for v in range(8)], 0)
    sh, sl = split(spread)
    pick = pick_ref[...].astype(BF16)
    part_ref[...] = dot_t(pick, sh) + dot_t(pick, sl)


def last_kernel(
    smooth_in, res_in, c_ref, uout_ref, rin_ref, rout_ref, coef_ref, d_ref, u_ref, slot_ref,
    arrived_ref,
    smooth_hbm, res_hbm, coarse_hbm, smooth_ref, res_ref, coarse_ref, sems,
):
    _, _, down, up = flags()
    total = jnp.sum(arrived_ref[...], axis=0, keepdims=True)
    for v in range(8):
        coarse_ref[v : v + 1, :] = total[:, v * GRP_DEV : (v + 1) * GRP_DEV]
    copies = [pltpu.make_async_copy(coarse_ref, coarse_hbm, sems.at[8])]
    copies[0].start()

    def send(ref, hbm, x, nx, row, rows):
        at = (pl.ds(x, nx), pl.ds(row, rows), slice(None))
        k = len(copies) - 1
        copies.append(pltpu.make_async_copy(ref.at[at], hbm.at[at], sems.at[k]))
        copies[-1].start()

    oh = onehot(slot_ref[...])
    sides = (
        (d_ref, down, jnp.broadcast_to(coef_ref[0, 1:2, :], (8, LANES))),
        (u_ref, up, jnp.broadcast_to(coef_ref[0, 5:6, :], (8, LANES))),
    )

    def added(x):
        out = []
        for slab, on, cy in sides:
            v = slab[0, x] * on
            out.append((v, slab[1, x] * on, cy * v))
        return out

    zero = jnp.zeros((8, LANES), F32)
    pairs = [added(x) for x in range(8)]
    for k, x in enumerate((0, 1, 6, 7)):
        (_, d0, d1), (_, e0, e1) = pairs[x]
        add = jnp.concatenate(
            [
                jnp.concatenate([d0, d1] + [zero] * 6, 0),
                jnp.concatenate([zero] * 6 + [e1, e0], 0),
            ],
            1,
        )
        res_ref[x] = to_slots(rout_ref[k] + add, oh)
        if k == 1:
            send(res_ref, res_hbm, 0, 2, 0, 64)
    send(res_ref, res_hbm, 6, 2, 0, 64)
    low, high = [], []
    for k in range(4):
        (_, d0, d1), (_, e0, e1) = pairs[2 + k]
        z2 = jnp.zeros((16, LANES), F32)
        low.append(
            rin_ref[k, 0:16, :] + jnp.concatenate([jnp.concatenate([d0, d1], 0), z2], 1)
        )
        high.append(
            rin_ref[k, 48:64, :] + jnp.concatenate([z2, jnp.concatenate([e1, e0], 0)], 1)
        )
    res_ref[2:6, 0:16, :] = to_slots(jnp.concatenate(low, 0), oh).reshape(4, 16, 256)
    send(res_ref, res_hbm, 2, 4, 0, 16)
    res_ref[2:6, 48:64, :] = to_slots(jnp.concatenate(high, 0), oh).reshape(4, 16, 256)
    send(res_ref, res_hbm, 2, 4, 48, 16)
    for k, x in enumerate((0, 7)):
        (d0, _, _), (e0, _, _) = pairs[x]
        both = [uout_ref[k, 0:8].reshape(64, LANES), uout_ref[k, 8:16].reshape(64, LANES)]
        both[0] = both[0] + jnp.concatenate([d0] + [zero] * 7, 0)
        both[1] = both[1] + jnp.concatenate([zero] * 7 + [e0], 0)
        smooth_ref[x] = to_slots(jnp.concatenate(both, 1), oh)
        send(smooth_ref, smooth_hbm, x, 1, 0, 64)
    low, high = [], []
    for x in range(1, 7):
        (d0, _, _), (e0, _, _) = pairs[x]
        c = [c_ref[x + 1, y] for y in (1, 9, 8, 16)]
        low.append(jnp.concatenate([c[0] + d0, c[1]], 1))
        high.append(jnp.concatenate([c[2], c[3] + e0], 1))
    smooth_ref[1:7, 0:8, :] = to_slots(jnp.concatenate(low, 0), oh).reshape(6, 8, 256)
    send(smooth_ref, smooth_hbm, 1, 6, 0, 8)
    smooth_ref[1:7, 56:64, :] = to_slots(jnp.concatenate(high, 0), oh).reshape(6, 8, 256)
    send(smooth_ref, smooth_hbm, 1, 6, 56, 8)
    for c in copies:
        c.wait()


def sd(*shape):
    return jax.ShapeDtypeStruct(shape, F32)


def vm(*shape):
    return pltpu.VMEM(shape, F32)


def ring(value, axis, by):
    n = lax.axis_size(axis)
    return lax.ppermute(value, axis, [(i, (i + by) % n) for i in range(n)])


def snake(value, by):
    nx = lax.axis_size("sx")
    ny = lax.axis_size("sy")
    pairs = []
    for i in range(nx):
        for j in range(ny):
            to = i + (by if j % 2 == 0 else -by)
            target = to * ny + j if 0 <= to < nx else i * ny + (j ^ 1)
            pairs.append((i * ny + j, target))
    return lax.ppermute(value, ("sx", "sy"), pairs)


def call(kernel, outs, args, scratch=(), hbm_in=0, hbm_out=0, sems=0, alias=0):
    vmem = pl.BlockSpec(memory_space=pltpu.VMEM)
    hbm = pl.BlockSpec(memory_space=pltpu.HBM)
    args = [
        pltpu.with_memory_space_constraint(a, pltpu.HBM if k < hbm_in else pltpu.VMEM)
        for k, a in enumerate(args)
    ]
    scratch = [pltpu.VMEM(s, F32) if isinstance(s, tuple) else s for s in scratch]
    if sems:
        scratch.append(pltpu.SemaphoreType.DMA((sems,)))
    return pl.pallas_call(
        kernel,
        out_shape=outs,
        in_specs=[hbm if k < hbm_in else vmem for k in range(len(args))],
        out_specs=[hbm if k < hbm_out else vmem for k in range(len(outs))],
        scratch_shapes=scratch,
        input_output_aliases={k: k for k in range(alias)},
        compiler_params=pltpu.CompilerParams(vmem_limit_bytes=16 << 20),
    )(*args)


def on_device(right_side, stretch, mass_term, slot_position, coarse_group):
    a1 = jnp.asarray(A_FWD, BF16)
    a2 = jnp.asarray(A_BWD, BF16)
    lam = jnp.asarray(np.stack([LAM_J, LAM_K]), F32)
    wm = jnp.asarray(W_MOM, BF16)
    wr = jnp.asarray(W_RIM, BF16)
    row = pltpu.VMEM((1, 256), jnp.int32)
    rhs = right_side.reshape(8, 64, 256)
    coef, to_d, to_u, slot = call(
        start_kernel,
        [vm(2, 8, LANES), vm(9, 8, LANES), vm(9, 8, LANES), row],
        (
            rhs,
            stretch,
            mass_term.reshape(1, 256),
            slot_position.reshape(1, 256),
            coarse_group.reshape(1, 256),
        ),
        [(2, 8, 8, 256), (3, 256), (1, 256), row],
        hbm_in=5,
        sems=6,
    )
    yd = ring(to_u, "sy", 1)
    yu = ring(to_d, "sy", -1)
    src, dinv = call(
        place_kernel,
        [vm(8, 16, 8, LANES), vm(10, 104, 256)],
        (rhs, lam, slot, coef),
        [(8, 64, 256), (2, 104, LANES)],
        hbm_in=2,
        sems=9,
    )
    to_l, to_r = call(rim_kernel, [vm(20, 8, LANES)] * 2, (src, coef, yd, yu))
    xl = ring(to_r, "sx", 1)
    xr = ring(to_l, "sx", -1)
    rin, sin = call(
        first_inner_kernel,
        [vm(8 * 192, LANES), vm(10, 104, 256)],
        (src, yd, yu, a1),
        [(8, 104, 256)],
    )

    side = vm(10, 3, 8, LANES)
    rout, w, to_d, to_u = call(
        first_kernel,
        [vm(2 * 192, LANES), vm(1920, LANES), side, side],
        (xl, xr, sin, dinv, a1, a2),
        [(2, 104, 256), (10, 104, 256)],
    )
    d = ring(to_u, "sy", 1)
    u = ring(to_d, "sy", -1)
    to_a, to_b = call(edge_kernel, [vm(3, 20, 8, LANES)] * 2, (w, d, u))
    a = snake(to_a, 1)
    b = snake(to_b, -1)
    hin, sin = call(
        second_inner_kernel,
        [vm(6, 20, 8, LANES), vm(10, 104, 256)],
        (rin, coef, yd, yu, w, d, u, a1),
        [(4, 5, 8, LANES), (4 * 192, LANES), (4, 104, 256)],
    )

    slab = vm(2, 18, 8, LANES)
    side = vm(10, 2, 8, LANES)
    c, to_a, to_b, own_d, own_u = call(
        second_kernel,
        [vm(10, 18, 8, LANES), slab, slab, side, side],
        (rin, rout, coef, xl, xr, yd, yu, w, a, b, d, u, hin, sin, dinv, a1, a2),
        [
            (6, 20, 8, LANES),
            (3, 4, 5, 8, LANES),
            (6 * 192, LANES),
            (6, 104, 256),
            (10, 104, 256),
            (1920, LANES),
        ],
    )
    a = snake(to_a, 1)
    b = snake(to_b, -1)
    edge = vm(2, 8, 8, LANES)
    ny = lax.axis_size("sy")
    smooth, res, rin, mom, pick, member = call(
        middle_inner_kernel,
        [sd(8, 64, 256), sd(8, 64, 256), vm(4, 64, 256), vm(16, 256), vm(ny, 512), vm(16, 512)],
        (src, coef, yd, yu, c, slot, wm),
        [(6, 18, 8, LANES), (6, 48, 256), (4, 32, 256)],
        hbm_out=2,
        sems=2,
    )
    uout, rout, to_d, to_u, part = call(
        middle_kernel,
        [vm(2, 16, 8, LANES), vm(4, 64, 256), edge, edge, vm(ny, LANES)],
        (src, coef, yd, yu, c, a, b, own_d, own_u, mom, pick, member, wm, wr),
        [(10, 18, 8, LANES), (256, 256), (2, 10, 2, 8, LANES)],
    )
    d = ring(to_u, "sy", 1)
    u = ring(to_d, "sy", -1)
    arrived = lax.all_to_all(part, "sy", split_axis=0, concat_axis=0, tiled=True)
    smooth, res, coarse = call(
        last_kernel,
        [sd(8, 64, 256), sd(8, 64, 256), sd(8, GRP_DEV)],
        (smooth, res, c, uout, rin, rout, coef, d, u, slot, arrived),
        [(8, 64, 256), (8, 64, 256), (8, GRP_DEV)],
        hbm_in=2,
        hbm_out=3,
        sems=9,
        alias=2,
    )
    return smooth.reshape(8, 8, 8, 256), res.reshape(8, 8, 8, 256), coarse


def solution(mesh):
    split_all = P(None, None, None, ("sx", "sy"))
    flat = P(("sx", "sy"))
    return jax.shard_map(
        on_device,
        mesh=mesh,
        in_specs=(split_all, P(None, ("sx", "sy")), flat, flat, flat),
        out_specs=(split_all, split_all, P(None, ("sx", "sy"))),
        check_vma=False,
    )
```

```python
import jax
import jax.numpy as jnp
import numpy as np
from jax import lax
from jax.experimental import pallas as pl
from jax.experimental.pallas import tpu as pltpu
from jax.sharding import PartitionSpec as P

NODES = 8
GRP_DEV = 16
LANES = 128
RELAX = 0.35
F32 = jnp.float32
BF16 = jnp.bfloat16


def split_np(a):
    a = np.asarray(a, np.float32)
    hi = np.asarray(jnp.asarray(a).astype(BF16).astype(F32))
    return hi, a - hi


def constants():
    n = NODES + 2
    col = np.arange(n, dtype=np.float64) + 1.0
    s = np.sqrt(2.0 / (n + 1.0)) * np.sin(np.pi * col[:, None] * col[None, :] / (n + 1.0))
    lam = 2.0 - 2.0 * np.cos(np.pi * col / (n + 1.0))
    fwd = np.zeros((104, 112))
    for q in range(n):
        for r in range(n):
            c = q * 8 + r - 1
            if r == 0:
                c = 80 + q
            if r == n - 1:
                c = 96 + q
            fwd[:100, c] = np.outer(s[:, q], s[:, r]).reshape(-1)
    fh, fl = split_np(fwd)
    a1 = np.concatenate([np.concatenate([fh, fh], 1), np.concatenate([fl, fl], 1)], 0)
    bh, bl = split_np(RELAX * fwd.T)
    a2 = np.concatenate([np.concatenate([bh, bh], 1), np.concatenate([bl, bl], 1)], 0)
    lam_j = np.ones((104, LANES), np.float32)
    lam_k = np.ones((104, LANES), np.float32)
    lam_j[:100] = np.repeat(lam, n)[:, None]
    lam_k[:100] = np.tile(lam, n)[:, None]
    t = np.arange(NODES) / (NODES - 1.0)
    w = np.stack([1.0 - t, t])
    wm = np.einsum("ax,by,cz->abcxyz", w, w, w).reshape(8, 512)
    wh, wl = split_np(wm)
    wm = np.concatenate([wh, wl], 0)
    rim = wm.reshape(16, 8, 8, 8)[:, :, [0, 1, 6, 7]].reshape(16, 256)
    return s, lam, a1, a2, lam_j, lam_k, wm, rim


SINES, LAM, A_FWD, A_BWD, LAM_J, LAM_K, W_MOM, W_RIM = constants()


def split(x):
    hi = x.astype(BF16)
    return hi, (x - hi.astype(F32)).astype(BF16)


def dot(a, b):
    return lax.dot_general(a, b, (((1,), (0,)), ((), ())), preferred_element_type=F32)


def dot_t(a, b):
    return lax.dot_general(a, b, (((1,), (1,)), ((), ())), preferred_element_type=F32)


def flags():
    i = lax.axis_index("sx")
    j = lax.axis_index("sy")
    nx = lax.axis_size("sx")
    ny = lax.axis_size("sy")
    one = lambda c: jnp.where(c, 1.0, 0.0).astype(F32)
    return one(i > 0), one(i < nx - 1), one(j > 0), one(j < ny - 1)


def even_row():
    return lax.rem(lax.axis_index("sy"), 2) == 0


class Picked:
    def __init__(self, first, second):
        self.refs = (first, second)

    def __getitem__(self, at):
        return jnp.where(even_row(), self.refs[0][at], self.refs[1][at])


def lane_up(x):
    lane = lax.broadcasted_iota(jnp.int32, x.shape, x.ndim - 1)
    return jnp.where(lane == LANES - 1, 0.0, pltpu.roll(x, LANES - 1, x.ndim - 1))


def lane_down(x):
    lane = lax.broadcasted_iota(jnp.int32, x.shape, x.ndim - 1)
    return jnp.where(lane == 0, 0.0, pltpu.roll(x, 1, x.ndim - 1))


def onehot(slot_row):
    p = lax.broadcasted_iota(jnp.int32, (256, 256), 0)
    return jnp.where(p == slot_row, 1.0, 0.0).astype(BF16)


def split3(a):
    a1 = a.astype(BF16)
    e = a - a1.astype(F32)
    a2 = e.astype(BF16)
    return a1, a2, (e - a2.astype(F32)).astype(BF16)


def start_kernel(
    rhs_hbm, stretch_hbm, mass_hbm, slot_hbm, group_hbm,
    coef_ref, to_down_ref, to_up_ref, slot_ref,
    face_ref, stretch_ref, mass_ref, group_ref, sems,
):
    pairs = (
        (slot_hbm, slot_ref),
        (rhs_hbm.at[:, pl.ds(0, 8), :], face_ref.at[0]),
        (rhs_hbm.at[:, pl.ds(56, 8), :], face_ref.at[1]),
        (stretch_hbm, stretch_ref),
        (mass_hbm, mass_ref),
        (group_hbm, group_ref),
    )
    copies = [pltpu.make_async_copy(h, v, sems.at[k]) for k, (h, v) in enumerate(pairs)]
    for c in copies:
        c.start()
    copies[0].wait()
    oh = onehot(slot_ref[...])
    for k, out, b in ((1, to_down_ref, 0), (2, to_up_ref, 1)):
        copies[k].wait()
        g = dot_t(jnp.concatenate(split3(face_ref[k - 1].reshape(64, 256)), 0), oh)
        g = g[0:64] + g[64:128] + g[128:192]
        out[0:8] = g[:, b * LANES : (b + 1) * LANES].reshape(8, 8, LANES)
    for c in copies[3:]:
        c.wait()
    c = jnp.concatenate(
        [
            stretch_ref[...],
            mass_ref[...],
            group_ref[...].astype(F32),
            jnp.zeros((3, 256), F32),
        ],
        0,
    )
    c1, c2, c3 = split3(c)
    cg = dot_t(c1, oh) + dot_t(c2, oh) + dot_t(c3, oh)
    coef = jnp.concatenate([cg[0:4, :LANES], cg[0:4, LANES:]], 0)
    gr = jnp.concatenate([cg[4:5, :LANES], cg[4:5, LANES:], jnp.zeros((6, LANES), F32)], 0)
    coef_ref[0] = coef
    coef_ref[1] = gr
    pad = jnp.zeros((3, LANES), F32)
    to_down_ref[8] = jnp.concatenate([coef[0:4], gr[0:1], pad], 0)
    to_up_ref[8] = jnp.concatenate([coef[4:8], gr[1:2], pad], 0)


def place_kernel(lam_hbm, rhs_ref, slot_ref, coef_ref, src_ref, dinv_ref, lam_ref, sems):
    lam = pltpu.make_async_copy(lam_hbm, lam_ref, sems.at[0])
    lam.start()
    oh = onehot(slot_ref[...])
    for x in range(8):
        g = dot_t(jnp.concatenate(split3(rhs_ref[x]), 0), oh)
        g = g[0:64] + g[64:128] + g[128:192]
        for b in range(2):
            src_ref[x, b * 8 : b * 8 + 8] = g[:, b * LANES : (b + 1) * LANES].reshape(8, 8, LANES)
    lam.wait()
    for b in range(2):
        lanes = slice(b * LANES, (b + 1) * LANES)
        cx, cy, cz, m, _ = rows_of(coef_ref[0], b * 4)
        cxl = [cx * float(v) for v in LAM]
        for t in range(13):
            row = slice(t * 8, t * 8 + 8)
            d0 = cy * lam_ref[0, row, :] + cz * lam_ref[1, row, :] + m
            for i in range(10):
                dinv_ref[i, row, lanes] = 1.0 / (d0 + cxl[i])


def rim_kernel(src_ref, coef_ref, yd_ref, yu_ref, to_a_ref, to_b_ref):
    coef_y = jnp.concatenate([yd_ref[8, 0:4, :], yu_ref[8, 0:4, :]], 0)
    even = even_row()
    coef = coef_ref[0]
    for out, x_even, x_odd in ((to_a_ref, 7, 0), (to_b_ref, 0, 7)):
        pick = lambda ref: jnp.where(even, ref[x_even], ref[x_odd])
        out[0] = pick(yd_ref)
        out[1:17] = pick(src_ref)
        out[17] = pick(yu_ref)
        out[18] = coef
        out[19] = coef_y


def forward(res, base, a1_ref):
    ends = []
    for z, shift in ((7, lane_down), (0, lane_up)):
        ends.append([shift(res[pl.ds(base + 64 * t + z, 8, stride=8), :]) for t in range(3)])
    halves = [
        jnp.concatenate(
            [res[base + 64 * b : base + 64 * b + 80, :]] + ends[0][b : b + 2] + ends[1][b : b + 2],
            0,
        )
        for b in range(2)
    ]
    hi, lo = split(jnp.concatenate(halves, 1))
    r = dot(a1_ref[...], jnp.concatenate([hi, lo], 0))
    return r[:104] + r[104:]


def along_x(layers, partial, row, lanes):
    acc = [None if partial is None else partial[i, row, lanes] for i in range(10)]
    for p, (low, high) in layers.items():
        v = low[0][low[1], row, lanes]
        w = high[0][high[1], row, lanes]
        h = (v + w, v - w)
        for i in range(10):
            term = h[i % 2] * float(SINES[i, p])
            acc[i] = term if acc[i] is None else acc[i] + term
    return acc


def partial_x(layers, out_ref):
    for b in range(2):
        lanes = slice(b * LANES, (b + 1) * LANES)

        def chunk(t, carry):
            row = pl.ds(pl.multiple_of(t * 8, 8), 8)
            for i, v in enumerate(along_x(layers, None, row, lanes)):
                out_ref[i, row, lanes] = v
            return carry

        lax.fori_loop(0, 13, chunk, 0)


def finish_solves(layers, partial, dinv_ref, a2_ref, spec, wout):
    for b in range(2):
        lanes = slice(b * LANES, (b + 1) * LANES)

        def chunk(t, carry):
            row = pl.ds(pl.multiple_of(t * 8, 8), 8)
            z = along_x(layers, partial, row, lanes)
            z = [z[i] * dinv_ref[i, row, lanes] for i in range(10)]
            for p in range(5):
                e = z[0] * float(SINES[0, p])
                o = z[1] * float(SINES[1, p])
                for i in range(2, 10, 2):
                    e = e + z[i] * float(SINES[i, p])
                    o = o + z[i + 1] * float(SINES[i + 1, p])
                spec[p, row, lanes] = e + o
                spec[9 - p, row, lanes] = e - o
            return carry

        lax.fori_loop(0, 13, chunk, 0)

    for p in range(10):
        base = p * 192
        hi, lo = split(spec[p])
        r = dot(a2_ref[...], jnp.concatenate([hi, lo], 0))
        r = r[:112] + r[112:]
        r0 = r[:, :LANES]
        r1 = r[:, LANES:]
        wout[base : base + 64, :] = r0[0:64]
        wout[base + 64 : base + 80, :] = r0[64:80] + r1[0:16]
        wout[base + 80 : base + 144, :] = r1[16:80]
        wout[base + 144 : base + 192, :] = jnp.zeros((48, LANES), F32)
        for off, z, shift in ((80, 7, lane_up), (96, 0, lane_down)):
            rows = [
                r0[off : off + 8],
                r0[off + 8 : off + 16] + r1[off : off + 8],
                r1[off + 8 : off + 16],
            ]
            for t in range(3):
                at = pl.ds(base + 64 * t + z, 8, stride=8)
                wout[at, :] = wout[at, :] + shift(rows[t])


def put(ref, p, y, value):
    n = value.shape[0]
    at = (p * 24 + y) * 8
    ref[at : at + n * 8, :] = value.reshape(n * 8, LANES)


def get(ref, p, y, n):
    at = (p * 24 + y) * 8
    return ref[at : at + n * 8, :].reshape(n, 8, LANES)


def with_rows(line, n, d, u, down, up):
    rows_d = d * down
    rows_u = u * up
    low = rows_d[n - 2 : n] + jnp.concatenate([line[0:1] * down, line[1:2]], 0)
    high = rows_u[0:2] + jnp.concatenate([line[16:17], line[17:18] * up], 0)
    parts = [low, line[2:16], high]
    if n > 2:
        parts = [rows_d[0 : n - 2]] + parts + [rows_u[2:n]]
    return jnp.concatenate(parts, 0)


def put_layer(ref, at, below, line, above):
    put(ref, at, 0, below)
    put(ref, at, 1, line)
    put(ref, at, 17, above)
    put(ref, at, 18, jnp.zeros((6, 8, LANES), F32))


def first_inner_kernel(src_ref, yd_ref, yu_ref, a1_ref, rin_ref, sin_ref, sout):
    _, _, down, up = flags()
    for x in range(8):
        put_layer(rin_ref, x, yd_ref[x : x + 1] * down, src_ref[x], yu_ref[x : x + 1] * up)
        sout[x] = forward(rin_ref, x * 192, a1_ref)
    partial_x({p: ((sout, p - 1), (sout, 8 - p)) for p in range(1, 5)}, sin_ref)


def first_kernel(
    xa_ref, xb_ref, sin_ref, dinv_ref, a1_ref, a2_ref,
    rout_ref, wout, to_down_ref, to_up_ref, sout, spec,
):
    left, right, down, up = flags()
    x_refs = Picked(xa_ref, xb_ref), Picked(xb_ref, xa_ref)
    for k, (x_ref, side) in enumerate(zip(x_refs, (left, right))):
        put_layer(
            rout_ref,
            k,
            x_ref[0:1] * (side * down),
            x_ref[1:17] * side,
            x_ref[17:18] * (side * up),
        )
        sout[k] = forward(rout_ref, k * 192, a1_ref)
    finish_solves({0: ((sout, 0), (sout, 1))}, sin_ref, dinv_ref, a2_ref, spec, wout)
    for p in range(10):
        to_down_ref[p] = get(wout, p, 0, 3)
        to_up_ref[p] = get(wout, p, 15, 3)


def edge_kernel(w_ref, d_ref, u_ref, a_ref, b_ref):
    _, _, down, up = flags()
    even = even_row()
    for k in range(3):
        to_l, to_r = [
            with_rows(get(w_ref, p, 0, 18), 3, d_ref[p], u_ref[p], down, up) for p in (k, 7 + k)
        ]
        a_ref[k] = jnp.where(even, to_r, to_l)
        b_ref[k] = jnp.where(even, to_l, to_r)


def neighbours_z(u):
    z = lax.broadcasted_iota(jnp.int32, u.shape, 1)
    s = pltpu.roll(u, 7, 1)
    above = jnp.where(z == 7, lane_up(s), s)
    s = pltpu.roll(u, 1, 1)
    below = jnp.where(z == 0, lane_down(s), s)
    return above, below


ROWS = ((0, 1, 0), (1, 4, 1), (5, 4, 1), (9, 4, 2), (13, 4, 2), (17, 1, 3))


def second_residual(get_h, get_r, cb, p, at, res_ref, left, right, down, up):
    for y, n, b in ROWS:
        v = get_h(p + 1, y + 1, n)
        res = get_r(y, n) - stencil(
            cb[b],
            v,
            get_h(p + 2, y + 1, n) + get_h(p, y + 1, n),
            get_h(p + 1, y + 2, n) + get_h(p + 1, y, n),
        )
        if p == 0:
            res = res * left
        if p == 9:
            res = res * right
        if y == 0:
            res = res * down
        if y == 17:
            res = res * up
        put(res_ref, at, y, res)
    put(res_ref, at, 18, jnp.zeros((6, 8, LANES), F32))


def spread_coefs(cb, rows):
    for b, (tile, at) in enumerate(rows):
        for k, v in enumerate(rows_of(tile, at)):
            cb[b, k] = v
    return [[cb.at[b, k] for k in range(5)] for b in range(4)]


class Loaded:
    def __init__(self, refs):
        self.refs = refs

    def __getitem__(self, k):
        return self.refs[k][...]


def second_inner_kernel(
    rin_ref, coef_ref, yd_ref, yu_ref, w_ref, d_ref, u_ref, a1_ref, h_ref, sin_ref, cb, r1, sout,
):
    left, right, down, up = flags()
    for x in range(3, 9):
        h_ref[x - 3] = with_rows(get(w_ref, x - 1, 0, 18), 3, d_ref[x - 1], u_ref[x - 1], down, up)
    tiles = spread_coefs(
        cb, ((yd_ref[8], 0), (coef_ref[0], 0), (coef_ref[0], 4), (yu_ref[8], 0))
    )
    coefs = [Loaded(t) for t in tiles]
    get_h = lambda x, y, n: h_ref[x - 3, y : y + n]
    for k in range(4):
        p = 3 + k
        get_r = lambda y, n: get(rin_ref, p - 1, y, n)
        second_residual(get_h, get_r, coefs, p, k, r1, left, right, down, up)
        sout[k] = forward(r1, k * 192, a1_ref)
    partial_x({p: ((sout, p - 3), (sout, 6 - p)) for p in (3, 4)}, sin_ref)


def second_kernel(
    rin_ref, rout_ref, coef_ref, xa_ref, xb_ref, yd_ref, yu_ref, w_ref, a_ref, b_ref, d_ref, u_ref,
    hin_ref, sin_ref, dinv_ref, a1_ref, a2_ref,
    c_ref, to_a_ref, to_b_ref, own_down_ref, own_up_ref, h, cb, r1, sout, spec, wout,
):
    left, right, down, up = flags()
    l_ref, r_ref = Picked(a_ref, b_ref), Picked(b_ref, a_ref)
    for x in (0, 1, 2, 9, 10, 11):
        if x == 0:
            g = l_ref[0] * left
        elif x == 11:
            g = r_ref[2] * right
        else:
            g = with_rows(get(w_ref, x - 1, 0, 18), 3, d_ref[x - 1], u_ref[x - 1], down, up)
            if x == 1:
                g = (g + l_ref[1]) * left
            elif x == 2:
                g = g + l_ref[2] * left
            elif x == 9:
                g = g + r_ref[0] * right
            elif x == 10:
                g = (g + r_ref[1]) * right
        h[x if x < 3 else x - 6] = g

    def get_h(x, y, n):
        if 3 <= x <= 8:
            return hin_ref[x - 3, y : y + n]
        return h[x if x < 3 else x - 6, y : y + n]

    coefs = []
    for a, x_ref in ((0, Picked(xa_ref, xb_ref)), (1, None), (2, Picked(xb_ref, xa_ref))):
        if x_ref is None:
            rows = ((yd_ref[8], 0), (coef_ref[0], 0), (coef_ref[0], 4), (yu_ref[8], 0))
        else:
            own, beside = x_ref[18], x_ref[19]
            rows = ((beside, 0), (own, 0), (own, 4), (beside, 4))
        coefs.append([Loaded(t) for t in spread_coefs(cb.at[a], rows)])
    for k, p in enumerate((0, 1, 2, 7, 8, 9)):
        if p in (0, 9):
            get_r = lambda y, n: get(rout_ref, 0 if p == 0 else 1, y, n)
        else:
            get_r = lambda y, n: get(rin_ref, p - 1, y, n)
        cb_p = coefs[0 if p == 0 else 2 if p == 9 else 1]
        second_residual(get_h, get_r, cb_p, p, k, r1, left, right, down, up)
        sout[k] = forward(r1, k * 192, a1_ref)
    layers = {p: ((sout, p), (sout, 5 - p)) for p in range(3)}
    finish_solves(layers, sin_ref, dinv_ref, a2_ref, spec, wout)
    for p in range(10):
        line = get(wout, p, 0, 18)
        c_ref[p] = get_h(p + 1, 1, 18) + line
        own_down_ref[p] = line[0:2]
        own_up_ref[p] = line[16:18]
    even = even_row()
    for k in range(2):
        to_l, to_r = get(wout, k, 0, 18), get(wout, 8 + k, 0, 18)
        to_a_ref[k] = jnp.where(even, to_r, to_l)
        to_b_ref[k] = jnp.where(even, to_l, to_r)


def add_x(g, p, l, r, left, right, y=slice(0, 18)):
    if p == 0:
        return (g + l[0, y]) * left
    if p == 1:
        return g + l[1, y] * left
    if p == 8:
        return g + r[0, y] * right
    if p == 9:
        return (g + r[1, y]) * right
    return g


def rows_of(tile, at):
    c = [jnp.broadcast_to(tile[at + k : at + k + 1, :], (8, LANES)) for k in range(4)]
    return c + [2.0 * (c[0] + c[1] + c[2]) + c[3]]


def stencil(cf, v, x_sum, y_sum):
    above, below = neighbours_z(v)
    return cf[4] * v - cf[0] * x_sum - cf[1] * y_sum - cf[2] * (above + below)


def column_residual(get_h, src_ref, cf, x, b, mr_ref, at):
    lanes = slice(b * LANES, (b + 1) * LANES)
    for y in (0, 4):
        yy = b * 8 + y + 1
        p = x + 1
        v = get_h(p, yy, 4)
        res = src_ref[x, yy - 1 : yy + 3] - stencil(
            cf,
            v,
            get_h(p + 1, yy, 4) + get_h(p - 1, yy, 4),
            get_h(p, yy + 1, 4) + get_h(p, yy - 1, 4),
        )
        mr_ref[at, y * 8 : y * 8 + 32, lanes] = res.reshape(32, LANES)


def moments(wm_ref, x, rows):
    rh, rl = split(rows)
    w = wm_ref[:, x * 64 : x * 64 + rows.shape[0]]
    return dot(w, rh) + dot(w, rl)


def to_slots(uv, oh):
    hi, lo = split(uv)
    n = uv.shape[0]
    o = dot(jnp.concatenate([hi, lo], 0), oh)
    return o[:n] + o[n:]


def middle_inner_kernel(
    src_ref, coef_ref, yd_ref, yu_ref, c_ref, slot_ref, wm_ref,
    smooth_hbm, res_hbm, mr_ref, mom_ref, pick_ref, member_ref, h, smooth_ref, res_ref, sems,
):
    _, _, down, up = flags()
    oh = onehot(slot_ref[...])
    copies = []
    for x in range(1, 7):
        both = [c_ref[x + 1, 8 * b + 2 : 8 * b + 8].reshape(48, LANES) for b in range(2)]
        smooth_ref[x - 1] = to_slots(jnp.concatenate(both, 1), oh)
    copies.append(
        pltpu.make_async_copy(smooth_ref, smooth_hbm.at[pl.ds(1, 6), pl.ds(8, 48), :], sems.at[0])
    )
    copies[0].start()
    for k in range(6):
        h[k] = c_ref[k + 2]
        h[k, 0] = c_ref[k + 2, 0] * down
        h[k, 17] = c_ref[k + 2, 17] * up
    get_h = lambda p, y, n: h[p - 2, y : y + n]
    coefs = [rows_of(coef_ref[0], 0), rows_of(coef_ref[0], 4)]
    for k in range(4):
        for b in range(2):
            column_residual(get_h, src_ref, coefs[b], 2 + k, b, mr_ref, k)
        res_ref[k] = to_slots(mr_ref[k, 16:48, :], oh)
    copies.append(
        pltpu.make_async_copy(res_ref, res_hbm.at[pl.ds(2, 4), pl.ds(16, 32), :], sems.at[1])
    )
    copies[1].start()
    mom = jnp.zeros((16, 256), F32)
    for k in (0, 2):
        mom = mom + moments(wm_ref, 2 + k, mr_ref[k : k + 2].reshape(128, 256))
    mom_ref[...] = mom
    gr = coef_ref[1]
    group = jnp.concatenate([gr[0:1], gr[1:2], yd_ref[8, 4:5, :], yu_ref[8, 4:5, :]], 1)
    ny = pick_ref.shape[0]
    col = (group + 0.5).astype(jnp.int32) - lax.axis_index("sx") * (ny * GRP_DEV)
    owner = lax.shift_right_logical(col, 4)
    member = jnp.bitwise_and(col, 15)
    sel = lax.broadcasted_iota(jnp.int32, (ny, 512), 0)
    pick_ref[...] = jnp.where(sel == owner, 1.0, 0.0)
    sel = lax.broadcasted_iota(jnp.int32, (16, 512), 0)
    member_ref[...] = jnp.where(sel == member, 1.0, 0.0)
    for c in copies:
        c.wait()


def middle_kernel(
    src_ref, coef_ref, yd_ref, yu_ref, c_ref, a_ref, b_ref, own_down_ref, own_up_ref,
    mom_ref, pick_ref, member_ref, wm_ref, wr_ref,
    u_ref, mr_ref, to_down_ref, to_up_ref, part_ref, h, rim, edge,
):
    left, right, down, up = flags()
    l_ref, r_ref = Picked(a_ref, b_ref), Picked(b_ref, a_ref)
    for p in range(10):
        e = add_x(own_down_ref[p], p, l_ref, r_ref, left, right, slice(0, 2))
        edge[0, p] = jnp.concatenate([e[0:1] * down, e[1:2]], 0)
        e = add_x(own_up_ref[p], p, l_ref, r_ref, left, right, slice(16, 18))
        edge[1, p] = jnp.concatenate([e[0:1], e[1:2] * up], 0)
        if 3 < p < 6:
            continue
        g = add_x(c_ref[p], p, l_ref, r_ref, left, right)
        h[p] = g
        h[p, 0] = g[0] * down
        h[p, 17] = g[17] * up
    u_ref[0] = h[1, 1:17]
    u_ref[1] = h[8, 1:17]
    get_h = lambda p, y, n: h[p, y : y + n]
    coefs = [rows_of(coef_ref[0], 0), rows_of(coef_ref[0], 4)]
    for k, x in enumerate((0, 1, 6, 7)):
        for b in range(2):
            column_residual(get_h, src_ref, coefs[b], x, b, mr_ref, k)
    rim[...] = jnp.zeros((256, 256), F32)
    for k, out, far, near, tile, lanes, y_far, y_near in (
        (0, to_down_ref, 0, 1, yd_ref, slice(0, LANES), 2, 3),
        (1, to_up_ref, 1, 0, yu_ref, slice(LANES, 256), 1, 0),
    ):
        slab = edge.at[k]
        cf = rows_of(tile[8], 0)
        for x in range(8):
            p = x + 1
            v = slab[p, far : far + 1]
            res = stencil(
                cf,
                v,
                slab[p + 1, far : far + 1] + slab[p - 1, far : far + 1],
                slab[p, near : near + 1],
            )
            out[0, x] = v[0]
            out[1, x] = -res[0]
            at = (x * 4 + y_near) * 8
            rim[at : at + 8, lanes] = -res[0]
            at = (x * 4 + y_far) * 8
            rim[at : at + 8, lanes] = cf[1] * v[0]
    mom = mom_ref[...]
    mom = mom + moments(wm_ref, 0, mr_ref[0:2].reshape(128, 256))
    mom = mom + moments(wm_ref, 6, mr_ref[2:4].reshape(128, 256))
    rh, rl = split(rim[...])
    mom_y = dot(wr_ref[...], rh) + dot(wr_ref[...], rl)
    mom_y = mom_y[0:8] + mom_y[8:16]
    mom = jnp.concatenate(
        [mom[0:8] + mom[8:16], mom_y[:, :LANES] * down, mom_y[:, LANES:] * up], 1
    )
    member = member_ref[...]
    spread = jnp.concatenate([member * mom[v : v + 1] for v in range(8)], 0)
    sh, sl = split(spread)
    pick = pick_ref[...].astype(BF16)
    part_ref[...] = dot_t(pick, sh) + dot_t(pick, sl)


def last_kernel(
    smooth_in, res_in, c_ref, uout_ref, rin_ref, rout_ref, coef_ref, d_ref, u_ref, slot_ref,
    arrived_ref,
    smooth_hbm, res_hbm, coarse_hbm, smooth_ref, res_ref, coarse_ref, sems,
):
    _, _, down, up = flags()
    total = jnp.sum(arrived_ref[...], axis=0, keepdims=True)
    for v in range(8):
        coarse_ref[v : v + 1, :] = total[:, v * GRP_DEV : (v + 1) * GRP_DEV]
    copies = [pltpu.make_async_copy(coarse_ref, coarse_hbm, sems.at[8])]
    copies[0].start()

    def send(ref, hbm, x, nx, row, rows):
        at = (pl.ds(x, nx), pl.ds(row, rows), slice(None))
        k = len(copies) - 1
        copies.append(pltpu.make_async_copy(ref.at[at], hbm.at[at], sems.at[k]))
        copies[-1].start()

    oh = onehot(slot_ref[...])
    sides = (
        (d_ref, down, jnp.broadcast_to(coef_ref[0, 1:2, :], (8, LANES))),
        (u_ref, up, jnp.broadcast_to(coef_ref[0, 5:6, :], (8, LANES))),
    )

    def added(x):
        out = []
        for slab, on, cy in sides:
            v = slab[0, x] * on
            out.append((v, slab[1, x] * on, cy * v))
        return out

    zero = jnp.zeros((8, LANES), F32)
    pairs = [added(x) for x in range(8)]
    for k, x in enumerate((0, 1, 6, 7)):
        (_, d0, d1), (_, e0, e1) = pairs[x]
        add = jnp.concatenate(
            [
                jnp.concatenate([d0, d1] + [zero] * 6, 0),
                jnp.concatenate([zero] * 6 + [e1, e0], 0),
            ],
            1,
        )
        res_ref[x] = to_slots(rout_ref[k] + add, oh)
        if k == 1:
            send(res_ref, res_hbm, 0, 2, 0, 64)
    send(res_ref, res_hbm, 6, 2, 0, 64)
    low, high = [], []
    for k in range(4):
        (_, d0, d1), (_, e0, e1) = pairs[2 + k]
        z2 = jnp.zeros((16, LANES), F32)
        low.append(
            rin_ref[k, 0:16, :] + jnp.concatenate([jnp.concatenate([d0, d1], 0), z2], 1)
        )
        high.append(
            rin_ref[k, 48:64, :] + jnp.concatenate([z2, jnp.concatenate([e1, e0], 0)], 1)
        )
    res_ref[2:6, 0:16, :] = to_slots(jnp.concatenate(low, 0), oh).reshape(4, 16, 256)
    send(res_ref, res_hbm, 2, 4, 0, 16)
    res_ref[2:6, 48:64, :] = to_slots(jnp.concatenate(high, 0), oh).reshape(4, 16, 256)
    send(res_ref, res_hbm, 2, 4, 48, 16)
    for k, x in enumerate((0, 7)):
        (d0, _, _), (e0, _, _) = pairs[x]
        both = [uout_ref[k, 0:8].reshape(64, LANES), uout_ref[k, 8:16].reshape(64, LANES)]
        both[0] = both[0] + jnp.concatenate([d0] + [zero] * 7, 0)
        both[1] = both[1] + jnp.concatenate([zero] * 7 + [e0], 0)
        smooth_ref[x] = to_slots(jnp.concatenate(both, 1), oh)
        send(smooth_ref, smooth_hbm, x, 1, 0, 64)
    low, high = [], []
    for x in range(1, 7):
        (d0, _, _), (e0, _, _) = pairs[x]
        c = [c_ref[x + 1, y] for y in (1, 9, 8, 16)]
        low.append(jnp.concatenate([c[0] + d0, c[1]], 1))
        high.append(jnp.concatenate([c[2], c[3] + e0], 1))
    smooth_ref[1:7, 0:8, :] = to_slots(jnp.concatenate(low, 0), oh).reshape(6, 8, 256)
    send(smooth_ref, smooth_hbm, 1, 6, 0, 8)
    smooth_ref[1:7, 56:64, :] = to_slots(jnp.concatenate(high, 0), oh).reshape(6, 8, 256)
    send(smooth_ref, smooth_hbm, 1, 6, 56, 8)
    for c in copies:
        c.wait()


def sd(*shape):
    return jax.ShapeDtypeStruct(shape, F32)


def vm(*shape):
    return pltpu.VMEM(shape, F32)


def ring(value, axis, by):
    n = lax.axis_size(axis)
    return lax.ppermute(value, axis, [(i, (i + by) % n) for i in range(n)])


def snake(value, by):
    nx = lax.axis_size("sx")
    ny = lax.axis_size("sy")
    pairs = []
    for i in range(nx):
        for j in range(ny):
            to = i + (by if j % 2 == 0 else -by)
            target = to * ny + j if 0 <= to < nx else i * ny + (j ^ 1)
            pairs.append((i * ny + j, target))
    return lax.ppermute(value, ("sx", "sy"), pairs)


def call(kernel, outs, args, scratch=(), hbm_in=0, hbm_out=0, sems=0, alias=0):
    vmem = pl.BlockSpec(memory_space=pltpu.VMEM)
    hbm = pl.BlockSpec(memory_space=pltpu.HBM)
    args = [
        pltpu.with_memory_space_constraint(a, pltpu.HBM if k < hbm_in else pltpu.VMEM)
        for k, a in enumerate(args)
    ]
    scratch = [pltpu.VMEM(s, F32) if isinstance(s, tuple) else s for s in scratch]
    if sems:
        scratch.append(pltpu.SemaphoreType.DMA((sems,)))
    return pl.pallas_call(
        kernel,
        out_shape=outs,
        in_specs=[hbm if k < hbm_in else vmem for k in range(len(args))],
        out_specs=[hbm if k < hbm_out else vmem for k in range(len(outs))],
        scratch_shapes=scratch,
        input_output_aliases={k: k for k in range(alias)},
        compiler_params=pltpu.CompilerParams(vmem_limit_bytes=16 << 20),
    )(*args)


def on_device(right_side, stretch, mass_term, slot_position, coarse_group):
    a1 = jnp.asarray(A_FWD, BF16)
    a2 = jnp.asarray(A_BWD, BF16)
    lam = jnp.asarray(np.stack([LAM_J, LAM_K]), F32)
    wm = jnp.asarray(W_MOM, BF16)
    wr = jnp.asarray(W_RIM, BF16)
    row = pltpu.VMEM((1, 256), jnp.int32)
    rhs = right_side.reshape(8, 64, 256)
    coef, to_d, to_u, slot = call(
        start_kernel,
        [vm(2, 8, LANES), vm(9, 8, LANES), vm(9, 8, LANES), row],
        (
            rhs,
            stretch,
            mass_term.reshape(1, 256),
            slot_position.reshape(1, 256),
            coarse_group.reshape(1, 256),
        ),
        [(2, 8, 8, 256), (3, 256), (1, 256), row],
        hbm_in=5,
        sems=6,
    )
    yd = ring(to_u, "sy", 1)
    yu = ring(to_d, "sy", -1)
    src, dinv = call(
        place_kernel,
        [vm(8, 16, 8, LANES), vm(10, 104, 256)],
        (lam, rhs, slot, coef),
        [(2, 104, LANES)],
        hbm_in=1,
        sems=1,
    )
    to_a, to_b = call(rim_kernel, [vm(20, 8, LANES)] * 2, (src, coef, yd, yu))
    xa = snake(to_a, 1)
    xb = snake(to_b, -1)
    rin, sin = call(
        first_inner_kernel,
        [vm(8 * 192, LANES), vm(10, 104, 256)],
        (src, yd, yu, a1),
        [(8, 104, 256)],
    )

    side = vm(10, 3, 8, LANES)
    rout, w, to_d, to_u = call(
        first_kernel,
        [vm(2 * 192, LANES), vm(1920, LANES), side, side],
        (xa, xb, sin, dinv, a1, a2),
        [(2, 104, 256), (10, 104, 256)],
    )
    d = ring(to_u, "sy", 1)
    u = ring(to_d, "sy", -1)
    to_a, to_b = call(edge_kernel, [vm(3, 20, 8, LANES)] * 2, (w, d, u))
    a = snake(to_a, 1)
    b = snake(to_b, -1)
    hin, sin = call(
        second_inner_kernel,
        [vm(6, 20, 8, LANES), vm(10, 104, 256)],
        (rin, coef, yd, yu, w, d, u, a1),
        [(4, 5, 8, LANES), (4 * 192, LANES), (4, 104, 256)],
    )

    slab = vm(2, 18, 8, LANES)
    side = vm(10, 2, 8, LANES)
    c, to_a, to_b, own_d, own_u = call(
        second_kernel,
        [vm(10, 18, 8, LANES), slab, slab, side, side],
        (rin, rout, coef, xa, xb, yd, yu, w, a, b, d, u, hin, sin, dinv, a1, a2),
        [
            (6, 20, 8, LANES),
            (3, 4, 5, 8, LANES),
            (6 * 192, LANES),
            (6, 104, 256),
            (10, 104, 256),
            (1920, LANES),
        ],
    )
    a = snake(to_a, 1)
    b = snake(to_b, -1)
    edge = vm(2, 8, 8, LANES)
    ny = lax.axis_size("sy")
    smooth, res, rin, mom, pick, member = call(
        middle_inner_kernel,
        [sd(8, 64, 256), sd(8, 64, 256), vm(4, 64, 256), vm(16, 256), vm(ny, 512), vm(16, 512)],
        (src, coef, yd, yu, c, slot, wm),
        [(6, 18, 8, LANES), (6, 48, 256), (4, 32, 256)],
        hbm_out=2,
        sems=2,
    )
    uout, rout, to_d, to_u, part = call(
        middle_kernel,
        [vm(2, 16, 8, LANES), vm(4, 64, 256), edge, edge, vm(ny, LANES)],
        (src, coef, yd, yu, c, a, b, own_d, own_u, mom, pick, member, wm, wr),
        [(10, 18, 8, LANES), (256, 256), (2, 10, 2, 8, LANES)],
    )
    d = ring(to_u, "sy", 1)
    u = ring(to_d, "sy", -1)
    arrived = lax.all_to_all(part, "sy", split_axis=0, concat_axis=0, tiled=True)
    smooth, res, coarse = call(
        last_kernel,
        [sd(8, 64, 256), sd(8, 64, 256), sd(8, GRP_DEV)],
        (smooth, res, c, uout, rin, rout, coef, d, u, slot, arrived),
        [(8, 64, 256), (8, 64, 256), (8, GRP_DEV)],
        hbm_in=2,
        hbm_out=3,
        sems=9,
        alias=2,
    )
    return smooth.reshape(8, 8, 8, 256), res.reshape(8, 8, 8, 256), coarse


def solution(mesh):
    split_all = P(None, None, None, ("sx", "sy"))
    flat = P(("sx", "sy"))
    return jax.shard_map(
        on_device,
        mesh=mesh,
        in_specs=(split_all, P(None, ("sx", "sy")), flat, flat, flat),
        out_specs=(split_all, split_all, P(None, ("sx", "sy"))),
        check_vma=False,
    )
```

```python
import jax
import jax.numpy as jnp
import numpy as np
from jax import lax
from jax.experimental import pallas as pl
from jax.experimental.pallas import tpu as pltpu
from jax.sharding import PartitionSpec as P

NODES = 8
GRP_DEV = 16
LANES = 128
RELAX = 0.35
F32 = jnp.float32
BF16 = jnp.bfloat16


def split_np(a):
    a = np.asarray(a, np.float32)
    hi = np.asarray(jnp.asarray(a).astype(BF16).astype(F32))
    return hi, a - hi


def constants():
    n = NODES + 2
    col = np.arange(n, dtype=np.float64) + 1.0
    s = np.sqrt(2.0 / (n + 1.0)) * np.sin(np.pi * col[:, None] * col[None, :] / (n + 1.0))
    lam = 2.0 - 2.0 * np.cos(np.pi * col / (n + 1.0))
    fwd = np.zeros((104, 112))
    for q in range(n):
        for r in range(n):
            c = q * 8 + r - 1
            if r == 0:
                c = 80 + q
            if r == n - 1:
                c = 96 + q
            fwd[:100, c] = np.outer(s[:, q], s[:, r]).reshape(-1)
    fh, fl = split_np(fwd)
    a1 = np.concatenate([np.concatenate([fh, fh], 1), np.concatenate([fl, fl], 1)], 0)
    bh, bl = split_np(RELAX * fwd.T)
    a2 = np.concatenate([np.concatenate([bh, bh], 1), np.concatenate([bl, bl], 1)], 0)
    lam_j = np.ones((104, LANES), np.float32)
    lam_k = np.ones((104, LANES), np.float32)
    lam_j[:100] = np.repeat(lam, n)[:, None]
    lam_k[:100] = np.tile(lam, n)[:, None]
    t = np.arange(NODES) / (NODES - 1.0)
    w = np.stack([1.0 - t, t])
    wm = np.einsum("ax,by,cz->abcxyz", w, w, w).reshape(8, 512)
    wh, wl = split_np(wm)
    wm = np.concatenate([wh, wl], 0)
    rim = wm.reshape(16, 8, 8, 8)[:, :, [0, 1, 6, 7]].reshape(16, 256)
    return s, lam, a1, a2, lam_j, lam_k, wm, rim


SINES, LAM, A_FWD, A_BWD, LAM_J, LAM_K, W_MOM, W_RIM = constants()


def split(x):
    hi = x.astype(BF16)
    return hi, (x - hi.astype(F32)).astype(BF16)


def dot(a, b):
    return lax.dot_general(a, b, (((1,), (0,)), ((), ())), preferred_element_type=F32)


def dot_t(a, b):
    return lax.dot_general(a, b, (((1,), (1,)), ((), ())), preferred_element_type=F32)


def flags():
    i = lax.axis_index("sx")
    j = lax.axis_index("sy")
    nx = lax.axis_size("sx")
    ny = lax.axis_size("sy")
    one = lambda c: jnp.where(c, 1.0, 0.0).astype(F32)
    return one(i > 0), one(i < nx - 1), one(j > 0), one(j < ny - 1)


def even_row():
    return lax.rem(lax.axis_index("sy"), 2) == 0


class Picked:
    def __init__(self, first, second):
        self.refs = (first, second)

    def __getitem__(self, at):
        return jnp.where(even_row(), self.refs[0][at], self.refs[1][at])


def from_y(near, odd):
    return Picked(odd, near), Picked(near, odd)


def put_y(near_ref, odd_ref, at, down, up):
    even = even_row()
    near_ref[at] = jnp.where(even, up, down)
    odd_ref[at] = jnp.where(even, down, up)


def lane_up(x):
    lane = lax.broadcasted_iota(jnp.int32, x.shape, x.ndim - 1)
    return jnp.where(lane == LANES - 1, 0.0, pltpu.roll(x, LANES - 1, x.ndim - 1))


def lane_down(x):
    lane = lax.broadcasted_iota(jnp.int32, x.shape, x.ndim - 1)
    return jnp.where(lane == 0, 0.0, pltpu.roll(x, 1, x.ndim - 1))


def onehot(slot_row):
    p = lax.broadcasted_iota(jnp.int32, (256, 256), 0)
    return jnp.where(p == slot_row, 1.0, 0.0).astype(BF16)


def split3(a):
    a1 = a.astype(BF16)
    e = a - a1.astype(F32)
    a2 = e.astype(BF16)
    return a1, a2, (e - a2.astype(F32)).astype(BF16)


def start_kernel(
    rhs_hbm, stretch_hbm, mass_hbm, slot_hbm, group_hbm,
    coef_ref, near_ref, odd_ref, slot_ref,
    face_ref, stretch_ref, mass_ref, group_ref, sems,
):
    pairs = (
        (slot_hbm, slot_ref),
        (rhs_hbm.at[:, pl.ds(0, 8), :], face_ref.at[0]),
        (rhs_hbm.at[:, pl.ds(56, 8), :], face_ref.at[1]),
        (stretch_hbm, stretch_ref),
        (mass_hbm, mass_ref),
        (group_hbm, group_ref),
    )
    copies = [pltpu.make_async_copy(h, v, sems.at[k]) for k, (h, v) in enumerate(pairs)]
    for c in copies:
        c.start()
    copies[0].wait()
    oh = onehot(slot_ref[...])
    faces = []
    for k, b in ((1, 0), (2, 1)):
        copies[k].wait()
        g = dot_t(jnp.concatenate(split3(face_ref[k - 1].reshape(64, 256)), 0), oh)
        g = g[0:64] + g[64:128] + g[128:192]
        faces.append(g[:, b * LANES : (b + 1) * LANES].reshape(8, 8, LANES))
    put_y(near_ref, odd_ref, slice(0, 8), *faces)
    for c in copies[3:]:
        c.wait()
    c = jnp.concatenate(
        [
            stretch_ref[...],
            mass_ref[...],
            group_ref[...].astype(F32),
            jnp.zeros((3, 256), F32),
        ],
        0,
    )
    c1, c2, c3 = split3(c)
    cg = dot_t(c1, oh) + dot_t(c2, oh) + dot_t(c3, oh)
    coef = jnp.concatenate([cg[0:4, :LANES], cg[0:4, LANES:]], 0)
    gr = jnp.concatenate([cg[4:5, :LANES], cg[4:5, LANES:], jnp.zeros((6, LANES), F32)], 0)
    coef_ref[0] = coef
    coef_ref[1] = gr
    pad = jnp.zeros((3, LANES), F32)
    down = jnp.concatenate([coef[0:4], gr[0:1], pad], 0)
    up = jnp.concatenate([coef[4:8], gr[1:2], pad], 0)
    put_y(near_ref, odd_ref, 8, down, up)


def place_kernel(lam_hbm, rhs_ref, slot_ref, coef_ref, src_ref, dinv_ref, lam_ref, sems):
    lam = pltpu.make_async_copy(lam_hbm, lam_ref, sems.at[0])
    lam.start()
    oh = onehot(slot_ref[...])
    for x in range(8):
        g = dot_t(jnp.concatenate(split3(rhs_ref[x]), 0), oh)
        g = g[0:64] + g[64:128] + g[128:192]
        for b in range(2):
            src_ref[x, b * 8 : b * 8 + 8] = g[:, b * LANES : (b + 1) * LANES].reshape(8, 8, LANES)
    lam.wait()
    for b in range(2):
        lanes = slice(b * LANES, (b + 1) * LANES)
        cx, cy, cz, m, _ = rows_of(coef_ref[0], b * 4)
        cxl = [cx * float(v) for v in LAM]
        for t in range(13):
            row = slice(t * 8, t * 8 + 8)
            d0 = cy * lam_ref[0, row, :] + cz * lam_ref[1, row, :] + m
            for i in range(10):
                dinv_ref[i, row, lanes] = 1.0 / (d0 + cxl[i])


def rim_kernel(src_ref, coef_ref, yd_ref, yu_ref, to_a_ref, to_b_ref):
    yd_ref, yu_ref = from_y(yd_ref, yu_ref)
    coef_y = jnp.concatenate([yd_ref[8, 0:4, :], yu_ref[8, 0:4, :]], 0)
    even = even_row()
    coef = coef_ref[0]
    for out, x_even, x_odd in ((to_a_ref, 7, 0), (to_b_ref, 0, 7)):
        pick = lambda ref: jnp.where(even, ref[x_even], ref[x_odd])
        out[0] = pick(yd_ref)
        out[1:17] = pick(src_ref)
        out[17] = pick(yu_ref)
        out[18] = coef
        out[19] = coef_y


def forward(res, base, a1_ref):
    ends = []
    for z, shift in ((7, lane_down), (0, lane_up)):
        ends.append([shift(res[pl.ds(base + 64 * t + z, 8, stride=8), :]) for t in range(3)])
    halves = [
        jnp.concatenate(
            [res[base + 64 * b : base + 64 * b + 80, :]] + ends[0][b : b + 2] + ends[1][b : b + 2],
            0,
        )
        for b in range(2)
    ]
    hi, lo = split(jnp.concatenate(halves, 1))
    r = dot(a1_ref[...], jnp.concatenate([hi, lo], 0))
    return r[:104] + r[104:]


def along_x(layers, partial, row, lanes):
    acc = [None if partial is None else partial[i, row, lanes] for i in range(10)]
    for p, (low, high) in layers.items():
        v = low[0][low[1], row, lanes]
        w = high[0][high[1], row, lanes]
        h = (v + w, v - w)
        for i in range(10):
            term = h[i % 2] * float(SINES[i, p])
            acc[i] = term if acc[i] is None else acc[i] + term
    return acc


def partial_x(layers, out_ref):
    for b in range(2):
        lanes = slice(b * LANES, (b + 1) * LANES)

        def chunk(t, carry):
            row = pl.ds(pl.multiple_of(t * 8, 8), 8)
            for i, v in enumerate(along_x(layers, None, row, lanes)):
                out_ref[i, row, lanes] = v
            return carry

        lax.fori_loop(0, 13, chunk, 0)


def finish_solves(layers, partial, dinv_ref, a2_ref, spec, wout):
    for b in range(2):
        lanes = slice(b * LANES, (b + 1) * LANES)

        def chunk(t, carry):
            row = pl.ds(pl.multiple_of(t * 8, 8), 8)
            z = along_x(layers, partial, row, lanes)
            z = [z[i] * dinv_ref[i, row, lanes] for i in range(10)]
            for p in range(5):
                e = z[0] * float(SINES[0, p])
                o = z[1] * float(SINES[1, p])
                for i in range(2, 10, 2):
                    e = e + z[i] * float(SINES[i, p])
                    o = o + z[i + 1] * float(SINES[i + 1, p])
                spec[p, row, lanes] = e + o
                spec[9 - p, row, lanes] = e - o
            return carry

        lax.fori_loop(0, 13, chunk, 0)

    for p in range(10):
        base = p * 192
        hi, lo = split(spec[p])
        r = dot(a2_ref[...], jnp.concatenate([hi, lo], 0))
        r = r[:112] + r[112:]
        r0 = r[:, :LANES]
        r1 = r[:, LANES:]
        wout[base : base + 64, :] = r0[0:64]
        wout[base + 64 : base + 80, :] = r0[64:80] + r1[0:16]
        wout[base + 80 : base + 144, :] = r1[16:80]
        wout[base + 144 : base + 192, :] = jnp.zeros((48, LANES), F32)
        for off, z, shift in ((80, 7, lane_up), (96, 0, lane_down)):
            rows = [
                r0[off : off + 8],
                r0[off + 8 : off + 16] + r1[off : off + 8],
                r1[off + 8 : off + 16],
            ]
            for t in range(3):
                at = pl.ds(base + 64 * t + z, 8, stride=8)
                wout[at, :] = wout[at, :] + shift(rows[t])


def put(ref, p, y, value):
    n = value.shape[0]
    at = (p * 24 + y) * 8
    ref[at : at + n * 8, :] = value.reshape(n * 8, LANES)


def get(ref, p, y, n):
    at = (p * 24 + y) * 8
    return ref[at : at + n * 8, :].reshape(n, 8, LANES)


def with_rows(line, n, d, u, down, up):
    rows_d = d * down
    rows_u = u * up
    low = rows_d[n - 2 : n] + jnp.concatenate([line[0:1] * down, line[1:2]], 0)
    high = rows_u[0:2] + jnp.concatenate([line[16:17], line[17:18] * up], 0)
    parts = [low, line[2:16], high]
    if n > 2:
        parts = [rows_d[0 : n - 2]] + parts + [rows_u[2:n]]
    return jnp.concatenate(parts, 0)


def put_layer(ref, at, below, line, above):
    put(ref, at, 0, below)
    put(ref, at, 1, line)
    put(ref, at, 17, above)
    put(ref, at, 18, jnp.zeros((6, 8, LANES), F32))


def first_inner_kernel(src_ref, yd_ref, yu_ref, a1_ref, rin_ref, sin_ref, sout):
    yd_ref, yu_ref = from_y(yd_ref, yu_ref)
    _, _, down, up = flags()
    for x in range(8):
        put_layer(rin_ref, x, yd_ref[x : x + 1] * down, src_ref[x], yu_ref[x : x + 1] * up)
        sout[x] = forward(rin_ref, x * 192, a1_ref)
    partial_x({p: ((sout, p - 1), (sout, 8 - p)) for p in range(1, 5)}, sin_ref)


def first_kernel(
    xa_ref, xb_ref, sin_ref, dinv_ref, a1_ref, a2_ref,
    rout_ref, wout, near_ref, odd_ref, sout, spec,
):
    left, right, down, up = flags()
    x_refs = Picked(xa_ref, xb_ref), Picked(xb_ref, xa_ref)
    for k, (x_ref, side) in enumerate(zip(x_refs, (left, right))):
        put_layer(
            rout_ref,
            k,
            x_ref[0:1] * (side * down),
            x_ref[1:17] * side,
            x_ref[17:18] * (side * up),
        )
        sout[k] = forward(rout_ref, k * 192, a1_ref)
    finish_solves({0: ((sout, 0), (sout, 1))}, sin_ref, dinv_ref, a2_ref, spec, wout)
    for p in range(10):
        put_y(near_ref, odd_ref, p, get(wout, p, 0, 3), get(wout, p, 15, 3))


def edge_kernel(w_ref, d_ref, u_ref, a_ref, b_ref):
    d_ref, u_ref = from_y(d_ref, u_ref)
    _, _, down, up = flags()
    even = even_row()
    for k in range(3):
        to_l, to_r = [
            with_rows(get(w_ref, p, 0, 18), 3, d_ref[p], u_ref[p], down, up) for p in (k, 7 + k)
        ]
        a_ref[k] = jnp.where(even, to_r, to_l)
        b_ref[k] = jnp.where(even, to_l, to_r)


def neighbours_z(u):
    z = lax.broadcasted_iota(jnp.int32, u.shape, 1)
    s = pltpu.roll(u, 7, 1)
    above = jnp.where(z == 7, lane_up(s), s)
    s = pltpu.roll(u, 1, 1)
    below = jnp.where(z == 0, lane_down(s), s)
    return above, below


ROWS = ((0, 1, 0), (1, 4, 1), (5, 4, 1), (9, 4, 2), (13, 4, 2), (17, 1, 3))


def second_residual(get_h, get_r, cb, p, at, res_ref, left, right, down, up):
    for y, n, b in ROWS:
        v = get_h(p + 1, y + 1, n)
        res = get_r(y, n) - stencil(
            cb[b],
            v,
            get_h(p + 2, y + 1, n) + get_h(p, y + 1, n),
            get_h(p + 1, y + 2, n) + get_h(p + 1, y, n),
        )
        if p == 0:
            res = res * left
        if p == 9:
            res = res * right
        if y == 0:
            res = res * down
        if y == 17:
            res = res * up
        put(res_ref, at, y, res)
    put(res_ref, at, 18, jnp.zeros((6, 8, LANES), F32))


def spread_coefs(cb, rows):
    for b, (tile, at) in enumerate(rows):
        for k, v in enumerate(rows_of(tile, at)):
            cb[b, k] = v
    return [[cb.at[b, k] for k in range(5)] for b in range(4)]


class Loaded:
    def __init__(self, refs):
        self.refs = refs

    def __getitem__(self, k):
        return self.refs[k][...]


def second_inner_kernel(
    rin_ref, coef_ref, yd_ref, yu_ref, w_ref, d_ref, u_ref, a1_ref, h_ref, sin_ref, cb, r1, sout,
):
    yd_ref, yu_ref = from_y(yd_ref, yu_ref)
    d_ref, u_ref = from_y(d_ref, u_ref)
    left, right, down, up = flags()
    for x in range(3, 9):
        h_ref[x - 3] = with_rows(get(w_ref, x - 1, 0, 18), 3, d_ref[x - 1], u_ref[x - 1], down, up)
    tiles = spread_coefs(
        cb, ((yd_ref[8], 0), (coef_ref[0], 0), (coef_ref[0], 4), (yu_ref[8], 0))
    )
    coefs = [Loaded(t) for t in tiles]
    get_h = lambda x, y, n: h_ref[x - 3, y : y + n]
    for k in range(4):
        p = 3 + k
        get_r = lambda y, n: get(rin_ref, p - 1, y, n)
        second_residual(get_h, get_r, coefs, p, k, r1, left, right, down, up)
        sout[k] = forward(r1, k * 192, a1_ref)
    partial_x({p: ((sout, p - 3), (sout, 6 - p)) for p in (3, 4)}, sin_ref)


def second_kernel(
    rin_ref, rout_ref, coef_ref, xa_ref, xb_ref, yd_ref, yu_ref, w_ref, a_ref, b_ref, d_ref, u_ref,
    hin_ref, sin_ref, dinv_ref, a1_ref, a2_ref,
    c_ref, to_a_ref, to_b_ref, own_down_ref, own_up_ref, h, cb, r1, sout, spec, wout,
):
    yd_ref, yu_ref = from_y(yd_ref, yu_ref)
    d_ref, u_ref = from_y(d_ref, u_ref)
    left, right, down, up = flags()
    l_ref, r_ref = Picked(a_ref, b_ref), Picked(b_ref, a_ref)
    for x in (0, 1, 2, 9, 10, 11):
        if x == 0:
            g = l_ref[0] * left
        elif x == 11:
            g = r_ref[2] * right
        else:
            g = with_rows(get(w_ref, x - 1, 0, 18), 3, d_ref[x - 1], u_ref[x - 1], down, up)
            if x == 1:
                g = (g + l_ref[1]) * left
            elif x == 2:
                g = g + l_ref[2] * left
            elif x == 9:
                g = g + r_ref[0] * right
            elif x == 10:
                g = (g + r_ref[1]) * right
        h[x if x < 3 else x - 6] = g

    def get_h(x, y, n):
        if 3 <= x <= 8:
            return hin_ref[x - 3, y : y + n]
        return h[x if x < 3 else x - 6, y : y + n]

    coefs = []
    for a, x_ref in ((0, Picked(xa_ref, xb_ref)), (1, None), (2, Picked(xb_ref, xa_ref))):
        if x_ref is None:
            rows = ((yd_ref[8], 0), (coef_ref[0], 0), (coef_ref[0], 4), (yu_ref[8], 0))
        else:
            own, beside = x_ref[18], x_ref[19]
            rows = ((beside, 0), (own, 0), (own, 4), (beside, 4))
        coefs.append([Loaded(t) for t in spread_coefs(cb.at[a], rows)])
    for k, p in enumerate((0, 1, 2, 7, 8, 9)):
        if p in (0, 9):
            get_r = lambda y, n: get(rout_ref, 0 if p == 0 else 1, y, n)
        else:
            get_r = lambda y, n: get(rin_ref, p - 1, y, n)
        cb_p = coefs[0 if p == 0 else 2 if p == 9 else 1]
        second_residual(get_h, get_r, cb_p, p, k, r1, left, right, down, up)
        sout[k] = forward(r1, k * 192, a1_ref)
    layers = {p: ((sout, p), (sout, 5 - p)) for p in range(3)}
    finish_solves(layers, sin_ref, dinv_ref, a2_ref, spec, wout)
    for p in range(10):
        line = get(wout, p, 0, 18)
        c_ref[p] = get_h(p + 1, 1, 18) + line
        own_down_ref[p] = line[0:2]
        own_up_ref[p] = line[16:18]
    even = even_row()
    for k in range(2):
        to_l, to_r = get(wout, k, 0, 18), get(wout, 8 + k, 0, 18)
        to_a_ref[k] = jnp.where(even, to_r, to_l)
        to_b_ref[k] = jnp.where(even, to_l, to_r)


def add_x(g, p, l, r, left, right, y=slice(0, 18)):
    if p == 0:
        return (g + l[0, y]) * left
    if p == 1:
        return g + l[1, y] * left
    if p == 8:
        return g + r[0, y] * right
    if p == 9:
        return (g + r[1, y]) * right
    return g


def rows_of(tile, at):
    c = [jnp.broadcast_to(tile[at + k : at + k + 1, :], (8, LANES)) for k in range(4)]
    return c + [2.0 * (c[0] + c[1] + c[2]) + c[3]]


def stencil(cf, v, x_sum, y_sum):
    above, below = neighbours_z(v)
    return cf[4] * v - cf[0] * x_sum - cf[1] * y_sum - cf[2] * (above + below)


def column_residual(get_h, src_ref, cf, x, b, mr_ref, at):
    lanes = slice(b * LANES, (b + 1) * LANES)
    for y in (0, 4):
        yy = b * 8 + y + 1
        p = x + 1
        v = get_h(p, yy, 4)
        res = src_ref[x, yy - 1 : yy + 3] - stencil(
            cf,
            v,
            get_h(p + 1, yy, 4) + get_h(p - 1, yy, 4),
            get_h(p, yy + 1, 4) + get_h(p, yy - 1, 4),
        )
        mr_ref[at, y * 8 : y * 8 + 32, lanes] = res.reshape(32, LANES)


def moments(wm_ref, x, rows):
    rh, rl = split(rows)
    w = wm_ref[:, x * 64 : x * 64 + rows.shape[0]]
    return dot(w, rh) + dot(w, rl)


def to_slots(uv, oh):
    hi, lo = split(uv)
    n = uv.shape[0]
    o = dot(jnp.concatenate([hi, lo], 0), oh)
    return o[:n] + o[n:]


def middle_inner_kernel(
    src_ref, coef_ref, yd_ref, yu_ref, c_ref, slot_ref, wm_ref,
    smooth_hbm, res_hbm, mr_ref, mom_ref, pick_ref, member_ref, h, smooth_ref, res_ref, sems,
):
    yd_ref, yu_ref = from_y(yd_ref, yu_ref)
    _, _, down, up = flags()
    oh = onehot(slot_ref[...])
    copies = []
    for x in range(1, 7):
        both = [c_ref[x + 1, 8 * b + 2 : 8 * b + 8].reshape(48, LANES) for b in range(2)]
        smooth_ref[x - 1] = to_slots(jnp.concatenate(both, 1), oh)
    copies.append(
        pltpu.make_async_copy(smooth_ref, smooth_hbm.at[pl.ds(1, 6), pl.ds(8, 48), :], sems.at[0])
    )
    copies[0].start()
    for k in range(6):
        h[k] = c_ref[k + 2]
        h[k, 0] = c_ref[k + 2, 0] * down
        h[k, 17] = c_ref[k + 2, 17] * up
    get_h = lambda p, y, n: h[p - 2, y : y + n]
    coefs = [rows_of(coef_ref[0], 0), rows_of(coef_ref[0], 4)]
    for k in range(4):
        for b in range(2):
            column_residual(get_h, src_ref, coefs[b], 2 + k, b, mr_ref, k)
        res_ref[k] = to_slots(mr_ref[k, 16:48, :], oh)
    copies.append(
        pltpu.make_async_copy(res_ref, res_hbm.at[pl.ds(2, 4), pl.ds(16, 32), :], sems.at[1])
    )
    copies[1].start()
    mom = jnp.zeros((16, 256), F32)
    for k in (0, 2):
        mom = mom + moments(wm_ref, 2 + k, mr_ref[k : k + 2].reshape(128, 256))
    mom_ref[...] = mom
    gr = coef_ref[1]
    group = jnp.concatenate([gr[0:1], gr[1:2], yd_ref[8, 4:5, :], yu_ref[8, 4:5, :]], 1)
    ny = pick_ref.shape[0]
    col = (group + 0.5).astype(jnp.int32) - lax.axis_index("sx") * (ny * GRP_DEV)
    owner = lax.shift_right_logical(col, 4)
    member = jnp.bitwise_and(col, 15)
    sel = lax.broadcasted_iota(jnp.int32, (ny, 512), 0)
    pick_ref[...] = jnp.where(sel == owner, 1.0, 0.0)
    sel = lax.broadcasted_iota(jnp.int32, (16, 512), 0)
    member_ref[...] = jnp.where(sel == member, 1.0, 0.0)
    for c in copies:
        c.wait()


def middle_kernel(
    src_ref, coef_ref, yd_ref, yu_ref, c_ref, a_ref, b_ref, own_down_ref, own_up_ref,
    mom_ref, pick_ref, member_ref, wm_ref, wr_ref,
    u_ref, mr_ref, near_ref, odd_ref, part_ref, h, rim, edge, slabs,
):
    yd_ref, yu_ref = from_y(yd_ref, yu_ref)
    left, right, down, up = flags()
    l_ref, r_ref = Picked(a_ref, b_ref), Picked(b_ref, a_ref)
    for p in range(10):
        e = add_x(own_down_ref[p], p, l_ref, r_ref, left, right, slice(0, 2))
        edge[0, p] = jnp.concatenate([e[0:1] * down, e[1:2]], 0)
        e = add_x(own_up_ref[p], p, l_ref, r_ref, left, right, slice(16, 18))
        edge[1, p] = jnp.concatenate([e[0:1], e[1:2] * up], 0)
        if 3 < p < 6:
            continue
        g = add_x(c_ref[p], p, l_ref, r_ref, left, right)
        h[p] = g
        h[p, 0] = g[0] * down
        h[p, 17] = g[17] * up
    u_ref[0] = h[1, 1:17]
    u_ref[1] = h[8, 1:17]
    get_h = lambda p, y, n: h[p, y : y + n]
    coefs = [rows_of(coef_ref[0], 0), rows_of(coef_ref[0], 4)]
    for k, x in enumerate((0, 1, 6, 7)):
        for b in range(2):
            column_residual(get_h, src_ref, coefs[b], x, b, mr_ref, k)
    rim[...] = jnp.zeros((256, 256), F32)
    for k, out, far, near, tile, lanes, y_far, y_near in (
        (0, slabs.at[0], 0, 1, yd_ref, slice(0, LANES), 2, 3),
        (1, slabs.at[1], 1, 0, yu_ref, slice(LANES, 256), 1, 0),
    ):
        slab = edge.at[k]
        cf = rows_of(tile[8], 0)
        for x in range(8):
            p = x + 1
            v = slab[p, far : far + 1]
            res = stencil(
                cf,
                v,
                slab[p + 1, far : far + 1] + slab[p - 1, far : far + 1],
                slab[p, near : near + 1],
            )
            out[0, x] = v[0]
            out[1, x] = -res[0]
            at = (x * 4 + y_near) * 8
            rim[at : at + 8, lanes] = -res[0]
            at = (x * 4 + y_far) * 8
            rim[at : at + 8, lanes] = cf[1] * v[0]
    for k in range(2):
        put_y(near_ref, odd_ref, k, slabs[0, k], slabs[1, k])
    mom = mom_ref[...]
    mom = mom + moments(wm_ref, 0, mr_ref[0:2].reshape(128, 256))
    mom = mom + moments(wm_ref, 6, mr_ref[2:4].reshape(128, 256))
    rh, rl = split(rim[...])
    mom_y = dot(wr_ref[...], rh) + dot(wr_ref[...], rl)
    mom_y = mom_y[0:8] + mom_y[8:16]
    mom = jnp.concatenate(
        [mom[0:8] + mom[8:16], mom_y[:, :LANES] * down, mom_y[:, LANES:] * up], 1
    )
    member = member_ref[...]
    spread = jnp.concatenate([member * mom[v : v + 1] for v in range(8)], 0)
    sh, sl = split(spread)
    pick = pick_ref[...].astype(BF16)
    part_ref[...] = dot_t(pick, sh) + dot_t(pick, sl)


def last_kernel(
    smooth_in, res_in, c_ref, uout_ref, rin_ref, rout_ref, coef_ref, d_ref, u_ref, slot_ref,
    arrived_ref,
    smooth_hbm, res_hbm, coarse_hbm, smooth_ref, res_ref, coarse_ref, sems,
):
    d_ref, u_ref = from_y(d_ref, u_ref)
    _, _, down, up = flags()
    total = jnp.sum(arrived_ref[...], axis=0, keepdims=True)
    for v in range(8):
        coarse_ref[v : v + 1, :] = total[:, v * GRP_DEV : (v + 1) * GRP_DEV]
    copies = [pltpu.make_async_copy(coarse_ref, coarse_hbm, sems.at[8])]
    copies[0].start()

    def send(ref, hbm, x, nx, row, rows):
        at = (pl.ds(x, nx), pl.ds(row, rows), slice(None))
        k = len(copies) - 1
        copies.append(pltpu.make_async_copy(ref.at[at], hbm.at[at], sems.at[k]))
        copies[-1].start()

    oh = onehot(slot_ref[...])
    sides = (
        (d_ref, down, jnp.broadcast_to(coef_ref[0, 1:2, :], (8, LANES))),
        (u_ref, up, jnp.broadcast_to(coef_ref[0, 5:6, :], (8, LANES))),
    )

    def added(x):
        out = []
        for slab, on, cy in sides:
            v = slab[0, x] * on
            out.append((v, slab[1, x] * on, cy * v))
        return out

    zero = jnp.zeros((8, LANES), F32)
    pairs = [added(x) for x in range(8)]
    for k, x in enumerate((0, 1, 6, 7)):
        (_, d0, d1), (_, e0, e1) = pairs[x]
        add = jnp.concatenate(
            [
                jnp.concatenate([d0, d1] + [zero] * 6, 0),
                jnp.concatenate([zero] * 6 + [e1, e0], 0),
            ],
            1,
        )
        res_ref[x] = to_slots(rout_ref[k] + add, oh)
        if k == 1:
            send(res_ref, res_hbm, 0, 2, 0, 64)
    send(res_ref, res_hbm, 6, 2, 0, 64)
    low, high = [], []
    for k in range(4):
        (_, d0, d1), (_, e0, e1) = pairs[2 + k]
        z2 = jnp.zeros((16, LANES), F32)
        low.append(
            rin_ref[k, 0:16, :] + jnp.concatenate([jnp.concatenate([d0, d1], 0), z2], 1)
        )
        high.append(
            rin_ref[k, 48:64, :] + jnp.concatenate([z2, jnp.concatenate([e1, e0], 0)], 1)
        )
    res_ref[2:6, 0:16, :] = to_slots(jnp.concatenate(low, 0), oh).reshape(4, 16, 256)
    send(res_ref, res_hbm, 2, 4, 0, 16)
    res_ref[2:6, 48:64, :] = to_slots(jnp.concatenate(high, 0), oh).reshape(4, 16, 256)
    send(res_ref, res_hbm, 2, 4, 48, 16)
    for k, x in enumerate((0, 7)):
        (d0, _, _), (e0, _, _) = pairs[x]
        both = [uout_ref[k, 0:8].reshape(64, LANES), uout_ref[k, 8:16].reshape(64, LANES)]
        both[0] = both[0] + jnp.concatenate([d0] + [zero] * 7, 0)
        both[1] = both[1] + jnp.concatenate([zero] * 7 + [e0], 0)
        smooth_ref[x] = to_slots(jnp.concatenate(both, 1), oh)
        send(smooth_ref, smooth_hbm, x, 1, 0, 64)
    low, high = [], []
    for x in range(1, 7):
        (d0, _, _), (e0, _, _) = pairs[x]
        c = [c_ref[x + 1, y] for y in (1, 9, 8, 16)]
        low.append(jnp.concatenate([c[0] + d0, c[1]], 1))
        high.append(jnp.concatenate([c[2], c[3] + e0], 1))
    smooth_ref[1:7, 0:8, :] = to_slots(jnp.concatenate(low, 0), oh).reshape(6, 8, 256)
    send(smooth_ref, smooth_hbm, 1, 6, 0, 8)
    smooth_ref[1:7, 56:64, :] = to_slots(jnp.concatenate(high, 0), oh).reshape(6, 8, 256)
    send(smooth_ref, smooth_hbm, 1, 6, 56, 8)
    for c in copies:
        c.wait()


def sd(*shape):
    return jax.ShapeDtypeStruct(shape, F32)


def vm(*shape):
    return pltpu.VMEM(shape, F32)


def swap_y(value, odd):
    nx = lax.axis_size("sx")
    ny = lax.axis_size("sy")
    pairs = []
    for i in range(nx):
        for j in range(ny):
            to = j + 1 if j % 2 == odd else j - 1
            target = i * ny + to if 0 <= to < ny else (i ^ 1) * ny + j
            pairs.append((i * ny + j, target))
    return lax.ppermute(value, ("sx", "sy"), pairs)


def snake(value, by):
    nx = lax.axis_size("sx")
    ny = lax.axis_size("sy")
    pairs = []
    for i in range(nx):
        for j in range(ny):
            to = i + (by if j % 2 == 0 else -by)
            target = to * ny + j if 0 <= to < nx else i * ny + (j ^ 1)
            pairs.append((i * ny + j, target))
    return lax.ppermute(value, ("sx", "sy"), pairs)


def call(kernel, outs, args, scratch=(), hbm_in=0, hbm_out=0, sems=0, alias=0):
    vmem = pl.BlockSpec(memory_space=pltpu.VMEM)
    hbm = pl.BlockSpec(memory_space=pltpu.HBM)
    args = [
        pltpu.with_memory_space_constraint(a, pltpu.HBM if k < hbm_in else pltpu.VMEM)
        for k, a in enumerate(args)
    ]
    scratch = [pltpu.VMEM(s, F32) if isinstance(s, tuple) else s for s in scratch]
    if sems:
        scratch.append(pltpu.SemaphoreType.DMA((sems,)))
    return pl.pallas_call(
        kernel,
        out_shape=outs,
        in_specs=[hbm if k < hbm_in else vmem for k in range(len(args))],
        out_specs=[hbm if k < hbm_out else vmem for k in range(len(outs))],
        scratch_shapes=scratch,
        input_output_aliases={k: k for k in range(alias)},
        compiler_params=pltpu.CompilerParams(vmem_limit_bytes=16 << 20),
    )(*args)


def on_device(right_side, stretch, mass_term, slot_position, coarse_group):
    a1 = jnp.asarray(A_FWD, BF16)
    a2 = jnp.asarray(A_BWD, BF16)
    lam = jnp.asarray(np.stack([LAM_J, LAM_K]), F32)
    wm = jnp.asarray(W_MOM, BF16)
    wr = jnp.asarray(W_RIM, BF16)
    row = pltpu.VMEM((1, 256), jnp.int32)
    rhs = right_side.reshape(8, 64, 256)
    coef, near, odd, slot = call(
        start_kernel,
        [vm(2, 8, LANES), vm(9, 8, LANES), vm(9, 8, LANES), row],
        (
            rhs,
            stretch,
            mass_term.reshape(1, 256),
            slot_position.reshape(1, 256),
            coarse_group.reshape(1, 256),
        ),
        [(2, 8, 8, 256), (3, 256), (1, 256), row],
        hbm_in=5,
        sems=6,
    )
    yn = swap_y(near, 0)
    yo = swap_y(odd, 1)
    src, dinv = call(
        place_kernel,
        [vm(8, 16, 8, LANES), vm(10, 104, 256)],
        (lam, rhs, slot, coef),
        [(2, 104, LANES)],
        hbm_in=1,
        sems=1,
    )
    to_a, to_b = call(rim_kernel, [vm(20, 8, LANES)] * 2, (src, coef, yn, yo))
    xa = snake(to_a, 1)
    xb = snake(to_b, -1)
    rin, sin = call(
        first_inner_kernel,
        [vm(8 * 192, LANES), vm(10, 104, 256)],
        (src, yn, yo, a1),
        [(8, 104, 256)],
    )

    side = vm(10, 3, 8, LANES)
    rout, w, near, odd = call(
        first_kernel,
        [vm(2 * 192, LANES), vm(1920, LANES), side, side],
        (xa, xb, sin, dinv, a1, a2),
        [(2, 104, 256), (10, 104, 256)],
    )
    n = swap_y(near, 0)
    o = swap_y(odd, 1)
    to_a, to_b = call(edge_kernel, [vm(3, 20, 8, LANES)] * 2, (w, n, o))
    a = snake(to_a, 1)
    b = snake(to_b, -1)
    hin, sin = call(
        second_inner_kernel,
        [vm(6, 20, 8, LANES), vm(10, 104, 256)],
        (rin, coef, yn, yo, w, n, o, a1),
        [(4, 5, 8, LANES), (4 * 192, LANES), (4, 104, 256)],
    )

    slab = vm(2, 18, 8, LANES)
    side = vm(10, 2, 8, LANES)
    c, to_a, to_b, own_d, own_u = call(
        second_kernel,
        [vm(10, 18, 8, LANES), slab, slab, side, side],
        (rin, rout, coef, xa, xb, yn, yo, w, a, b, n, o, hin, sin, dinv, a1, a2),
        [
            (6, 20, 8, LANES),
            (3, 4, 5, 8, LANES),
            (6 * 192, LANES),
            (6, 104, 256),
            (10, 104, 256),
            (1920, LANES),
        ],
    )
    a = snake(to_a, 1)
    b = snake(to_b, -1)
    edge = vm(2, 8, 8, LANES)
    ny = lax.axis_size("sy")
    smooth, res, rin, mom, pick, member = call(
        middle_inner_kernel,
        [sd(8, 64, 256), sd(8, 64, 256), vm(4, 64, 256), vm(16, 256), vm(ny, 512), vm(16, 512)],
        (src, coef, yn, yo, c, slot, wm),
        [(6, 18, 8, LANES), (6, 48, 256), (4, 32, 256)],
        hbm_out=2,
        sems=2,
    )
    uout, rout, near, odd, part = call(
        middle_kernel,
        [vm(2, 16, 8, LANES), vm(4, 64, 256), edge, edge, vm(ny, LANES)],
        (src, coef, yn, yo, c, a, b, own_d, own_u, mom, pick, member, wm, wr),
        [(10, 18, 8, LANES), (256, 256), (2, 10, 2, 8, LANES), (2, 2, 8, 8, LANES)],
    )
    n = swap_y(near, 0)
    o = swap_y(odd, 1)
    arrived = lax.all_to_all(part, "sy", split_axis=0, concat_axis=0, tiled=True)
    smooth, res, coarse = call(
        last_kernel,
        [sd(8, 64, 256), sd(8, 64, 256), sd(8, GRP_DEV)],
        (smooth, res, c, uout, rin, rout, coef, n, o, slot, arrived),
        [(8, 64, 256), (8, 64, 256), (8, GRP_DEV)],
        hbm_in=2,
        hbm_out=3,
        sems=9,
        alias=2,
    )
    return smooth.reshape(8, 8, 8, 256), res.reshape(8, 8, 8, 256), coarse


def solution(mesh):
    split_all = P(None, None, None, ("sx", "sy"))
    flat = P(("sx", "sy"))
    return jax.shard_map(
        on_device,
        mesh=mesh,
        in_specs=(split_all, P(None, ("sx", "sy")), flat, flat, flat),
        out_specs=(split_all, split_all, P(None, ("sx", "sy"))),
        check_vma=False,
    )
```

```python
import jax
import jax.numpy as jnp
import numpy as np
from jax import lax
from jax.experimental import pallas as pl
from jax.experimental.pallas import tpu as pltpu
from jax.sharding import PartitionSpec as P

NODES = 8
GRP_DEV = 16
LANES = 128
RELAX = 0.35
F32 = jnp.float32
BF16 = jnp.bfloat16


def split_np(a):
    a = np.asarray(a, np.float32)
    hi = np.asarray(jnp.asarray(a).astype(BF16).astype(F32))
    return hi, a - hi


def constants():
    n = NODES + 2
    col = np.arange(n, dtype=np.float64) + 1.0
    s = np.sqrt(2.0 / (n + 1.0)) * np.sin(np.pi * col[:, None] * col[None, :] / (n + 1.0))
    lam = 2.0 - 2.0 * np.cos(np.pi * col / (n + 1.0))
    fwd = np.zeros((104, 112))
    for q in range(n):
        for r in range(n):
            c = q * 8 + r - 1
            if r == 0:
                c = 80 + q
            if r == n - 1:
                c = 96 + q
            fwd[:100, c] = np.outer(s[:, q], s[:, r]).reshape(-1)
    fh, fl = split_np(fwd)
    a1 = np.concatenate([np.concatenate([fh, fh], 1), np.concatenate([fl, fl], 1)], 0)
    bh, bl = split_np(RELAX * fwd.T)
    a2 = np.concatenate([np.concatenate([bh, bh], 1), np.concatenate([bl, bl], 1)], 0)
    lam_j = np.ones((104, LANES), np.float32)
    lam_k = np.ones((104, LANES), np.float32)
    lam_j[:100] = np.repeat(lam, n)[:, None]
    lam_k[:100] = np.tile(lam, n)[:, None]
    t = np.arange(NODES) / (NODES - 1.0)
    w = np.stack([1.0 - t, t])
    wm = np.einsum("ax,by,cz->abcxyz", w, w, w).reshape(8, 512)
    wh, wl = split_np(wm)
    wm = np.concatenate([wh, wl], 0)
    rim = wm.reshape(16, 8, 8, 8)[:, :, [0, 1, 6, 7]].reshape(16, 256)
    return s, lam, a1, a2, lam_j, lam_k, wm, rim


SINES, LAM, A_FWD, A_BWD, LAM_J, LAM_K, W_MOM, W_RIM = constants()


def split(x):
    hi = x.astype(BF16)
    return hi, (x - hi.astype(F32)).astype(BF16)


def dot(a, b):
    return lax.dot_general(a, b, (((1,), (0,)), ((), ())), preferred_element_type=F32)


def dot_t(a, b):
    return lax.dot_general(a, b, (((1,), (1,)), ((), ())), preferred_element_type=F32)


def flags():
    i = lax.axis_index("sx")
    j = lax.axis_index("sy")
    nx = lax.axis_size("sx")
    ny = lax.axis_size("sy")
    one = lambda c: jnp.where(c, 1.0, 0.0).astype(F32)
    return one(i > 0), one(i < nx - 1), one(j > 0), one(j < ny - 1)


def even_row():
    return lax.rem(lax.axis_index("sy"), 2) == 0


class Picked:
    def __init__(self, first, second):
        self.refs = (first, second)

    def __getitem__(self, at):
        return jnp.where(even_row(), self.refs[0][at], self.refs[1][at])


def lane_up(x):
    lane = lax.broadcasted_iota(jnp.int32, x.shape, x.ndim - 1)
    return jnp.where(lane == LANES - 1, 0.0, pltpu.roll(x, LANES - 1, x.ndim - 1))


def lane_down(x):
    lane = lax.broadcasted_iota(jnp.int32, x.shape, x.ndim - 1)
    return jnp.where(lane == 0, 0.0, pltpu.roll(x, 1, x.ndim - 1))


def onehot(slot_row):
    p = lax.broadcasted_iota(jnp.int32, (256, 256), 0)
    return jnp.where(p == slot_row, 1.0, 0.0).astype(BF16)


def split3(a):
    a1 = a.astype(BF16)
    e = a - a1.astype(F32)
    a2 = e.astype(BF16)
    return a1, a2, (e - a2.astype(F32)).astype(BF16)


def start_kernel(
    rhs_hbm, stretch_hbm, mass_hbm, slot_hbm, group_hbm,
    coef_ref, to_down_ref, to_up_ref, slot_ref,
    face_ref, stretch_ref, mass_ref, group_ref, sems,
):
    pairs = (
        (slot_hbm, slot_ref),
        (rhs_hbm.at[:, pl.ds(0, 8), :], face_ref.at[0]),
        (rhs_hbm.at[:, pl.ds(56, 8), :], face_ref.at[1]),
        (stretch_hbm, stretch_ref),
        (mass_hbm, mass_ref),
        (group_hbm, group_ref),
    )
    copies = [pltpu.make_async_copy(h, v, sems.at[k]) for k, (h, v) in enumerate(pairs)]
    for c in copies:
        c.start()
    copies[0].wait()
    oh = onehot(slot_ref[...])
    for k, out, b in ((1, to_down_ref, 0), (2, to_up_ref, 1)):
        copies[k].wait()
        g = dot_t(jnp.concatenate(split3(face_ref[k - 1].reshape(64, 256)), 0), oh)
        g = g[0:64] + g[64:128] + g[128:192]
        out[0:8] = g[:, b * LANES : (b + 1) * LANES].reshape(8, 8, LANES)
    for c in copies[3:]:
        c.wait()
    c = jnp.concatenate(
        [
            stretch_ref[...],
            mass_ref[...],
            group_ref[...].astype(F32),
            jnp.zeros((3, 256), F32),
        ],
        0,
    )
    c1, c2, c3 = split3(c)
    cg = dot_t(c1, oh) + dot_t(c2, oh) + dot_t(c3, oh)
    coef = jnp.concatenate([cg[0:4, :LANES], cg[0:4, LANES:]], 0)
    gr = jnp.concatenate([cg[4:5, :LANES], cg[4:5, LANES:], jnp.zeros((6, LANES), F32)], 0)
    coef_ref[0] = coef
    coef_ref[1] = gr
    pad = jnp.zeros((3, LANES), F32)
    to_down_ref[8] = jnp.concatenate([coef[0:4], gr[0:1], pad], 0)
    to_up_ref[8] = jnp.concatenate([coef[4:8], gr[1:2], pad], 0)


def place_kernel(lam_hbm, rhs_ref, slot_ref, coef_ref, src_ref, dinv_ref, lam_ref, sems):
    lam = pltpu.make_async_copy(lam_hbm, lam_ref, sems.at[0])
    lam.start()
    oh = onehot(slot_ref[...])
    for x in range(8):
        g = dot_t(jnp.concatenate(split3(rhs_ref[x]), 0), oh)
        g = g[0:64] + g[64:128] + g[128:192]
        for b in range(2):
            src_ref[x, b * 8 : b * 8 + 8] = g[:, b * LANES : (b + 1) * LANES].reshape(8, 8, LANES)
    lam.wait()
    for b in range(2):
        lanes = slice(b * LANES, (b + 1) * LANES)
        cx, cy, cz, m, _ = rows_of(coef_ref[0], b * 4)
        cxl = [cx * float(v) for v in LAM]
        for t in range(13):
            row = slice(t * 8, t * 8 + 8)
            d0 = cy * lam_ref[0, row, :] + cz * lam_ref[1, row, :] + m
            for i in range(10):
                dinv_ref[i, row, lanes] = 1.0 / (d0 + cxl[i])


def rim_kernel(src_ref, coef_ref, yd_ref, yu_ref, to_a_ref, to_b_ref):
    coef_y = jnp.concatenate([yd_ref[8, 0:4, :], yu_ref[8, 0:4, :]], 0)
    even = even_row()
    coef = coef_ref[0]
    for out, x_even, x_odd in ((to_a_ref, 7, 0), (to_b_ref, 0, 7)):
        pick = lambda ref: jnp.where(even, ref[x_even], ref[x_odd])
        out[0] = pick(yd_ref)
        out[1:17] = pick(src_ref)
        out[17] = pick(yu_ref)
        out[18] = coef
        out[19] = coef_y


def forward(res, base, a1_ref):
    ends = []
    for z, shift in ((7, lane_down), (0, lane_up)):
        ends.append([shift(res[pl.ds(base + 64 * t + z, 8, stride=8), :]) for t in range(3)])
    halves = [
        jnp.concatenate(
            [res[base + 64 * b : base + 64 * b + 80, :]] + ends[0][b : b + 2] + ends[1][b : b + 2],
            0,
        )
        for b in range(2)
    ]
    hi, lo = split(jnp.concatenate(halves, 1))
    r = dot(a1_ref[...], jnp.concatenate([hi, lo], 0))
    return r[:104] + r[104:]


def along_x(layers, partial, row, lanes):
    acc = [None if partial is None else partial[i, row, lanes] for i in range(10)]
    for p, (low, high) in layers.items():
        v = low[0][low[1], row, lanes]
        w = high[0][high[1], row, lanes]
        h = (v + w, v - w)
        for i in range(10):
            term = h[i % 2] * float(SINES[i, p])
            acc[i] = term if acc[i] is None else acc[i] + term
    return acc


HALVES = (slice(0, LANES), slice(LANES, 256))


def partial_x(layers, out_ref):
    def chunk(t, carry):
        row = pl.ds(pl.multiple_of(t * 8, 8), 8)
        for lanes in HALVES:
            for i, v in enumerate(along_x(layers, None, row, lanes)):
                out_ref[i, row, lanes] = v
        return carry

    lax.fori_loop(0, 13, chunk, 0, unroll=True)


def finish_solves(layers, partial, dinv_ref, a2_ref, spec, wout):
    def chunk(t, carry):
        row = pl.ds(pl.multiple_of(t * 8, 8), 8)
        for lanes in HALVES:
            z = along_x(layers, partial, row, lanes)
            z = [z[i] * dinv_ref[i, row, lanes] for i in range(10)]
            for p in range(5):
                e = z[0] * float(SINES[0, p])
                o = z[1] * float(SINES[1, p])
                for i in range(2, 10, 2):
                    e = e + z[i] * float(SINES[i, p])
                    o = o + z[i + 1] * float(SINES[i + 1, p])
                spec[p, row, lanes] = e + o
                spec[9 - p, row, lanes] = e - o
        return carry

    lax.fori_loop(0, 13, chunk, 0, unroll=True)

    for p in range(10):
        base = p * 192
        hi, lo = split(spec[p])
        r = dot(a2_ref[...], jnp.concatenate([hi, lo], 0))
        r = r[:112] + r[112:]
        r0 = r[:, :LANES]
        r1 = r[:, LANES:]
        wout[base : base + 64, :] = r0[0:64]
        wout[base + 64 : base + 80, :] = r0[64:80] + r1[0:16]
        wout[base + 80 : base + 144, :] = r1[16:80]
        wout[base + 144 : base + 192, :] = jnp.zeros((48, LANES), F32)
        for off, z, shift in ((80, 7, lane_up), (96, 0, lane_down)):
            rows = [
                r0[off : off + 8],
                r0[off + 8 : off + 16] + r1[off : off + 8],
                r1[off + 8 : off + 16],
            ]
            for t in range(3):
                at = pl.ds(base + 64 * t + z, 8, stride=8)
                wout[at, :] = wout[at, :] + shift(rows[t])


def put(ref, p, y, value):
    n = value.shape[0]
    at = (p * 24 + y) * 8
    ref[at : at + n * 8, :] = value.reshape(n * 8, LANES)


def get(ref, p, y, n):
    at = (p * 24 + y) * 8
    return ref[at : at + n * 8, :].reshape(n, 8, LANES)


def with_rows(line, n, d, u, down, up):
    rows_d = d * down
    rows_u = u * up
    low = rows_d[n - 2 : n] + jnp.concatenate([line[0:1] * down, line[1:2]], 0)
    high = rows_u[0:2] + jnp.concatenate([line[16:17], line[17:18] * up], 0)
    parts = [low, line[2:16], high]
    if n > 2:
        parts = [rows_d[0 : n - 2]] + parts + [rows_u[2:n]]
    return jnp.concatenate(parts, 0)


def put_layer(ref, at, below, line, above):
    put(ref, at, 0, below)
    put(ref, at, 1, line)
    put(ref, at, 17, above)
    put(ref, at, 18, jnp.zeros((6, 8, LANES), F32))


def first_inner_kernel(src_ref, yd_ref, yu_ref, a1_ref, rin_ref, sin_ref, sout):
    _, _, down, up = flags()
    for x in range(8):
        put_layer(rin_ref, x, yd_ref[x : x + 1] * down, src_ref[x], yu_ref[x : x + 1] * up)
        sout[x] = forward(rin_ref, x * 192, a1_ref)
    partial_x({p: ((sout, p - 1), (sout, 8 - p)) for p in range(1, 5)}, sin_ref)


def first_kernel(
    xa_ref, xb_ref, sin_ref, dinv_ref, a1_ref, a2_ref,
    rout_ref, wout, to_down_ref, to_up_ref, sout, spec,
):
    left, right, down, up = flags()
    x_refs = Picked(xa_ref, xb_ref), Picked(xb_ref, xa_ref)
    for k, (x_ref, side) in enumerate(zip(x_refs, (left, right))):
        put_layer(
            rout_ref,
            k,
            x_ref[0:1] * (side * down),
            x_ref[1:17] * side,
            x_ref[17:18] * (side * up),
        )
        sout[k] = forward(rout_ref, k * 192, a1_ref)
    finish_solves({0: ((sout, 0), (sout, 1))}, sin_ref, dinv_ref, a2_ref, spec, wout)
    for p in range(10):
        to_down_ref[p] = get(wout, p, 0, 3)
        to_up_ref[p] = get(wout, p, 15, 3)


def edge_kernel(w_ref, d_ref, u_ref, a_ref, b_ref):
    _, _, down, up = flags()
    even = even_row()
    for k in range(3):
        to_l, to_r = [
            with_rows(get(w_ref, p, 0, 18), 3, d_ref[p], u_ref[p], down, up) for p in (k, 7 + k)
        ]
        a_ref[k] = jnp.where(even, to_r, to_l)
        b_ref[k] = jnp.where(even, to_l, to_r)


def neighbours_z(u):
    z = lax.broadcasted_iota(jnp.int32, u.shape, 1)
    s = pltpu.roll(u, 7, 1)
    above = jnp.where(z == 7, lane_up(s), s)
    s = pltpu.roll(u, 1, 1)
    below = jnp.where(z == 0, lane_down(s), s)
    return above, below


ROWS = ((0, 1, 0), (1, 4, 1), (5, 4, 1), (9, 4, 2), (13, 4, 2), (17, 1, 3))


def second_residual(get_h, get_r, cb, p, at, res_ref, left, right, down, up):
    for y, n, b in ROWS:
        v = get_h(p + 1, y + 1, n)
        res = get_r(y, n) - stencil(
            cb[b],
            v,
            get_h(p + 2, y + 1, n) + get_h(p, y + 1, n),
            get_h(p + 1, y + 2, n) + get_h(p + 1, y, n),
        )
        if p == 0:
            res = res * left
        if p == 9:
            res = res * right
        if y == 0:
            res = res * down
        if y == 17:
            res = res * up
        put(res_ref, at, y, res)
    put(res_ref, at, 18, jnp.zeros((6, 8, LANES), F32))


def spread_coefs(cb, rows):
    for b, (tile, at) in enumerate(rows):
        for k, v in enumerate(rows_of(tile, at)):
            cb[b, k] = v
    return [[cb.at[b, k] for k in range(5)] for b in range(4)]


class Loaded:
    def __init__(self, refs):
        self.refs = refs

    def __getitem__(self, k):
        return self.refs[k][...]


def second_inner_kernel(
    rin_ref, coef_ref, yd_ref, yu_ref, w_ref, d_ref, u_ref, a1_ref, h_ref, sin_ref, cb, r1, sout,
):
    left, right, down, up = flags()
    for x in range(3, 9):
        h_ref[x - 3] = with_rows(get(w_ref, x - 1, 0, 18), 3, d_ref[x - 1], u_ref[x - 1], down, up)
    tiles = spread_coefs(
        cb, ((yd_ref[8], 0), (coef_ref[0], 0), (coef_ref[0], 4), (yu_ref[8], 0))
    )
    coefs = [Loaded(t) for t in tiles]
    get_h = lambda x, y, n: h_ref[x - 3, y : y + n]
    for k in range(4):
        p = 3 + k
        get_r = lambda y, n: get(rin_ref, p - 1, y, n)
        second_residual(get_h, get_r, coefs, p, k, r1, left, right, down, up)
        sout[k] = forward(r1, k * 192, a1_ref)
    partial_x({p: ((sout, p - 3), (sout, 6 - p)) for p in (3, 4)}, sin_ref)


def second_kernel(
    rin_ref, rout_ref, coef_ref, xa_ref, xb_ref, yd_ref, yu_ref, w_ref, a_ref, b_ref, d_ref, u_ref,
    hin_ref, sin_ref, dinv_ref, a1_ref, a2_ref,
    c_ref, to_a_ref, to_b_ref, own_down_ref, own_up_ref, h, cb, r1, sout, spec, wout,
):
    left, right, down, up = flags()
    l_ref, r_ref = Picked(a_ref, b_ref), Picked(b_ref, a_ref)
    for x in (0, 1, 2, 9, 10, 11):
        if x == 0:
            g = l_ref[0] * left
        elif x == 11:
            g = r_ref[2] * right
        else:
            g = with_rows(get(w_ref, x - 1, 0, 18), 3, d_ref[x - 1], u_ref[x - 1], down, up)
            if x == 1:
                g = (g + l_ref[1]) * left
            elif x == 2:
                g = g + l_ref[2] * left
            elif x == 9:
                g = g + r_ref[0] * right
            elif x == 10:
                g = (g + r_ref[1]) * right
        h[x if x < 3 else x - 6] = g

    def get_h(x, y, n):
        if 3 <= x <= 8:
            return hin_ref[x - 3, y : y + n]
        return h[x if x < 3 else x - 6, y : y + n]

    coefs = []
    for a, x_ref in ((0, Picked(xa_ref, xb_ref)), (1, None), (2, Picked(xb_ref, xa_ref))):
        if x_ref is None:
            rows = ((yd_ref[8], 0), (coef_ref[0], 0), (coef_ref[0], 4), (yu_ref[8], 0))
        else:
            own, beside = x_ref[18], x_ref[19]
            rows = ((beside, 0), (own, 0), (own, 4), (beside, 4))
        coefs.append([Loaded(t) for t in spread_coefs(cb.at[a], rows)])
    for k, p in enumerate((0, 1, 2, 7, 8, 9)):
        if p in (0, 9):
            get_r = lambda y, n: get(rout_ref, 0 if p == 0 else 1, y, n)
        else:
            get_r = lambda y, n: get(rin_ref, p - 1, y, n)
        cb_p = coefs[0 if p == 0 else 2 if p == 9 else 1]
        second_residual(get_h, get_r, cb_p, p, k, r1, left, right, down, up)
        sout[k] = forward(r1, k * 192, a1_ref)
    layers = {p: ((sout, p), (sout, 5 - p)) for p in range(3)}
    finish_solves(layers, sin_ref, dinv_ref, a2_ref, spec, wout)
    for p in range(10):
        line = get(wout, p, 0, 18)
        c_ref[p] = get_h(p + 1, 1, 18) + line
        own_down_ref[p] = line[0:2]
        own_up_ref[p] = line[16:18]
    even = even_row()
    for k in range(2):
        to_l, to_r = get(wout, k, 0, 18), get(wout, 8 + k, 0, 18)
        to_a_ref[k] = jnp.where(even, to_r, to_l)
        to_b_ref[k] = jnp.where(even, to_l, to_r)


def add_x(g, p, l, r, left, right, y=slice(0, 18)):
    if p == 0:
        return (g + l[0, y]) * left
    if p == 1:
        return g + l[1, y] * left
    if p == 8:
        return g + r[0, y] * right
    if p == 9:
        return (g + r[1, y]) * right
    return g


def rows_of(tile, at):
    c = [jnp.broadcast_to(tile[at + k : at + k + 1, :], (8, LANES)) for k in range(4)]
    return c + [2.0 * (c[0] + c[1] + c[2]) + c[3]]


def stencil(cf, v, x_sum, y_sum):
    above, below = neighbours_z(v)
    return cf[4] * v - cf[0] * x_sum - cf[1] * y_sum - cf[2] * (above + below)


def column_residual(get_h, src_ref, cf, x, b, mr_ref, at):
    lanes = slice(b * LANES, (b + 1) * LANES)
    for y in (0, 4):
        yy = b * 8 + y + 1
        p = x + 1
        v = get_h(p, yy, 4)
        res = src_ref[x, yy - 1 : yy + 3] - stencil(
            cf,
            v,
            get_h(p + 1, yy, 4) + get_h(p - 1, yy, 4),
            get_h(p, yy + 1, 4) + get_h(p, yy - 1, 4),
        )
        mr_ref[at, y * 8 : y * 8 + 32, lanes] = res.reshape(32, LANES)


def moments(wm_ref, x, rows):
    rh, rl = split(rows)
    w = wm_ref[:, x * 64 : x * 64 + rows.shape[0]]
    return dot(w, rh) + dot(w, rl)


def to_slots(uv, oh):
    hi, lo = split(uv)
    n = uv.shape[0]
    o = dot(jnp.concatenate([hi, lo], 0), oh)
    return o[:n] + o[n:]


def middle_inner_kernel(
    src_ref, coef_ref, yd_ref, yu_ref, c_ref, slot_ref, wm_ref,
    smooth_hbm, res_hbm, mr_ref, mom_ref, pick_ref, member_ref, h, smooth_ref, res_ref, sems,
):
    _, _, down, up = flags()
    oh = onehot(slot_ref[...])
    copies = []
    for x in range(1, 7):
        both = [c_ref[x + 1, 8 * b + 2 : 8 * b + 8].reshape(48, LANES) for b in range(2)]
        smooth_ref[x - 1] = to_slots(jnp.concatenate(both, 1), oh)
    copies.append(
        pltpu.make_async_copy(smooth_ref, smooth_hbm.at[pl.ds(1, 6), pl.ds(8, 48), :], sems.at[0])
    )
    copies[0].start()
    for k in range(6):
        h[k] = c_ref[k + 2]
        h[k, 0] = c_ref[k + 2, 0] * down
        h[k, 17] = c_ref[k + 2, 17] * up
    get_h = lambda p, y, n: h[p - 2, y : y + n]
    coefs = [rows_of(coef_ref[0], 0), rows_of(coef_ref[0], 4)]
    for k in range(4):
        for b in range(2):
            column_residual(get_h, src_ref, coefs[b], 2 + k, b, mr_ref, k)
        res_ref[k] = to_slots(mr_ref[k, 16:48, :], oh)
    copies.append(
        pltpu.make_async_copy(res_ref, res_hbm.at[pl.ds(2, 4), pl.ds(16, 32), :], sems.at[1])
    )
    copies[1].start()
    mom = jnp.zeros((16, 256), F32)
    for k in (0, 2):
        mom = mom + moments(wm_ref, 2 + k, mr_ref[k : k + 2].reshape(128, 256))
    mom_ref[...] = mom
    gr = coef_ref[1]
    group = jnp.concatenate([gr[0:1], gr[1:2], yd_ref[8, 4:5, :], yu_ref[8, 4:5, :]], 1)
    ny = pick_ref.shape[0]
    col = (group + 0.5).astype(jnp.int32) - lax.axis_index("sx") * (ny * GRP_DEV)
    owner = lax.shift_right_logical(col, 4)
    member = jnp.bitwise_and(col, 15)
    sel = lax.broadcasted_iota(jnp.int32, (ny, 512), 0)
    pick_ref[...] = jnp.where(sel == owner, 1.0, 0.0)
    sel = lax.broadcasted_iota(jnp.int32, (16, 512), 0)
    member_ref[...] = jnp.where(sel == member, 1.0, 0.0)
    for c in copies:
        c.wait()


def middle_kernel(
    src_ref, coef_ref, yd_ref, yu_ref, c_ref, a_ref, b_ref, own_down_ref, own_up_ref,
    mom_ref, pick_ref, member_ref, wm_ref, wr_ref,
    u_ref, mr_ref, to_down_ref, to_up_ref, part_ref, h, rim, edge,
):
    left, right, down, up = flags()
    l_ref, r_ref = Picked(a_ref, b_ref), Picked(b_ref, a_ref)
    for p in range(10):
        e = add_x(own_down_ref[p], p, l_ref, r_ref, left, right, slice(0, 2))
        edge[0, p] = jnp.concatenate([e[0:1] * down, e[1:2]], 0)
        e = add_x(own_up_ref[p], p, l_ref, r_ref, left, right, slice(16, 18))
        edge[1, p] = jnp.concatenate([e[0:1], e[1:2] * up], 0)
        if 3 < p < 6:
            continue
        g = add_x(c_ref[p], p, l_ref, r_ref, left, right)
        h[p] = g
        h[p, 0] = g[0] * down
        h[p, 17] = g[17] * up
    u_ref[0] = h[1, 1:17]
    u_ref[1] = h[8, 1:17]
    get_h = lambda p, y, n: h[p, y : y + n]
    coefs = [rows_of(coef_ref[0], 0), rows_of(coef_ref[0], 4)]
    for k, x in enumerate((0, 1, 6, 7)):
        for b in range(2):
            column_residual(get_h, src_ref, coefs[b], x, b, mr_ref, k)
    rim[...] = jnp.zeros((256, 256), F32)
    for k, out, far, near, tile, lanes, y_far, y_near in (
        (0, to_down_ref, 0, 1, yd_ref, slice(0, LANES), 2, 3),
        (1, to_up_ref, 1, 0, yu_ref, slice(LANES, 256), 1, 0),
    ):
        slab = edge.at[k]
        cf = rows_of(tile[8], 0)
        for x in range(8):
            p = x + 1
            v = slab[p, far : far + 1]
            res = stencil(
                cf,
                v,
                slab[p + 1, far : far + 1] + slab[p - 1, far : far + 1],
                slab[p, near : near + 1],
            )
            out[0, x] = v[0]
            out[1, x] = -res[0]
            at = (x * 4 + y_near) * 8
            rim[at : at + 8, lanes] = -res[0]
            at = (x * 4 + y_far) * 8
            rim[at : at + 8, lanes] = cf[1] * v[0]
    mom = mom_ref[...]
    mom = mom + moments(wm_ref, 0, mr_ref[0:2].reshape(128, 256))
    mom = mom + moments(wm_ref, 6, mr_ref[2:4].reshape(128, 256))
    rh, rl = split(rim[...])
    mom_y = dot(wr_ref[...], rh) + dot(wr_ref[...], rl)
    mom_y = mom_y[0:8] + mom_y[8:16]
    mom = jnp.concatenate(
        [mom[0:8] + mom[8:16], mom_y[:, :LANES] * down, mom_y[:, LANES:] * up], 1
    )
    member = member_ref[...]
    spread = jnp.concatenate([member * mom[v : v + 1] for v in range(8)], 0)
    sh, sl = split(spread)
    pick = pick_ref[...].astype(BF16)
    part_ref[...] = dot_t(pick, sh) + dot_t(pick, sl)


def last_kernel(
    smooth_in, res_in, c_ref, uout_ref, rin_ref, rout_ref, coef_ref, d_ref, u_ref, slot_ref,
    arrived_ref,
    smooth_hbm, res_hbm, coarse_hbm, smooth_ref, res_ref, coarse_ref, sems,
):
    _, _, down, up = flags()
    total = jnp.sum(arrived_ref[...], axis=0, keepdims=True)
    for v in range(8):
        coarse_ref[v : v + 1, :] = total[:, v * GRP_DEV : (v + 1) * GRP_DEV]
    copies = [pltpu.make_async_copy(coarse_ref, coarse_hbm, sems.at[8])]
    copies[0].start()

    def send(ref, hbm, x, nx, row, rows):
        at = (pl.ds(x, nx), pl.ds(row, rows), slice(None))
        k = len(copies) - 1
        copies.append(pltpu.make_async_copy(ref.at[at], hbm.at[at], sems.at[k]))
        copies[-1].start()

    oh = onehot(slot_ref[...])
    sides = (
        (d_ref, down, jnp.broadcast_to(coef_ref[0, 1:2, :], (8, LANES))),
        (u_ref, up, jnp.broadcast_to(coef_ref[0, 5:6, :], (8, LANES))),
    )

    def added(x):
        out = []
        for slab, on, cy in sides:
            v = slab[0, x] * on
            out.append((v, slab[1, x] * on, cy * v))
        return out

    zero = jnp.zeros((8, LANES), F32)
    pairs = [added(x) for x in range(8)]
    for k, x in enumerate((0, 1, 6, 7)):
        (_, d0, d1), (_, e0, e1) = pairs[x]
        add = jnp.concatenate(
            [
                jnp.concatenate([d0, d1] + [zero] * 6, 0),
                jnp.concatenate([zero] * 6 + [e1, e0], 0),
            ],
            1,
        )
        res_ref[x] = to_slots(rout_ref[k] + add, oh)
        if k == 1:
            send(res_ref, res_hbm, 0, 2, 0, 64)
    send(res_ref, res_hbm, 6, 2, 0, 64)
    low, high = [], []
    for k in range(4):
        (_, d0, d1), (_, e0, e1) = pairs[2 + k]
        z2 = jnp.zeros((16, LANES), F32)
        low.append(
            rin_ref[k, 0:16, :] + jnp.concatenate([jnp.concatenate([d0, d1], 0), z2], 1)
        )
        high.append(
            rin_ref[k, 48:64, :] + jnp.concatenate([z2, jnp.concatenate([e1, e0], 0)], 1)
        )
    res_ref[2:6, 0:16, :] = to_slots(jnp.concatenate(low, 0), oh).reshape(4, 16, 256)
    send(res_ref, res_hbm, 2, 4, 0, 16)
    res_ref[2:6, 48:64, :] = to_slots(jnp.concatenate(high, 0), oh).reshape(4, 16, 256)
    send(res_ref, res_hbm, 2, 4, 48, 16)
    for k, x in enumerate((0, 7)):
        (d0, _, _), (e0, _, _) = pairs[x]
        both = [uout_ref[k, 0:8].reshape(64, LANES), uout_ref[k, 8:16].reshape(64, LANES)]
        both[0] = both[0] + jnp.concatenate([d0] + [zero] * 7, 0)
        both[1] = both[1] + jnp.concatenate([zero] * 7 + [e0], 0)
        smooth_ref[x] = to_slots(jnp.concatenate(both, 1), oh)
        send(smooth_ref, smooth_hbm, x, 1, 0, 64)
    low, high = [], []
    for x in range(1, 7):
        (d0, _, _), (e0, _, _) = pairs[x]
        c = [c_ref[x + 1, y] for y in (1, 9, 8, 16)]
        low.append(jnp.concatenate([c[0] + d0, c[1]], 1))
        high.append(jnp.concatenate([c[2], c[3] + e0], 1))
    smooth_ref[1:7, 0:8, :] = to_slots(jnp.concatenate(low, 0), oh).reshape(6, 8, 256)
    send(smooth_ref, smooth_hbm, 1, 6, 0, 8)
    smooth_ref[1:7, 56:64, :] = to_slots(jnp.concatenate(high, 0), oh).reshape(6, 8, 256)
    send(smooth_ref, smooth_hbm, 1, 6, 56, 8)
    for c in copies:
        c.wait()


def sd(*shape):
    return jax.ShapeDtypeStruct(shape, F32)


def vm(*shape):
    return pltpu.VMEM(shape, F32)


def ring(value, axis, by):
    n = lax.axis_size(axis)
    return lax.ppermute(value, axis, [(i, (i + by) % n) for i in range(n)])


def snake(value, by):
    nx = lax.axis_size("sx")
    ny = lax.axis_size("sy")
    pairs = []
    for i in range(nx):
        for j in range(ny):
            to = i + (by if j % 2 == 0 else -by)
            target = to * ny + j if 0 <= to < nx else i * ny + (j ^ 1)
            pairs.append((i * ny + j, target))
    return lax.ppermute(value, ("sx", "sy"), pairs)


def call(kernel, outs, args, scratch=(), hbm_in=0, hbm_out=0, sems=0, alias=0):
    vmem = pl.BlockSpec(memory_space=pltpu.VMEM)
    hbm = pl.BlockSpec(memory_space=pltpu.HBM)
    args = [
        pltpu.with_memory_space_constraint(a, pltpu.HBM if k < hbm_in else pltpu.VMEM)
        for k, a in enumerate(args)
    ]
    scratch = [pltpu.VMEM(s, F32) if isinstance(s, tuple) else s for s in scratch]
    if sems:
        scratch.append(pltpu.SemaphoreType.DMA((sems,)))
    return pl.pallas_call(
        kernel,
        out_shape=outs,
        in_specs=[hbm if k < hbm_in else vmem for k in range(len(args))],
        out_specs=[hbm if k < hbm_out else vmem for k in range(len(outs))],
        scratch_shapes=scratch,
        input_output_aliases={k: k for k in range(alias)},
        compiler_params=pltpu.CompilerParams(vmem_limit_bytes=16 << 20),
    )(*args)


def on_device(right_side, stretch, mass_term, slot_position, coarse_group):
    a1 = jnp.asarray(A_FWD, BF16)
    a2 = jnp.asarray(A_BWD, BF16)
    lam = jnp.asarray(np.stack([LAM_J, LAM_K]), F32)
    wm = jnp.asarray(W_MOM, BF16)
    wr = jnp.asarray(W_RIM, BF16)
    row = pltpu.VMEM((1, 256), jnp.int32)
    rhs = right_side.reshape(8, 64, 256)
    coef, to_d, to_u, slot = call(
        start_kernel,
        [vm(2, 8, LANES), vm(9, 8, LANES), vm(9, 8, LANES), row],
        (
            rhs,
            stretch,
            mass_term.reshape(1, 256),
            slot_position.reshape(1, 256),
            coarse_group.reshape(1, 256),
        ),
        [(2, 8, 8, 256), (3, 256), (1, 256), row],
        hbm_in=5,
        sems=6,
    )
    yd = ring(to_u, "sy", 1)
    yu = ring(to_d, "sy", -1)
    src, dinv = call(
        place_kernel,
        [vm(8, 16, 8, LANES), vm(10, 104, 256)],
        (lam, rhs, slot, coef),
        [(2, 104, LANES)],
        hbm_in=1,
        sems=1,
    )
    to_a, to_b = call(rim_kernel, [vm(20, 8, LANES)] * 2, (src, coef, yd, yu))
    xa = snake(to_a, 1)
    xb = snake(to_b, -1)
    rin, sin = call(
        first_inner_kernel,
        [vm(8 * 192, LANES), vm(10, 104, 256)],
        (src, yd, yu, a1),
        [(8, 104, 256)],
    )

    side = vm(10, 3, 8, LANES)
    rout, w, to_d, to_u = call(
        first_kernel,
        [vm(2 * 192, LANES), vm(1920, LANES), side, side],
        (xa, xb, sin, dinv, a1, a2),
        [(2, 104, 256), (10, 104, 256)],
    )
    d = ring(to_u, "sy", 1)
    u = ring(to_d, "sy", -1)
    to_a, to_b = call(edge_kernel, [vm(3, 20, 8, LANES)] * 2, (w, d, u))
    a = snake(to_a, 1)
    b = snake(to_b, -1)
    hin, sin = call(
        second_inner_kernel,
        [vm(6, 20, 8, LANES), vm(10, 104, 256)],
        (rin, coef, yd, yu, w, d, u, a1),
        [(4, 5, 8, LANES), (4 * 192, LANES), (4, 104, 256)],
    )

    slab = vm(2, 18, 8, LANES)
    side = vm(10, 2, 8, LANES)
    c, to_a, to_b, own_d, own_u = call(
        second_kernel,
        [vm(10, 18, 8, LANES), slab, slab, side, side],
        (rin, rout, coef, xa, xb, yd, yu, w, a, b, d, u, hin, sin, dinv, a1, a2),
        [
            (6, 20, 8, LANES),
            (3, 4, 5, 8, LANES),
            (6 * 192, LANES),
            (6, 104, 256),
            (10, 104, 256),
            (1920, LANES),
        ],
    )
    a = snake(to_a, 1)
    b = snake(to_b, -1)
    edge = vm(2, 8, 8, LANES)
    ny = lax.axis_size("sy")
    smooth, res, rin, mom, pick, member = call(
        middle_inner_kernel,
        [sd(8, 64, 256), sd(8, 64, 256), vm(4, 64, 256), vm(16, 256), vm(ny, 512), vm(16, 512)],
        (src, coef, yd, yu, c, slot, wm),
        [(6, 18, 8, LANES), (6, 48, 256), (4, 32, 256)],
        hbm_out=2,
        sems=2,
    )
    uout, rout, to_d, to_u, part = call(
        middle_kernel,
        [vm(2, 16, 8, LANES), vm(4, 64, 256), edge, edge, vm(ny, LANES)],
        (src, coef, yd, yu, c, a, b, own_d, own_u, mom, pick, member, wm, wr),
        [(10, 18, 8, LANES), (256, 256), (2, 10, 2, 8, LANES)],
    )
    d = ring(to_u, "sy", 1)
    u = ring(to_d, "sy", -1)
    arrived = lax.all_to_all(part, "sy", split_axis=0, concat_axis=0, tiled=True)
    smooth, res, coarse = call(
        last_kernel,
        [sd(8, 64, 256), sd(8, 64, 256), sd(8, GRP_DEV)],
        (smooth, res, c, uout, rin, rout, coef, d, u, slot, arrived),
        [(8, 64, 256), (8, 64, 256), (8, GRP_DEV)],
        hbm_in=2,
        hbm_out=3,
        sems=9,
        alias=2,
    )
    return smooth.reshape(8, 8, 8, 256), res.reshape(8, 8, 8, 256), coarse


def solution(mesh):
    split_all = P(None, None, None, ("sx", "sy"))
    flat = P(("sx", "sy"))
    return jax.shard_map(
        on_device,
        mesh=mesh,
        in_specs=(split_all, P(None, ("sx", "sy")), flat, flat, flat),
        out_specs=(split_all, split_all, P(None, ("sx", "sy"))),
        check_vma=False,
    )
```

```python
import jax
import jax.numpy as jnp
import numpy as np
from jax import lax
from jax.experimental import pallas as pl
from jax.experimental.pallas import tpu as pltpu
from jax.sharding import PartitionSpec as P

NODES = 8
GRP_DEV = 16
LANES = 128
RELAX = 0.35
F32 = jnp.float32
BF16 = jnp.bfloat16


def split_np(a):
    a = np.asarray(a, np.float32)
    hi = np.asarray(jnp.asarray(a).astype(BF16).astype(F32))
    return hi, a - hi


def constants():
    n = NODES + 2
    col = np.arange(n, dtype=np.float64) + 1.0
    s = np.sqrt(2.0 / (n + 1.0)) * np.sin(np.pi * col[:, None] * col[None, :] / (n + 1.0))
    lam = 2.0 - 2.0 * np.cos(np.pi * col / (n + 1.0))
    fwd = np.zeros((104, 112))
    for q in range(n):
        for r in range(n):
            c = q * 8 + r - 1
            if r == 0:
                c = 80 + q
            if r == n - 1:
                c = 96 + q
            fwd[:100, c] = np.outer(s[:, q], s[:, r]).reshape(-1)
    fh, fl = split_np(fwd)
    a1 = np.concatenate([np.concatenate([fh, fh], 1), np.concatenate([fl, fl], 1)], 0)
    bh, bl = split_np(RELAX * fwd.T)
    a2 = np.concatenate([np.concatenate([bh, bh], 1), np.concatenate([bl, bl], 1)], 0)
    lam_j = np.ones((104, LANES), np.float32)
    lam_k = np.ones((104, LANES), np.float32)
    lam_j[:100] = np.repeat(lam, n)[:, None]
    lam_k[:100] = np.tile(lam, n)[:, None]
    t = np.arange(NODES) / (NODES - 1.0)
    w = np.stack([1.0 - t, t])
    wm = np.einsum("ax,by,cz->abcxyz", w, w, w).reshape(8, 512)
    wh, wl = split_np(wm)
    wm = np.concatenate([wh, wl], 0)
    rim = wm.reshape(16, 8, 8, 8)[:, :, [0, 1, 6, 7]].reshape(16, 256)
    return s, lam, a1, a2, lam_j, lam_k, wm, rim


SINES, LAM, A_FWD, A_BWD, LAM_J, LAM_K, W_MOM, W_RIM = constants()


def split(x):
    hi = x.astype(BF16)
    return hi, (x - hi.astype(F32)).astype(BF16)


def dot(a, b):
    return lax.dot_general(a, b, (((1,), (0,)), ((), ())), preferred_element_type=F32)


def dot_t(a, b):
    return lax.dot_general(a, b, (((1,), (1,)), ((), ())), preferred_element_type=F32)


def flags():
    i = lax.axis_index("sx")
    j = lax.axis_index("sy")
    nx = lax.axis_size("sx")
    ny = lax.axis_size("sy")
    one = lambda c: jnp.where(c, 1.0, 0.0).astype(F32)
    return one(i > 0), one(i < nx - 1), one(j > 0), one(j < ny - 1)


def even_row():
    return lax.rem(lax.axis_index("sy"), 2) == 0


class Picked:
    def __init__(self, first, second):
        self.refs = (first, second)

    def __getitem__(self, at):
        return jnp.where(even_row(), self.refs[0][at], self.refs[1][at])


def lane_up(x):
    lane = lax.broadcasted_iota(jnp.int32, x.shape, x.ndim - 1)
    return jnp.where(lane == LANES - 1, 0.0, pltpu.roll(x, LANES - 1, x.ndim - 1))


def lane_down(x):
    lane = lax.broadcasted_iota(jnp.int32, x.shape, x.ndim - 1)
    return jnp.where(lane == 0, 0.0, pltpu.roll(x, 1, x.ndim - 1))


def onehot(slot_row):
    p = lax.broadcasted_iota(jnp.int32, (256, 256), 0)
    return jnp.where(p == slot_row, 1.0, 0.0).astype(BF16)


def split3(a):
    a1 = a.astype(BF16)
    e = a - a1.astype(F32)
    a2 = e.astype(BF16)
    return a1, a2, (e - a2.astype(F32)).astype(BF16)


def start_kernel(
    rhs_hbm, stretch_hbm, mass_hbm, slot_hbm, group_hbm,
    coef_ref, to_down_ref, to_up_ref, slot_ref,
    face_ref, stretch_ref, mass_ref, group_ref, sems,
):
    pairs = (
        (slot_hbm, slot_ref),
        (rhs_hbm.at[:, pl.ds(0, 8), :], face_ref.at[0]),
        (rhs_hbm.at[:, pl.ds(56, 8), :], face_ref.at[1]),
        (stretch_hbm, stretch_ref),
        (mass_hbm, mass_ref),
        (group_hbm, group_ref),
    )
    copies = [pltpu.make_async_copy(h, v, sems.at[k]) for k, (h, v) in enumerate(pairs)]
    for c in copies:
        c.start()
    copies[0].wait()
    oh = onehot(slot_ref[...])
    for k, out, b in ((1, to_down_ref, 0), (2, to_up_ref, 1)):
        copies[k].wait()
        g = dot_t(jnp.concatenate(split3(face_ref[k - 1].reshape(64, 256)), 0), oh)
        g = g[0:64] + g[64:128] + g[128:192]
        out[0:8] = g[:, b * LANES : (b + 1) * LANES].reshape(8, 8, LANES)
    for c in copies[3:]:
        c.wait()
    c = jnp.concatenate(
        [
            stretch_ref[...],
            mass_ref[...],
            group_ref[...].astype(F32),
            jnp.zeros((3, 256), F32),
        ],
        0,
    )
    c1, c2, c3 = split3(c)
    cg = dot_t(c1, oh) + dot_t(c2, oh) + dot_t(c3, oh)
    coef = jnp.concatenate([cg[0:4, :LANES], cg[0:4, LANES:]], 0)
    gr = jnp.concatenate([cg[4:5, :LANES], cg[4:5, LANES:], jnp.zeros((6, LANES), F32)], 0)
    coef_ref[0] = coef
    coef_ref[1] = gr
    pad = jnp.zeros((3, LANES), F32)
    to_down_ref[8] = jnp.concatenate([coef[0:4], gr[0:1], pad], 0)
    to_up_ref[8] = jnp.concatenate([coef[4:8], gr[1:2], pad], 0)


def place_kernel(lam_hbm, rhs_ref, slot_ref, coef_ref, src_ref, dinv_ref, lam_ref, sems):
    lam = pltpu.make_async_copy(lam_hbm, lam_ref, sems.at[0])
    lam.start()
    oh = onehot(slot_ref[...])
    for x in range(8):
        g = dot_t(jnp.concatenate(split3(rhs_ref[x]), 0), oh)
        g = g[0:64] + g[64:128] + g[128:192]
        for b in range(2):
            src_ref[x, b * 8 : b * 8 + 8] = g[:, b * LANES : (b + 1) * LANES].reshape(8, 8, LANES)
    lam.wait()
    for b in range(2):
        lanes = slice(b * LANES, (b + 1) * LANES)
        cx, cy, cz, m, _ = rows_of(coef_ref[0], b * 4)
        cxl = [cx * float(v) for v in LAM]
        for t in range(13):
            row = slice(t * 8, t * 8 + 8)
            d0 = cy * lam_ref[0, row, :] + cz * lam_ref[1, row, :] + m
            for i in range(10):
                dinv_ref[i, row, lanes] = 1.0 / (d0 + cxl[i])


def rim_kernel(src_ref, coef_ref, yu_ref, yd_ref, to_a_ref, to_b_ref):
    coef_y = jnp.concatenate([yd_ref[8, 0:4, :], yu_ref[8, 0:4, :]], 0)
    even = even_row()
    coef = coef_ref[0]
    for out, x_even, x_odd in ((to_a_ref, 7, 0), (to_b_ref, 0, 7)):
        pick = lambda ref: jnp.where(even, ref[x_even], ref[x_odd])
        out[0] = pick(yd_ref)
        out[1:17] = pick(src_ref)
        out[17] = pick(yu_ref)
        out[18] = coef
        out[19] = coef_y


def forward(res, base, a1_ref):
    ends = []
    for z, shift in ((7, lane_down), (0, lane_up)):
        ends.append([shift(res[pl.ds(base + 64 * t + z, 8, stride=8), :]) for t in range(3)])
    halves = [
        jnp.concatenate(
            [res[base + 64 * b : base + 64 * b + 80, :]] + ends[0][b : b + 2] + ends[1][b : b + 2],
            0,
        )
        for b in range(2)
    ]
    hi, lo = split(jnp.concatenate(halves, 1))
    r = dot(a1_ref[...], jnp.concatenate([hi, lo], 0))
    return r[:104] + r[104:]


def along_x(layers, partial, row, lanes):
    acc = [None if partial is None else partial[i, row, lanes] for i in range(10)]
    for p, (low, high) in layers.items():
        v = low[0][low[1], row, lanes]
        w = high[0][high[1], row, lanes]
        h = (v + w, v - w)
        for i in range(10):
            term = h[i % 2] * float(SINES[i, p])
            acc[i] = term if acc[i] is None else acc[i] + term
    return acc


HALVES = (slice(0, LANES), slice(LANES, 256))


def partial_x(layers, out_ref):
    def chunk(t, carry):
        row = pl.ds(pl.multiple_of(t * 8, 8), 8)
        for lanes in HALVES:
            for i, v in enumerate(along_x(layers, None, row, lanes)):
                out_ref[i, row, lanes] = v
        return carry

    lax.fori_loop(0, 13, chunk, 0, unroll=True)


def finish_solves(layers, partial, dinv_ref, a2_ref, spec, wout):
    def chunk(t, carry):
        row = pl.ds(pl.multiple_of(t * 8, 8), 8)
        for lanes in HALVES:
            z = along_x(layers, partial, row, lanes)
            z = [z[i] * dinv_ref[i, row, lanes] for i in range(10)]
            for p in range(5):
                e = z[0] * float(SINES[0, p])
                o = z[1] * float(SINES[1, p])
                for i in range(2, 10, 2):
                    e = e + z[i] * float(SINES[i, p])
                    o = o + z[i + 1] * float(SINES[i + 1, p])
                spec[p, row, lanes] = e + o
                spec[9 - p, row, lanes] = e - o
        return carry

    lax.fori_loop(0, 13, chunk, 0, unroll=True)

    for p in range(10):
        base = p * 192
        hi, lo = split(spec[p])
        r = dot(a2_ref[...], jnp.concatenate([hi, lo], 0))
        r = r[:112] + r[112:]
        r0 = r[:, :LANES]
        r1 = r[:, LANES:]
        wout[base : base + 64, :] = r0[0:64]
        wout[base + 64 : base + 80, :] = r0[64:80] + r1[0:16]
        wout[base + 80 : base + 144, :] = r1[16:80]
        wout[base + 144 : base + 192, :] = jnp.zeros((48, LANES), F32)
        for off, z, shift in ((80, 7, lane_up), (96, 0, lane_down)):
            rows = [
                r0[off : off + 8],
                r0[off + 8 : off + 16] + r1[off : off + 8],
                r1[off + 8 : off + 16],
            ]
            for t in range(3):
                at = pl.ds(base + 64 * t + z, 8, stride=8)
                wout[at, :] = wout[at, :] + shift(rows[t])


def put(ref, p, y, value):
    n = value.shape[0]
    at = (p * 24 + y) * 8
    ref[at : at + n * 8, :] = value.reshape(n * 8, LANES)


def get(ref, p, y, n):
    at = (p * 24 + y) * 8
    return ref[at : at + n * 8, :].reshape(n, 8, LANES)


def with_rows(line, n, d, u, down, up):
    rows_d = d * down
    rows_u = u * up
    low = rows_d[n - 2 : n] + jnp.concatenate([line[0:1] * down, line[1:2]], 0)
    high = rows_u[0:2] + jnp.concatenate([line[16:17], line[17:18] * up], 0)
    parts = [low, line[2:16], high]
    if n > 2:
        parts = [rows_d[0 : n - 2]] + parts + [rows_u[2:n]]
    return jnp.concatenate(parts, 0)


def put_layer(ref, at, below, line, above):
    put(ref, at, 0, below)
    put(ref, at, 1, line)
    put(ref, at, 17, above)
    put(ref, at, 18, jnp.zeros((6, 8, LANES), F32))


def first_inner_kernel(src_ref, yd_ref, yu_ref, a1_ref, rin_ref, sin_ref, sout):
    _, _, down, up = flags()
    for x in range(8):
        put_layer(rin_ref, x, yd_ref[x : x + 1] * down, src_ref[x], yu_ref[x : x + 1] * up)
        sout[x] = forward(rin_ref, x * 192, a1_ref)
    partial_x({p: ((sout, p - 1), (sout, 8 - p)) for p in range(1, 5)}, sin_ref)


def first_kernel(
    xa_ref, xb_ref, sin_ref, dinv_ref, a1_ref, a2_ref,
    rout_ref, wout, to_down_ref, to_up_ref, sout, spec,
):
    left, right, down, up = flags()
    x_refs = Picked(xa_ref, xb_ref), Picked(xb_ref, xa_ref)
    for k, (x_ref, side) in enumerate(zip(x_refs, (left, right))):
        put_layer(
            rout_ref,
            k,
            x_ref[0:1] * (side * down),
            x_ref[1:17] * side,
            x_ref[17:18] * (side * up),
        )
        sout[k] = forward(rout_ref, k * 192, a1_ref)
    finish_solves({0: ((sout, 0), (sout, 1))}, sin_ref, dinv_ref, a2_ref, spec, wout)
    for p in range(10):
        to_down_ref[p] = get(wout, p, 0, 3)
        to_up_ref[p] = get(wout, p, 15, 3)


def edge_kernel(w_ref, u_ref, d_ref, a_ref, b_ref):
    _, _, down, up = flags()
    even = even_row()
    for k in range(3):
        to_l, to_r = [
            with_rows(get(w_ref, p, 0, 18), 3, d_ref[p], u_ref[p], down, up) for p in (k, 7 + k)
        ]
        a_ref[k] = jnp.where(even, to_r, to_l)
        b_ref[k] = jnp.where(even, to_l, to_r)


def neighbours_z(u):
    z = lax.broadcasted_iota(jnp.int32, u.shape, 1)
    s = pltpu.roll(u, 7, 1)
    above = jnp.where(z == 7, lane_up(s), s)
    s = pltpu.roll(u, 1, 1)
    below = jnp.where(z == 0, lane_down(s), s)
    return above, below


ROWS = ((0, 1, 0), (1, 4, 1), (5, 4, 1), (9, 4, 2), (13, 4, 2), (17, 1, 3))


def second_residual(get_h, get_r, cb, p, at, res_ref, left, right, down, up):
    for y, n, b in ROWS:
        v = get_h(p + 1, y + 1, n)
        res = get_r(y, n) - stencil(
            cb[b],
            v,
            get_h(p + 2, y + 1, n) + get_h(p, y + 1, n),
            get_h(p + 1, y + 2, n) + get_h(p + 1, y, n),
        )
        if p == 0:
            res = res * left
        if p == 9:
            res = res * right
        if y == 0:
            res = res * down
        if y == 17:
            res = res * up
        put(res_ref, at, y, res)
    put(res_ref, at, 18, jnp.zeros((6, 8, LANES), F32))


def spread_coefs(cb, rows):
    for b, (tile, at) in enumerate(rows):
        for k, v in enumerate(rows_of(tile, at)):
            cb[b, k] = v
    return [[cb.at[b, k] for k in range(5)] for b in range(4)]


class Loaded:
    def __init__(self, refs):
        self.refs = refs

    def __getitem__(self, k):
        return self.refs[k][...]


def second_inner_kernel(
    rin_ref, coef_ref, yd_ref, yu_ref, w_ref, d_ref, u_ref, a1_ref, h_ref, sin_ref, cb, r1, sout,
):
    left, right, down, up = flags()
    for x in range(3, 9):
        h_ref[x - 3] = with_rows(get(w_ref, x - 1, 0, 18), 3, d_ref[x - 1], u_ref[x - 1], down, up)
    tiles = spread_coefs(
        cb, ((yd_ref[8], 0), (coef_ref[0], 0), (coef_ref[0], 4), (yu_ref[8], 0))
    )
    coefs = [Loaded(t) for t in tiles]
    get_h = lambda x, y, n: h_ref[x - 3, y : y + n]
    for k in range(4):
        p = 3 + k
        get_r = lambda y, n: get(rin_ref, p - 1, y, n)
        second_residual(get_h, get_r, coefs, p, k, r1, left, right, down, up)
        sout[k] = forward(r1, k * 192, a1_ref)
    partial_x({p: ((sout, p - 3), (sout, 6 - p)) for p in (3, 4)}, sin_ref)


def second_kernel(
    rin_ref, rout_ref, coef_ref, xa_ref, xb_ref, yd_ref, yu_ref, w_ref, a_ref, b_ref, d_ref, u_ref,
    hin_ref, sin_ref, dinv_ref, a1_ref, a2_ref,
    c_ref, to_a_ref, to_b_ref, own_down_ref, own_up_ref, h, cb, r1, sout, spec, wout,
):
    left, right, down, up = flags()
    l_ref, r_ref = Picked(a_ref, b_ref), Picked(b_ref, a_ref)
    for x in (0, 1, 2, 9, 10, 11):
        if x == 0:
            g = l_ref[0] * left
        elif x == 11:
            g = r_ref[2] * right
        else:
            g = with_rows(get(w_ref, x - 1, 0, 18), 3, d_ref[x - 1], u_ref[x - 1], down, up)
            if x == 1:
                g = (g + l_ref[1]) * left
            elif x == 2:
                g = g + l_ref[2] * left
            elif x == 9:
                g = g + r_ref[0] * right
            elif x == 10:
                g = (g + r_ref[1]) * right
        h[x if x < 3 else x - 6] = g

    def get_h(x, y, n):
        if 3 <= x <= 8:
            return hin_ref[x - 3, y : y + n]
        return h[x if x < 3 else x - 6, y : y + n]

    coefs = []
    for a, x_ref in ((0, Picked(xa_ref, xb_ref)), (1, None), (2, Picked(xb_ref, xa_ref))):
        if x_ref is None:
            rows = ((yd_ref[8], 0), (coef_ref[0], 0), (coef_ref[0], 4), (yu_ref[8], 0))
        else:
            own, beside = x_ref[18], x_ref[19]
            rows = ((beside, 0), (own, 0), (own, 4), (beside, 4))
        coefs.append([Loaded(t) for t in spread_coefs(cb.at[a], rows)])
    for k, p in enumerate((0, 1, 2, 7, 8, 9)):
        if p in (0, 9):
            get_r = lambda y, n: get(rout_ref, 0 if p == 0 else 1, y, n)
        else:
            get_r = lambda y, n: get(rin_ref, p - 1, y, n)
        cb_p = coefs[0 if p == 0 else 2 if p == 9 else 1]
        second_residual(get_h, get_r, cb_p, p, k, r1, left, right, down, up)
        sout[k] = forward(r1, k * 192, a1_ref)
    layers = {p: ((sout, p), (sout, 5 - p)) for p in range(3)}
    finish_solves(layers, sin_ref, dinv_ref, a2_ref, spec, wout)
    for p in range(10):
        line = get(wout, p, 0, 18)
        c_ref[p] = get_h(p + 1, 1, 18) + line
        own_down_ref[p] = line[0:2]
        own_up_ref[p] = line[16:18]
    even = even_row()
    for k in range(2):
        to_l, to_r = get(wout, k, 0, 18), get(wout, 8 + k, 0, 18)
        to_a_ref[k] = jnp.where(even, to_r, to_l)
        to_b_ref[k] = jnp.where(even, to_l, to_r)


def add_x(g, p, l, r, left, right, y=slice(0, 18)):
    if p == 0:
        return (g + l[0, y]) * left
    if p == 1:
        return g + l[1, y] * left
    if p == 8:
        return g + r[0, y] * right
    if p == 9:
        return (g + r[1, y]) * right
    return g


def rows_of(tile, at):
    c = [jnp.broadcast_to(tile[at + k : at + k + 1, :], (8, LANES)) for k in range(4)]
    return c + [2.0 * (c[0] + c[1] + c[2]) + c[3]]


def stencil(cf, v, x_sum, y_sum):
    above, below = neighbours_z(v)
    return cf[4] * v - cf[0] * x_sum - cf[1] * y_sum - cf[2] * (above + below)


def column_residual(get_h, src_ref, cf, x, b, mr_ref, at):
    lanes = slice(b * LANES, (b + 1) * LANES)
    for y in (0, 4):
        yy = b * 8 + y + 1
        p = x + 1
        v = get_h(p, yy, 4)
        res = src_ref[x, yy - 1 : yy + 3] - stencil(
            cf,
            v,
            get_h(p + 1, yy, 4) + get_h(p - 1, yy, 4),
            get_h(p, yy + 1, 4) + get_h(p, yy - 1, 4),
        )
        mr_ref[at, y * 8 : y * 8 + 32, lanes] = res.reshape(32, LANES)


def moments(wm_ref, x, rows):
    rh, rl = split(rows)
    w = wm_ref[:, x * 64 : x * 64 + rows.shape[0]]
    return dot(w, rh) + dot(w, rl)


def to_slots(uv, oh):
    hi, lo = split(uv)
    n = uv.shape[0]
    o = dot(jnp.concatenate([hi, lo], 0), oh)
    return o[:n] + o[n:]


def middle_inner_kernel(
    src_ref, coef_ref, yd_ref, yu_ref, c_ref, slot_ref, wm_ref,
    smooth_hbm, res_hbm, mr_ref, mom_ref, pick_ref, member_ref, h, smooth_ref, res_ref, sems,
):
    _, _, down, up = flags()
    oh = onehot(slot_ref[...])
    copies = []
    for x in range(1, 7):
        both = [c_ref[x + 1, 8 * b + 2 : 8 * b + 8].reshape(48, LANES) for b in range(2)]
        smooth_ref[x - 1] = to_slots(jnp.concatenate(both, 1), oh)
    copies.append(
        pltpu.make_async_copy(smooth_ref, smooth_hbm.at[pl.ds(1, 6), pl.ds(8, 48), :], sems.at[0])
    )
    copies[0].start()
    for k in range(6):
        h[k] = c_ref[k + 2]
        h[k, 0] = c_ref[k + 2, 0] * down
        h[k, 17] = c_ref[k + 2, 17] * up
    get_h = lambda p, y, n: h[p - 2, y : y + n]
    coefs = [rows_of(coef_ref[0], 0), rows_of(coef_ref[0], 4)]
    for k in range(4):
        for b in range(2):
            column_residual(get_h, src_ref, coefs[b], 2 + k, b, mr_ref, k)
        res_ref[k] = to_slots(mr_ref[k, 16:48, :], oh)
    copies.append(
        pltpu.make_async_copy(res_ref, res_hbm.at[pl.ds(2, 4), pl.ds(16, 32), :], sems.at[1])
    )
    copies[1].start()
    mom = jnp.zeros((16, 256), F32)
    for k in (0, 2):
        mom = mom + moments(wm_ref, 2 + k, mr_ref[k : k + 2].reshape(128, 256))
    mom_ref[...] = mom
    gr = coef_ref[1]
    group = jnp.concatenate([gr[0:1], gr[1:2], yd_ref[8, 4:5, :], yu_ref[8, 4:5, :]], 1)
    ny = pick_ref.shape[0]
    col = (group + 0.5).astype(jnp.int32) - lax.axis_index("sx") * (ny * GRP_DEV)
    owner = lax.shift_right_logical(col, 4)
    member = jnp.bitwise_and(col, 15)
    sel = lax.broadcasted_iota(jnp.int32, (ny, 512), 0)
    pick_ref[...] = jnp.where(sel == owner, 1.0, 0.0)
    sel = lax.broadcasted_iota(jnp.int32, (16, 512), 0)
    member_ref[...] = jnp.where(sel == member, 1.0, 0.0)
    for c in copies:
        c.wait()


def middle_kernel(
    src_ref, coef_ref, yd_ref, yu_ref, c_ref, a_ref, b_ref, own_down_ref, own_up_ref,
    mom_ref, pick_ref, member_ref, wm_ref, wr_ref,
    u_ref, mr_ref, to_down_ref, to_up_ref, part_ref, h, rim, edge,
):
    left, right, down, up = flags()
    l_ref, r_ref = Picked(a_ref, b_ref), Picked(b_ref, a_ref)
    for p in range(10):
        e = add_x(own_down_ref[p], p, l_ref, r_ref, left, right, slice(0, 2))
        edge[0, p] = jnp.concatenate([e[0:1] * down, e[1:2]], 0)
        e = add_x(own_up_ref[p], p, l_ref, r_ref, left, right, slice(16, 18))
        edge[1, p] = jnp.concatenate([e[0:1], e[1:2] * up], 0)
        if 3 < p < 6:
            continue
        g = add_x(c_ref[p], p, l_ref, r_ref, left, right)
        h[p] = g
        h[p, 0] = g[0] * down
        h[p, 17] = g[17] * up
    u_ref[0] = h[1, 1:17]
    u_ref[1] = h[8, 1:17]
    get_h = lambda p, y, n: h[p, y : y + n]
    coefs = [rows_of(coef_ref[0], 0), rows_of(coef_ref[0], 4)]
    for k, x in enumerate((0, 1, 6, 7)):
        for b in range(2):
            column_residual(get_h, src_ref, coefs[b], x, b, mr_ref, k)
    rim[...] = jnp.zeros((256, 256), F32)
    for k, out, far, near, tile, lanes, y_far, y_near in (
        (0, to_down_ref, 0, 1, yd_ref, slice(0, LANES), 2, 3),
        (1, to_up_ref, 1, 0, yu_ref, slice(LANES, 256), 1, 0),
    ):
        slab = edge.at[k]
        cf = rows_of(tile[8], 0)
        for x in range(8):
            p = x + 1
            v = slab[p, far : far + 1]
            res = stencil(
                cf,
                v,
                slab[p + 1, far : far + 1] + slab[p - 1, far : far + 1],
                slab[p, near : near + 1],
            )
            out[0, x] = v[0]
            out[1, x] = -res[0]
            at = (x * 4 + y_near) * 8
            rim[at : at + 8, lanes] = -res[0]
            at = (x * 4 + y_far) * 8
            rim[at : at + 8, lanes] = cf[1] * v[0]
    mom = mom_ref[...]
    mom = mom + moments(wm_ref, 0, mr_ref[0:2].reshape(128, 256))
    mom = mom + moments(wm_ref, 6, mr_ref[2:4].reshape(128, 256))
    rh, rl = split(rim[...])
    mom_y = dot(wr_ref[...], rh) + dot(wr_ref[...], rl)
    mom_y = mom_y[0:8] + mom_y[8:16]
    mom = jnp.concatenate(
        [mom[0:8] + mom[8:16], mom_y[:, :LANES] * down, mom_y[:, LANES:] * up], 1
    )
    member = member_ref[...]
    spread = jnp.concatenate([member * mom[v : v + 1] for v in range(8)], 0)
    sh, sl = split(spread)
    pick = pick_ref[...].astype(BF16)
    part_ref[...] = dot_t(pick, sh) + dot_t(pick, sl)


def last_kernel(
    smooth_in, res_in, c_ref, uout_ref, rin_ref, rout_ref, coef_ref, u_ref, d_ref, slot_ref,
    arrived_ref,
    smooth_hbm, res_hbm, coarse_hbm, smooth_ref, res_ref, coarse_ref, sems,
):
    _, _, down, up = flags()
    total = jnp.sum(arrived_ref[...], axis=0, keepdims=True)
    for v in range(8):
        coarse_ref[v : v + 1, :] = total[:, v * GRP_DEV : (v + 1) * GRP_DEV]
    copies = [pltpu.make_async_copy(coarse_ref, coarse_hbm, sems.at[8])]
    copies[0].start()

    def send(ref, hbm, x, nx, row, rows):
        at = (pl.ds(x, nx), pl.ds(row, rows), slice(None))
        k = len(copies) - 1
        copies.append(pltpu.make_async_copy(ref.at[at], hbm.at[at], sems.at[k]))
        copies[-1].start()

    oh = onehot(slot_ref[...])
    sides = (
        (d_ref, down, jnp.broadcast_to(coef_ref[0, 1:2, :], (8, LANES))),
        (u_ref, up, jnp.broadcast_to(coef_ref[0, 5:6, :], (8, LANES))),
    )

    def added(x):
        out = []
        for slab, on, cy in sides:
            v = slab[0, x] * on
            out.append((v, slab[1, x] * on, cy * v))
        return out

    zero = jnp.zeros((8, LANES), F32)
    pairs = [added(x) for x in range(8)]
    for k, x in enumerate((0, 1, 6, 7)):
        (_, d0, d1), (_, e0, e1) = pairs[x]
        add = jnp.concatenate(
            [
                jnp.concatenate([d0, d1] + [zero] * 6, 0),
                jnp.concatenate([zero] * 6 + [e1, e0], 0),
            ],
            1,
        )
        res_ref[x] = to_slots(rout_ref[k] + add, oh)
        if k == 1:
            send(res_ref, res_hbm, 0, 2, 0, 64)
    send(res_ref, res_hbm, 6, 2, 0, 64)
    low, high = [], []
    for k in range(4):
        (_, d0, d1), (_, e0, e1) = pairs[2 + k]
        z2 = jnp.zeros((16, LANES), F32)
        low.append(
            rin_ref[k, 0:16, :] + jnp.concatenate([jnp.concatenate([d0, d1], 0), z2], 1)
        )
        high.append(
            rin_ref[k, 48:64, :] + jnp.concatenate([z2, jnp.concatenate([e1, e0], 0)], 1)
        )
    res_ref[2:6, 0:16, :] = to_slots(jnp.concatenate(low, 0), oh).reshape(4, 16, 256)
    send(res_ref, res_hbm, 2, 4, 0, 16)
    res_ref[2:6, 48:64, :] = to_slots(jnp.concatenate(high, 0), oh).reshape(4, 16, 256)
    send(res_ref, res_hbm, 2, 4, 48, 16)
    for k, x in enumerate((0, 7)):
        (d0, _, _), (e0, _, _) = pairs[x]
        both = [uout_ref[k, 0:8].reshape(64, LANES), uout_ref[k, 8:16].reshape(64, LANES)]
        both[0] = both[0] + jnp.concatenate([d0] + [zero] * 7, 0)
        both[1] = both[1] + jnp.concatenate([zero] * 7 + [e0], 0)
        smooth_ref[x] = to_slots(jnp.concatenate(both, 1), oh)
        send(smooth_ref, smooth_hbm, x, 1, 0, 64)
    low, high = [], []
    for x in range(1, 7):
        (d0, _, _), (e0, _, _) = pairs[x]
        c = [c_ref[x + 1, y] for y in (1, 9, 8, 16)]
        low.append(jnp.concatenate([c[0] + d0, c[1]], 1))
        high.append(jnp.concatenate([c[2], c[3] + e0], 1))
    smooth_ref[1:7, 0:8, :] = to_slots(jnp.concatenate(low, 0), oh).reshape(6, 8, 256)
    send(smooth_ref, smooth_hbm, 1, 6, 0, 8)
    smooth_ref[1:7, 56:64, :] = to_slots(jnp.concatenate(high, 0), oh).reshape(6, 8, 256)
    send(smooth_ref, smooth_hbm, 1, 6, 56, 8)
    for c in copies:
        c.wait()


def sd(*shape):
    return jax.ShapeDtypeStruct(shape, F32)


def vm(*shape):
    return pltpu.VMEM(shape, F32)


def ring(value, axis, by):
    n = lax.axis_size(axis)
    return lax.ppermute(value, axis, [(i, (i + by) % n) for i in range(n)])


def snake(value, by):
    nx = lax.axis_size("sx")
    ny = lax.axis_size("sy")
    pairs = []
    for i in range(nx):
        for j in range(ny):
            to = i + (by if j % 2 == 0 else -by)
            target = to * ny + j if 0 <= to < nx else i * ny + (j ^ 1)
            pairs.append((i * ny + j, target))
    return lax.ppermute(value, ("sx", "sy"), pairs)


def call(kernel, outs, args, scratch=(), hbm_in=0, hbm_out=0, sems=0, alias=0):
    vmem = pl.BlockSpec(memory_space=pltpu.VMEM)
    hbm = pl.BlockSpec(memory_space=pltpu.HBM)
    args = [
        pltpu.with_memory_space_constraint(a, pltpu.HBM if k < hbm_in else pltpu.VMEM)
        for k, a in enumerate(args)
    ]
    scratch = [pltpu.VMEM(s, F32) if isinstance(s, tuple) else s for s in scratch]
    if sems:
        scratch.append(pltpu.SemaphoreType.DMA((sems,)))
    return pl.pallas_call(
        kernel,
        out_shape=outs,
        in_specs=[hbm if k < hbm_in else vmem for k in range(len(args))],
        out_specs=[hbm if k < hbm_out else vmem for k in range(len(outs))],
        scratch_shapes=scratch,
        input_output_aliases={k: k for k in range(alias)},
        compiler_params=pltpu.CompilerParams(vmem_limit_bytes=16 << 20),
    )(*args)


def on_device(right_side, stretch, mass_term, slot_position, coarse_group):
    a1 = jnp.asarray(A_FWD, BF16)
    a2 = jnp.asarray(A_BWD, BF16)
    lam = jnp.asarray(np.stack([LAM_J, LAM_K]), F32)
    wm = jnp.asarray(W_MOM, BF16)
    wr = jnp.asarray(W_RIM, BF16)
    row = pltpu.VMEM((1, 256), jnp.int32)
    rhs = right_side.reshape(8, 64, 256)
    coef, to_d, to_u, slot = call(
        start_kernel,
        [vm(2, 8, LANES), vm(9, 8, LANES), vm(9, 8, LANES), row],
        (
            rhs,
            stretch,
            mass_term.reshape(1, 256),
            slot_position.reshape(1, 256),
            coarse_group.reshape(1, 256),
        ),
        [(2, 8, 8, 256), (3, 256), (1, 256), row],
        hbm_in=5,
        sems=6,
    )
    yu = ring(to_d, "sy", -1)
    yd = ring(to_u, "sy", 1)
    src, dinv = call(
        place_kernel,
        [vm(8, 16, 8, LANES), vm(10, 104, 256)],
        (lam, rhs, slot, coef),
        [(2, 104, LANES)],
        hbm_in=1,
        sems=1,
    )
    to_a, to_b = call(rim_kernel, [vm(20, 8, LANES)] * 2, (src, coef, yu, yd))
    xa = snake(to_a, 1)
    xb = snake(to_b, -1)
    rin, sin = call(
        first_inner_kernel,
        [vm(8 * 192, LANES), vm(10, 104, 256)],
        (src, yd, yu, a1),
        [(8, 104, 256)],
    )

    side = vm(10, 3, 8, LANES)
    rout, w, to_d, to_u = call(
        first_kernel,
        [vm(2 * 192, LANES), vm(1920, LANES), side, side],
        (xa, xb, sin, dinv, a1, a2),
        [(2, 104, 256), (10, 104, 256)],
    )
    u = ring(to_d, "sy", -1)
    d = ring(to_u, "sy", 1)
    to_a, to_b = call(edge_kernel, [vm(3, 20, 8, LANES)] * 2, (w, u, d))
    a = snake(to_a, 1)
    b = snake(to_b, -1)
    hin, sin = call(
        second_inner_kernel,
        [vm(6, 20, 8, LANES), vm(10, 104, 256)],
        (rin, coef, yd, yu, w, d, u, a1),
        [(4, 5, 8, LANES), (4 * 192, LANES), (4, 104, 256)],
    )

    slab = vm(2, 18, 8, LANES)
    side = vm(10, 2, 8, LANES)
    c, to_a, to_b, own_d, own_u = call(
        second_kernel,
        [vm(10, 18, 8, LANES), slab, slab, side, side],
        (rin, rout, coef, xa, xb, yd, yu, w, a, b, d, u, hin, sin, dinv, a1, a2),
        [
            (6, 20, 8, LANES),
            (3, 4, 5, 8, LANES),
            (6 * 192, LANES),
            (6, 104, 256),
            (10, 104, 256),
            (1920, LANES),
        ],
    )
    a = snake(to_a, 1)
    b = snake(to_b, -1)
    edge = vm(2, 8, 8, LANES)
    ny = lax.axis_size("sy")
    smooth, res, rin, mom, pick, member = call(
        middle_inner_kernel,
        [sd(8, 64, 256), sd(8, 64, 256), vm(4, 64, 256), vm(16, 256), vm(ny, 512), vm(16, 512)],
        (src, coef, yd, yu, c, slot, wm),
        [(6, 18, 8, LANES), (6, 48, 256), (4, 32, 256)],
        hbm_out=2,
        sems=2,
    )
    uout, rout, to_d, to_u, part = call(
        middle_kernel,
        [vm(2, 16, 8, LANES), vm(4, 64, 256), edge, edge, vm(ny, LANES)],
        (src, coef, yd, yu, c, a, b, own_d, own_u, mom, pick, member, wm, wr),
        [(10, 18, 8, LANES), (256, 256), (2, 10, 2, 8, LANES)],
    )
    u = ring(to_d, "sy", -1)
    d = ring(to_u, "sy", 1)
    arrived = lax.all_to_all(part, "sy", split_axis=0, concat_axis=0, tiled=True)
    smooth, res, coarse = call(
        last_kernel,
        [sd(8, 64, 256), sd(8, 64, 256), sd(8, GRP_DEV)],
        (smooth, res, c, uout, rin, rout, coef, u, d, slot, arrived),
        [(8, 64, 256), (8, 64, 256), (8, GRP_DEV)],
        hbm_in=2,
        hbm_out=3,
        sems=9,
        alias=2,
    )
    return smooth.reshape(8, 8, 8, 256), res.reshape(8, 8, 8, 256), coarse


def solution(mesh):
    split_all = P(None, None, None, ("sx", "sy"))
    flat = P(("sx", "sy"))
    return jax.shard_map(
        on_device,
        mesh=mesh,
        in_specs=(split_all, P(None, ("sx", "sy")), flat, flat, flat),
        out_specs=(split_all, split_all, P(None, ("sx", "sy"))),
        check_vma=False,
    )
```
